32 devices in a mesh: dp: 16 (over z, y, x), mp: 2 (over core).
Axes of the slice: x: 2, y: 2, z: 4, core: 2. Of those that a mesh axis runs over, the one named last changes fastest.
Arguments:
- tokens: bfloat16 [192, 196, 512], P('dp'), may hold values from -6 to 6
- cotangent: float32 [192, 196, 512], P('dp'), may hold values from -6 to 6
- image_count: int32 [16], P('dp'), may hold values from 1 to 12, as said below
- rel_index: int32 [49, 49], replicated, may hold values from 0 to 168, as said below
- w_qkv: float32 [2, 512, 3, 512], P(None, 'dp', None, 'mp'), may hold values from -0.25 to 0.25
- w_proj: float32 [2, 512, 512], P(None, 'mp', 'dp'), may hold values from -0.5 to 0.5
- w_fc_one: float32 [2, 512, 2048], P(None, 'dp', 'mp'), may hold values from -0.25 to 0.25
- w_fc_two: float32 [2, 2048, 512], P(None, 'mp', 'dp'), may hold values from -0.125 to 0.125
- qv_bias: float32 [2, 2, 512], P(None, None, 'mp'), may hold values from -3 to 3
- fc_one_bias: float32 [2, 2048], P(None, 'mp'), may hold values from -3 to 3
- rel_table: float32 [2, 169, 16], P(None, None, 'mp'), may hold values from -4 to 4
- norm_vec: float32 [2, 6, 512], replicated, may hold values from 0.1 to 1.9
- m_qkv: float32 [2, 512, 3, 512], P(None, 'dp', None, 'mp'), may hold values from -40 to 40
- m_proj: float32 [2, 512, 512], P(None, 'mp', 'dp'), may hold values from -40 to 40
- m_fc_one: float32 [2, 512, 2048], P(None, 'dp', 'mp'), may hold values from -40 to 40
- m_fc_two: float32 [2, 2048, 512], P(None, 'mp', 'dp'), may hold values from -40 to 40
- m_qv_bias: float32 [2, 2, 512], P(None, None, 'mp'), may hold values from -40 to 40
- m_fc_one_bias: float32 [2, 2048], P(None, 'mp'), may hold values from -40 to 40
- m_rel_table: float32 [2, 169, 16], P(None, None, 'mp'), may hold values from -40 to 40
- m_norm_vec: float32 [2, 6, 512], replicated, may hold values from -40 to 40
- v_qkv: float32 [2, 512, 3, 512], P(None, 'dp', None, 'mp'), may hold values from 3.7632 to 37.632
- v_proj: float32 [2, 512, 512], P(None, 'mp', 'dp'), may hold values from 3.7632 to 37.632
- v_fc_one: float32 [2, 512, 2048], P(None, 'dp', 'mp'), may hold values from 3.7632 to 37.632
- v_fc_two: float32 [2, 2048, 512], P(None, 'mp', 'dp'), may hold values from 3.7632 to 37.632
- v_qv_bias: float32 [2, 2, 512], P(None, None, 'mp'), may hold values from 3.7632 to 37.632
- v_fc_one_bias: float32 [2, 2048], P(None, 'mp'), may hold values from 3.7632 to 37.632
- v_rel_table: float32 [2, 169, 16], P(None, None, 'mp'), may hold values from 3.7632 to 37.632
- v_norm_vec: float32 [2, 6, 512], replicated, may hold values from 3.7632 to 37.632
Outputs:
- out: float32 [192, 196, 512], P('dp')
- x_grad: float32 [192, 196, 512], P('dp')
- new_w_qkv: float32 [2, 512, 3, 512], P(None, 'dp', None, 'mp')
- new_w_proj: float32 [2, 512, 512], P(None, 'mp', 'dp')
- new_w_fc_one: float32 [2, 512, 2048], P(None, 'dp', 'mp')
- new_w_fc_two: float32 [2, 2048, 512], P(None, 'mp', 'dp')
- new_qv_bias: float32 [2, 2, 512], P(None, None, 'mp')
- new_fc_one_bias: float32 [2, 2048], P(None, 'mp')
- new_rel_table: float32 [2, 169, 16], P(None, None, 'mp')
- new_norm_vec: float32 [2, 6, 512], replicated
- new_m_qkv: float32 [2, 512, 3, 512], P(None, 'dp', None, 'mp')
- new_m_proj: float32 [2, 512, 512], P(None, 'mp', 'dp')
- new_m_fc_one: float32 [2, 512, 2048], P(None, 'dp', 'mp')
- new_m_fc_two: float32 [2, 2048, 512], P(None, 'mp', 'dp')
- new_m_qv_bias: float32 [2, 2, 512], P(None, None, 'mp')
- new_m_fc_one_bias: float32 [2, 2048], P(None, 'mp')
- new_m_rel_table: float32 [2, 169, 16], P(None, None, 'mp')
- new_m_norm_vec: float32 [2, 6, 512], replicated
- new_v_qkv: float32 [2, 512, 3, 512], P(None, 'dp', None, 'mp')
- new_v_proj: float32 [2, 512, 512], P(None, 'mp', 'dp')
- new_v_fc_one: float32 [2, 512, 2048], P(None, 'dp', 'mp')
- new_v_fc_two: float32 [2, 2048, 512], P(None, 'mp', 'dp')
- new_v_qv_bias: float32 [2, 2, 512], P(None, None, 'mp')
- new_v_fc_one_bias: float32 [2, 2048], P(None, 'mp')
- new_v_rel_table: float32 [2, 169, 16], P(None, None, 'mp')
- new_v_norm_vec: float32 [2, 6, 512], replicated
The draws below stay inside these ranges and needn't reach their ends.
Inputs may be any that keep to these rules, and one draw needn't show every extreme that they name: `image_count`: slots below a device's count hold live images; some index of dp holds 12. `rel_index`: pairs of window positions with the same relative offset share one entry; distinct offsets have distinct entries.
All inputs are finite; a program needn't handle non-finite values.
Results may differ from the reference program's by a relative error of at most 0.023.
Values may be sent and summed in bfloat16 or wider, within the bound.
A program may use at most 320 MiB of HBM per device.

```python
import math
import jax
import jax.numpy as jnp
from jax import lax

D = 512
HEADS = 16
FF = 2048
HD = 32
SIDE = 14
WIN = 7
SHIFT = 3
SEQ = 196
WSEQ = 49
TABLE = 169
LAYERS = 2
IMG_DEV = 12
IMAGES = 192
N_DP = 16


def draw_image_count(key, part):
    key_one, key_two = jax.random.split(jax.random.fold_in(key, 11))
    counts = jax.random.randint(key_one, (N_DP,), 1, IMG_DEV + 1)
    busiest = jax.random.randint(key_two, (), 0, N_DP)
    return counts.at[busiest].set(IMG_DEV).astype(jnp.int32)


def draw_rel_index(key, part):
    positions = jnp.arange(WSEQ, dtype=jnp.int32)
    row_pos = positions // WIN
    col_pos = positions % WIN
    delta_row = row_pos[:, None] - row_pos[None, :] + WIN - 1
    delta_col = col_pos[:, None] - col_pos[None, :] + WIN - 1
    natural = delta_row * (2 * WIN - 1) + delta_col
    relabel = jax.random.permutation(jax.random.fold_in(key, 23), TABLE).astype(jnp.int32)
    return relabel[natural].astype(jnp.int32)


def level_of(key, shape, cuts, low, top_value):
    gain, own = 1.0, jax.random.fold_in(key, 6)
    for dim, blocks in cuts:
        draws = jnp.exp(jax.random.uniform(jax.random.fold_in(own, dim), (blocks,), jnp.float32, low / len(cuts), top_value / len(cuts)))
        gain = gain * jnp.repeat(draws, shape[dim] // blocks).reshape([-1 if axis == dim else 1 for axis in range(len(shape))])
    return gain


def gaussian(rng, shape, scale, reach, cuts=(), kind=jnp.bfloat16):
    drawn = jax.random.normal(rng, shape, jnp.float32) * scale
    if len(cuts) > 0:
        drawn = level_of(rng, shape, cuts, -0.22, 0.18) * drawn
    return jnp.clip(drawn, min=-reach, max=reach).astype(kind)


def setup_inputs(seed: int = 0) -> dict:
    seeds = jax.random.split(jax.random.key(seed), 29)
    return {
        "tokens": gaussian(seeds[0], (IMAGES, SEQ, D), 1.0, 6.0, ((0, 16),)),
        "cotangent": gaussian(seeds[1], (IMAGES, SEQ, D), 1.0, 6.0, ((0, 16),), jnp.float32),
        "image_count": draw_image_count(jax.random.fold_in(seeds[28], 71), 0),
        "rel_index": draw_rel_index(jax.random.fold_in(seeds[28], 71), 0),
        "w_qkv": gaussian(seeds[4], (LAYERS, D, 3, D), D ** -0.5, 0.25, ((1, 16), (3, 2)), jnp.float32),
        "w_proj": gaussian(seeds[5], (LAYERS, D, D), (D // 4) ** -0.5, 0.5, ((1, 2), (2, 16)), jnp.float32),
        "w_fc_one": gaussian(seeds[6], (LAYERS, D, FF), D ** -0.5, 0.25, ((1, 16), (2, 2)), jnp.float32),
        "w_fc_two": gaussian(seeds[7], (LAYERS, FF, D), FF ** -0.5, 0.125, ((1, 2), (2, 16)), jnp.float32),
        "qv_bias": gaussian(seeds[8], (LAYERS, 2, D), 0.5, 3.0, ((2, 2),), jnp.float32),
        "fc_one_bias": gaussian(seeds[9], (LAYERS, FF), 0.5, 3.0, ((1, 2),), jnp.float32),
        "rel_table": gaussian(seeds[10], (LAYERS, TABLE, HEADS), 1.0, 4.0, ((2, 2),), jnp.float32),
        "norm_vec": jnp.clip(1.0 + 0.18 * jax.random.normal(seeds[11], (LAYERS, 6, D), jnp.float32), 0.1, 1.9),
        "m_qkv": gaussian(seeds[12], (LAYERS, D, 3, D), (0.05 * (IMG_DEV * N_DP * 98) ** 0.5), 40.0, ((1, 16), (3, 2)), jnp.float32),
        "m_proj": gaussian(seeds[13], (LAYERS, D, D), (0.05 * (IMG_DEV * N_DP * 98) ** 0.5), 40.0, ((1, 2), (2, 16)), jnp.float32),
        "m_fc_one": gaussian(seeds[14], (LAYERS, D, FF), (0.05 * (IMG_DEV * N_DP * 98) ** 0.5), 40.0, ((1, 16), (2, 2)), jnp.float32),
        "m_fc_two": gaussian(seeds[15], (LAYERS, FF, D), (0.05 * (IMG_DEV * N_DP * 98) ** 0.5), 40.0, ((1, 2), (2, 16)), jnp.float32),
        "m_qv_bias": gaussian(seeds[16], (LAYERS, 2, D), (0.05 * (IMG_DEV * N_DP * 98) ** 0.5), 40.0, ((2, 2),), jnp.float32),
        "m_fc_one_bias": gaussian(seeds[17], (LAYERS, FF), (0.05 * (IMG_DEV * N_DP * 98) ** 0.5), 40.0, ((1, 2),), jnp.float32),
        "m_rel_table": gaussian(seeds[18], (LAYERS, TABLE, HEADS), (0.05 * (IMG_DEV * N_DP * 98) ** 0.5), 40.0, ((2, 2),), jnp.float32),
        "m_norm_vec": gaussian(seeds[19], (LAYERS, 6, D), (0.05 * (IMG_DEV * N_DP * 98) ** 0.5), 40.0, (), jnp.float32),
        "v_qkv": jnp.clip(jnp.exp(math.log(37.632) - 2.3025851 * jax.random.uniform(seeds[20], (LAYERS, D, 3, D), jnp.float32) ** level_of(seeds[20], (LAYERS, D, 3, D), ((1, 16), (3, 2)), -0.2, 0.2)), 3.7632, 37.632),
        "v_proj": jnp.clip(jnp.exp(math.log(37.632) - 2.3025851 * jax.random.uniform(seeds[21], (LAYERS, D, D), jnp.float32) ** level_of(seeds[21], (LAYERS, D, D), ((1, 2), (2, 16)), -0.2, 0.2)), 3.7632, 37.632),
        "v_fc_one": jnp.clip(jnp.exp(math.log(37.632) - 2.3025851 * jax.random.uniform(seeds[22], (LAYERS, D, FF), jnp.float32) ** level_of(seeds[22], (LAYERS, D, FF), ((1, 16), (2, 2)), -0.2, 0.2)), 3.7632, 37.632),
        "v_fc_two": jnp.clip(jnp.exp(math.log(37.632) - 2.3025851 * jax.random.uniform(seeds[23], (LAYERS, FF, D), jnp.float32) ** level_of(seeds[23], (LAYERS, FF, D), ((1, 2), (2, 16)), -0.2, 0.2)), 3.7632, 37.632),
        "v_qv_bias": jnp.clip(jnp.exp(math.log(37.632) - 2.3025851 * jax.random.uniform(seeds[24], (LAYERS, 2, D), jnp.float32) ** level_of(seeds[24], (LAYERS, 2, D), ((2, 2),), -0.2, 0.2)), 3.7632, 37.632),
        "v_fc_one_bias": jnp.clip(jnp.exp(math.log(37.632) - 2.3025851 * jax.random.uniform(seeds[25], (LAYERS, FF), jnp.float32) ** level_of(seeds[25], (LAYERS, FF), ((1, 2),), -0.2, 0.2)), 3.7632, 37.632),
        "v_rel_table": jnp.clip(jnp.exp(math.log(37.632) - 2.3025851 * jax.random.uniform(seeds[26], (LAYERS, TABLE, HEADS), jnp.float32) ** level_of(seeds[26], (LAYERS, TABLE, HEADS), ((2, 2),), -0.2, 0.2)), 3.7632, 37.632),
        "v_norm_vec": jnp.clip(jnp.exp(jax.random.uniform(seeds[27], (LAYERS, 6, D), jnp.float32, math.log(3.7632), math.log(37.632))), 3.7632, 37.632),
    }


norm_eps = 1e-05
mask_fill = -100.0
beta_one = 0.9
beta_two = 0.999
adam_eps = 1e-08
learn_rate = 0.02
decay_rate = 0.05
adam_step = 3.0
root_half = 0.7071067811865476
inv_root_two_pi = 0.3989422804014327

def region_map():
    positions = jnp.arange(SIDE, dtype=jnp.int32)
    band = (positions >= SIDE - WIN).astype(jnp.int32) + (positions >= SIDE - SHIFT).astype(jnp.int32)
    return 3 * band[:, None] + band[None, :]

def to_windows(tensor, shifted):
    channels = tensor.shape[-1]
    num_images = tensor.shape[0] // SEQ
    across = SIDE // WIN
    layout = tensor.reshape(num_images, SIDE, SIDE, channels)
    if shifted:
        layout = jnp.roll(layout, (-SHIFT, -SHIFT), axis=(1, 2))
    layout = layout.reshape(num_images, across, WIN, across, WIN, channels).transpose(0, 1, 3, 2, 4, 5)
    return layout.reshape(num_images * across * across, WSEQ, channels)

def from_windows(tensor, shifted):
    channels = tensor.shape[-1]
    across = SIDE // WIN
    num_images = tensor.shape[0] // (across * across)
    layout = tensor.reshape(num_images, across, across, WIN, WIN, channels).transpose(0, 1, 3, 2, 4, 5)
    layout = layout.reshape(num_images, SIDE, SIDE, channels)
    if shifted:
        layout = jnp.roll(layout, (SHIFT, SHIFT), axis=(1, 2))
    return layout.reshape(num_images * SEQ, channels)

def split_heads(row_data, shifted, num_heads):
    windows = to_windows(row_data, shifted)
    return windows.reshape(windows.shape[0], WSEQ, num_heads, HD)

def merge_heads(windows, shifted):
    return from_windows(windows.reshape(windows.shape[0], WSEQ, -1), shifted)

def norm_forward(layer_in, gain_vec, shift_vec):
    row_mean = lax.optimization_barrier(jnp.mean(layer_in, -1, keepdims=True))
    centered = layer_in - row_mean
    row_var = lax.optimization_barrier(jnp.mean(centered * centered, -1, keepdims=True))
    inv_std = lax.rsqrt(row_var + norm_eps)
    norm_hat = centered * inv_std
    return (norm_hat * gain_vec + shift_vec, norm_hat, inv_std)

def norm_backward(grad_norm, norm_hat, inv_std, gain_vec):
    scaled = grad_norm * gain_vec
    grad_in = inv_std * (scaled - lax.optimization_barrier(jnp.mean(scaled, -1, keepdims=True)) - norm_hat * lax.optimization_barrier(jnp.mean(scaled * norm_hat, -1, keepdims=True)))
    return (grad_in, lax.optimization_barrier(jnp.sum(grad_norm * norm_hat, 0)), lax.optimization_barrier(jnp.sum(grad_norm, 0)))

def gelu_value(pre_value):
    return pre_value * 0.5 * (1.0 + lax.erf(pre_value * root_half))

def gelu_slope(pre_value):
    return 0.5 * (1.0 + lax.erf(pre_value * root_half)) + pre_value * jnp.exp(-0.5 * pre_value * pre_value) * inv_root_two_pi

def head_bias(onehot_table, table_vals):
    picked = jnp.dot(onehot_table, table_vals, precision=lax.Precision.HIGHEST)
    return picked.T.reshape(table_vals.shape[1], WSEQ, WSEQ)

def attend(q_win, k_win, bias_heads, mask_add):
    scores = jnp.einsum('wihd,wjhd->whij', q_win.astype(jnp.float32), k_win.astype(jnp.float32)) * HD ** (-0.5)
    scores = scores + bias_heads[None]
    if mask_add is not None:
        shaped = scores.reshape(-1, mask_add.shape[0], scores.shape[1], WSEQ, WSEQ) + mask_add[None, :, None]
        scores = shaped.reshape(scores.shape)
    return jax.nn.softmax(scores, axis=-1)

def layer_forward(layer_in, weights, qv_vec, one_vec, norm_rows, bias_heads, mask_add, shifted):
    weight_qkv, weight_proj, weight_one, weight_two = weights
    num_heads = bias_heads.shape[0]
    head_cols = num_heads * HD
    normed, hat_one, std_one = norm_forward(layer_in, norm_rows[0], norm_rows[1])
    normed_b = normed.astype(jnp.bfloat16)
    qkv_rows = jnp.dot(normed_b, weight_qkv.reshape(D, 3 * head_cols).astype(jnp.bfloat16), preferred_element_type=jnp.float32).reshape(-1, 3, head_cols)
    query_b = (qkv_rows[:, 0] + qv_vec[0]).astype(jnp.bfloat16)
    key_b = qkv_rows[:, 1].astype(jnp.bfloat16)
    value_b = (qkv_rows[:, 2] + qv_vec[1]).astype(jnp.bfloat16)
    q_win = split_heads(query_b, shifted, num_heads)
    k_win = split_heads(key_b, shifted, num_heads)
    v_win = split_heads(value_b, shifted, num_heads)
    attn_probs = attend(q_win, k_win, bias_heads, mask_add)
    probs_b = attn_probs.astype(jnp.bfloat16)
    mixed_win = jnp.einsum('whij,wjhd->wihd', probs_b.astype(jnp.float32), v_win.astype(jnp.float32)).astype(jnp.bfloat16)
    mixed_rows = merge_heads(mixed_win, shifted)
    mid_state = layer_in + jnp.dot(mixed_rows, weight_proj.astype(jnp.bfloat16), preferred_element_type=jnp.float32) + norm_rows[4]
    hidden, hat_two, std_two = norm_forward(mid_state, norm_rows[2], norm_rows[3])
    hidden_b = hidden.astype(jnp.bfloat16)
    pre_value = jnp.dot(hidden_b, weight_one.astype(jnp.bfloat16), preferred_element_type=jnp.float32) + one_vec
    act_b = gelu_value(pre_value).astype(jnp.bfloat16)
    layer_out = mid_state + jnp.dot(act_b, weight_two.astype(jnp.bfloat16), preferred_element_type=jnp.float32) + norm_rows[5]
    saved_list = (hat_one, std_one, normed_b, q_win, k_win, v_win, mixed_rows, hat_two, std_two, hidden_b, pre_value, act_b)
    return (layer_out, saved_list)

def layer_backward(grad_out, saved_list, weights, norm_rows, bias_heads, mask_add, shifted, onehot_table):
    hat_one, std_one, normed_b, q_win, k_win, v_win, mixed_rows, hat_two, std_two, hidden_b, pre_value, act_b = saved_list
    weight_qkv, weight_proj, weight_one, weight_two = weights
    num_heads = bias_heads.shape[0]
    head_cols = num_heads * HD
    grad_b = grad_out.astype(jnp.bfloat16)
    grad_two = jnp.dot(act_b.T, grad_b, preferred_element_type=jnp.float32)
    grad_bias_two = lax.optimization_barrier(jnp.sum(grad_out, 0))
    grad_pre = jnp.dot(grad_b, weight_two.astype(jnp.bfloat16).T, preferred_element_type=jnp.float32) * gelu_slope(pre_value)
    grad_pre_b = grad_pre.astype(jnp.bfloat16)
    grad_bias_one = lax.optimization_barrier(jnp.sum(grad_pre, 0))
    grad_one = jnp.dot(hidden_b.T, grad_pre_b, preferred_element_type=jnp.float32)
    grad_hidden = jnp.dot(grad_pre_b, weight_one.astype(jnp.bfloat16).T, preferred_element_type=jnp.float32)
    back_two, gain_two, shift_two = norm_backward(grad_hidden, hat_two, std_two, norm_rows[2])
    grad_mid = grad_out + back_two
    mid_b = grad_mid.astype(jnp.bfloat16)
    grad_bias_proj = lax.optimization_barrier(jnp.sum(grad_mid, 0))
    grad_proj = jnp.dot(mixed_rows.T, mid_b, preferred_element_type=jnp.float32)
    grad_mixed = jnp.dot(mid_b, weight_proj.astype(jnp.bfloat16).T, preferred_element_type=jnp.float32).astype(jnp.bfloat16)
    gm_win = split_heads(grad_mixed, shifted, num_heads)
    attn_probs = attend(q_win, k_win, bias_heads, mask_add)
    probs_b = attn_probs.astype(jnp.bfloat16)
    grad_probs = jnp.einsum('wihd,wjhd->whij', gm_win.astype(jnp.float32), v_win.astype(jnp.float32))
    grad_v = jnp.einsum('whij,wihd->wjhd', probs_b.astype(jnp.float32), gm_win.astype(jnp.float32))
    grad_scores = attn_probs * (grad_probs - lax.optimization_barrier(jnp.sum(grad_probs * attn_probs, -1, keepdims=True)))
    pair_sums = lax.optimization_barrier(jnp.sum(grad_scores, 0)).reshape(num_heads, WSEQ * WSEQ)
    grad_table = jnp.dot(onehot_table.T, pair_sums.T, precision=lax.Precision.HIGHEST)
    scores_b = grad_scores.astype(jnp.bfloat16).astype(jnp.float32)
    grad_q = jnp.einsum('whij,wjhd->wihd', scores_b, k_win.astype(jnp.float32)) * HD ** (-0.5)
    grad_k = jnp.einsum('whij,wihd->wjhd', scores_b, q_win.astype(jnp.float32)) * HD ** (-0.5)
    q_rows = merge_heads(grad_q, shifted)
    k_rows = merge_heads(grad_k, shifted)
    v_rows = merge_heads(grad_v, shifted)
    grad_qv = jnp.stack([lax.optimization_barrier(jnp.sum(q_rows, 0)), lax.optimization_barrier(jnp.sum(v_rows, 0))])
    grad_qkv_b = jnp.stack([q_rows, k_rows, v_rows], axis=1).astype(jnp.bfloat16).reshape(-1, 3 * head_cols)
    grad_qkv = jnp.dot(normed_b.T, grad_qkv_b, preferred_element_type=jnp.float32).reshape(D, 3, head_cols)
    grad_normed = jnp.dot(grad_qkv_b, weight_qkv.reshape(D, 3 * head_cols).astype(jnp.bfloat16).T, preferred_element_type=jnp.float32)
    back_one, gain_one, shift_one = norm_backward(grad_normed, hat_one, std_one, norm_rows[0])
    grad_in = grad_mid + back_one
    norm_grads = jnp.stack([gain_one, shift_one, gain_two, shift_two, grad_bias_proj, grad_bias_two])
    return (grad_in, (grad_qkv, grad_proj, grad_one, grad_two, grad_qv, grad_bias_one, grad_table, norm_grads))

def adam_update(weight_in, moment_one, moment_two, grad_sum, decay):
    new_one = beta_one * moment_one + (1.0 - beta_one) * grad_sum
    new_two = beta_two * moment_two + (1.0 - beta_two) * grad_sum * grad_sum
    hat_one = new_one / (1.0 - beta_one ** adam_step)
    hat_two = new_two / (1.0 - beta_two ** adam_step)
    new_weight = weight_in - learn_rate * (hat_one / (jnp.sqrt(hat_two) + adam_eps) + decay * weight_in)
    return (new_weight, new_one, new_two)

def reference(tokens, cotangent, image_count, rel_index, w_qkv, w_proj, w_fc_one, w_fc_two, qv_bias, fc_one_bias, rel_table, norm_vec, m_qkv, m_proj, m_fc_one, m_fc_two, m_qv_bias, m_fc_one_bias, m_rel_table, m_norm_vec, v_qkv, v_proj, v_fc_one, v_fc_two, v_qv_bias, v_fc_one_bias, v_rel_table, v_norm_vec):
    onehot_table = (rel_index.reshape(WSEQ * WSEQ)[:, None] == jnp.arange(TABLE, dtype=jnp.int32)[None, :]).astype(jnp.float32)
    across = SIDE // WIN
    region_ids = region_map()
    region_win = region_ids.reshape(across, WIN, across, WIN).transpose(0, 2, 1, 3).reshape(across * across, WSEQ)
    mask_add = jnp.where(region_win[:, :, None] != region_win[:, None, :], mask_fill, 0.0).astype(jnp.float32)
    bias_list = [head_bias(onehot_table, rel_table[layer_idx]) for layer_idx in range(LAYERS)]
    params = (w_qkv, w_proj, w_fc_one, w_fc_two, qv_bias, fc_one_bias, rel_table, norm_vec)

    def one_group(grad_sums, inputs):
        image_block, cot_block, group_count = inputs
        live_mask = (jnp.arange(IMG_DEV, dtype=jnp.int32) < group_count).astype(jnp.float32)
        layer_in = image_block.astype(jnp.float32).reshape(IMG_DEV * SEQ, D)
        saved_all = []
        for layer_idx in range(LAYERS):
            shifted = layer_idx % 2 == 1
            layer_in, saved_list = layer_forward(layer_in, (w_qkv[layer_idx], w_proj[layer_idx], w_fc_one[layer_idx], w_fc_two[layer_idx]), qv_bias[layer_idx], fc_one_bias[layer_idx], norm_vec[layer_idx], bias_list[layer_idx], mask_add if shifted else None, shifted)
            saved_all.append(saved_list)
        grad_out = (cot_block.astype(jnp.float32) * live_mask[:, None, None]).reshape(IMG_DEV * SEQ, D)
        per_layer = [None] * LAYERS
        for layer_idx in reversed(range(LAYERS)):
            shifted = layer_idx % 2 == 1
            grad_out, per_layer[layer_idx] = layer_backward(grad_out, saved_all[layer_idx], (w_qkv[layer_idx], w_proj[layer_idx], w_fc_one[layer_idx], w_fc_two[layer_idx]), norm_vec[layer_idx], bias_list[layer_idx], mask_add if shifted else None, shifted, onehot_table)
        new_sums = tuple((grad_sums[slot] + jnp.stack([per_layer[layer_idx][slot] for layer_idx in range(LAYERS)]) for slot in range(8)))
        return (new_sums, (layer_in.reshape(IMG_DEV, SEQ, D), grad_out.reshape(IMG_DEV, SEQ, D)))
    start_sums = tuple((jnp.zeros(param.shape, jnp.float32) for param in params))
    grad_sums, (out_blocks, grad_blocks) = lax.scan(one_group, start_sums, (tokens.reshape(N_DP, IMG_DEV, SEQ, D), cotangent.reshape(N_DP, IMG_DEV, SEQ, D), image_count))
    out = out_blocks.reshape(IMAGES, SEQ, D)
    x_grad = grad_blocks.reshape(IMAGES, SEQ, D)
    new_w_qkv, new_m_qkv, new_v_qkv = adam_update(w_qkv, m_qkv, v_qkv, grad_sums[0], decay_rate)
    new_w_proj, new_m_proj, new_v_proj = adam_update(w_proj, m_proj, v_proj, grad_sums[1], decay_rate)
    new_w_fc_one, new_m_fc_one, new_v_fc_one = adam_update(w_fc_one, m_fc_one, v_fc_one, grad_sums[2], decay_rate)
    new_w_fc_two, new_m_fc_two, new_v_fc_two = adam_update(w_fc_two, m_fc_two, v_fc_two, grad_sums[3], decay_rate)
    new_qv_bias, new_m_qv_bias, new_v_qv_bias = adam_update(qv_bias, m_qv_bias, v_qv_bias, grad_sums[4], 0.0)
    new_fc_one_bias, new_m_fc_one_bias, new_v_fc_one_bias = adam_update(fc_one_bias, m_fc_one_bias, v_fc_one_bias, grad_sums[5], 0.0)
    new_rel_table, new_m_rel_table, new_v_rel_table = adam_update(rel_table, m_rel_table, v_rel_table, grad_sums[6], 0.0)
    new_norm_vec, new_m_norm_vec, new_v_norm_vec = adam_update(norm_vec, m_norm_vec, v_norm_vec, grad_sums[7], 0.0)
    return (out, x_grad, new_w_qkv, new_w_proj, new_w_fc_one, new_w_fc_two, new_qv_bias, new_fc_one_bias, new_rel_table, new_norm_vec, new_m_qkv, new_m_proj, new_m_fc_one, new_m_fc_two, new_m_qv_bias, new_m_fc_one_bias, new_m_rel_table, new_m_norm_vec, new_v_qkv, new_v_proj, new_v_fc_one, new_v_fc_two, new_v_qv_bias, new_v_fc_one_bias, new_v_rel_table, new_v_norm_vec)
```

```python
import functools

import jax
import jax.numpy as jnp
import numpy as np
from jax import lax
from jax.experimental import pallas as pl
from jax.experimental.pallas import tpu as pltpu
from jax.sharding import PartitionSpec as P

D = 512
HD = 32
SIDE = 14
WIN = 7
SHIFT = 3
SEQ = 196
WSEQ = 49
TABLE = 169
LAYERS = 2
SEQP = 200
PAIR = 2
ROWS = PAIR * SEQP
WROW = 64
WIMG = 4 * WROW
WPAIR = PAIR * WIMG
HALF = 256
GROUP = 8
LANES = GROUP * WROW
FFH = 1024
QKV = 3 * HALF
COLS = 2 * FFH + QKV + HALF
ATT = 2 * FFH

norm_eps = 1e-05
mask_fill = -100.0
pad_fill = -1e30
beta_one = 0.9
beta_two = 0.999
adam_eps = 1e-08
learn_rate = 0.02
decay_rate = 0.05
adam_step = 3.0
root_half = 0.7071067811865476
inv_root_two_pi = 0.3989422804014327
score_scale = HD**-0.5

f32 = jnp.float32
bf16 = jnp.bfloat16


def dot(a, b, ca=1, cb=0):
    return lax.dot_general(a, b, (((ca,), (cb,)), ((), ())), preferred_element_type=f32)


def window_tokens(shifted):
    off = SHIFT if shifted else 0
    out = np.zeros((4, WSEQ), np.int64)
    for wr in range(2):
        for wc in range(2):
            for p in range(WSEQ):
                r = (7 * wr + p // 7 + off) % SIDE
                c = (7 * wc + p % 7 + off) % SIDE
                out[wr * 2 + wc, p] = r * SIDE + c
    return out


def permutation(shifted):
    tok = window_tokens(shifted)
    perm = np.zeros((WIMG, SEQP), np.float32)
    for w in range(4):
        perm[w * WROW + np.arange(WSEQ), tok[w]] = 1.0
    return perm


def region_mask():
    pos = np.arange(SIDE)
    band = (pos >= SIDE - WIN).astype(int) + (pos >= SIDE - SHIFT).astype(int)
    region = 3 * band[:, None] + band[None, :]
    win = region.reshape(2, WIN, 2, WIN).transpose(0, 2, 1, 3).reshape(4, WSEQ)
    out = np.zeros((4, WROW, WROW), np.float32)
    out[:, :WSEQ, :WSEQ] = np.where(win[:, :, None] != win[:, None, :], mask_fill, 0.0)
    return out


def norm_stats(z):
    mean = jnp.mean(z, -1, keepdims=True)
    cen = z - mean
    var = jnp.mean(cen * cen, -1, keepdims=True)
    inv = lax.rsqrt(var + norm_eps)
    return cen * inv, inv


def norm_back(e, hat, inv, gain):
    s = e * gain
    return inv * (s - jnp.mean(s, -1, keepdims=True) - hat * jnp.mean(s * hat, -1, keepdims=True))


def row_sum(v):
    return jnp.sum(v, 0, keepdims=True)


def put_images(ref, blk):
    for im in range(PAIR):
        ref[im * SEQP : im * SEQP + SEQ, :] = blk[im].astype(f32)
        ref[im * SEQP + SEQ : (im + 1) * SEQP, :] = jnp.zeros((SEQP - SEQ, D), f32)


def to_window_rows(perm, rows, out_ref):
    for im in range(PAIR):
        part = rows[im * SEQP : (im + 1) * SEQP].astype(bf16)
        out_ref[im * WIMG : (im + 1) * WIMG, :] = dot(perm, part).astype(bf16)


def to_token_rows(perm_t, ref):
    return jnp.concatenate(
        [dot(perm_t, ref[im * WIMG : (im + 1) * WIMG, :]) for im in range(PAIR)], 0
    ).astype(bf16)


def expand_heads(x, hm_ref):
    return jnp.concatenate([x * hm_ref[h : h + 1, :] for h in range(GROUP)], 0)


def fold_heads(o):
    lane = lax.broadcasted_iota(jnp.int32, (WROW, HALF), 1) // HD
    acc = o[:WROW]
    for h in range(1, GROUP):
        acc = jnp.where(lane == h, o[h * WROW : (h + 1) * WROW], acc)
    return acc


def softmax_cols(k, qx, bias):
    s = dot(k, qx, 1, 1) * score_scale + bias
    e = jnp.exp(s - jnp.max(s, 0, keepdims=True))
    return e * (1.0 / jnp.sum(e, 0, keepdims=True))


def attend_forward(x, w_ref, bias_ref, qvb_ref, nv_ref, perm_ref, perm_t_ref, hm_ref,
                   qkv_ref, mixed_ref, nperm, mixw, windows):
    hat, _ = norm_stats(x)
    normed = hat * nv_ref[0:1, :] + nv_ref[1:2, :]
    to_window_rows(perm_ref[...], normed, nperm)
    for m in range(2):
        r = dot(nperm[...], w_ref[m, :, :QKV])
        qkv_ref[:, m * QKV : (m + 1) * QKV] = (r + qvb_ref[m : m + 1, :]).astype(bf16)

    def body(w, carry):
        rows = pl.ds(pl.multiple_of(w * WROW, WROW), WROW)
        wt = lax.rem(w, windows) if windows > 1 else 0
        for m in range(2):
            base = m * QKV
            q = qkv_ref[rows, base : base + HALF]
            k = qkv_ref[rows, base + HALF : base + 2 * HALF]
            v = qkv_ref[rows, base + 2 * HALF : base + QKV]
            pr = softmax_cols(k, expand_heads(q, hm_ref), bias_ref[wt, m])
            o = dot(pr.astype(bf16), v, 0, 0)
            mixw[rows, m * HALF : (m + 1) * HALF] = fold_heads(o).astype(bf16)
        return carry

    lax.fori_loop(0, 4 * PAIR, body, 0)
    mixed = to_token_rows(perm_t_ref[...], mixw)
    mixed_ref[...] = mixed
    attn = dot(mixed[:, :HALF], w_ref[0, :, QKV:], 1, 1) + dot(mixed[:, HALF:], w_ref[1, :, QKV:], 1, 1)
    return x + attn + nv_ref[4:5, :]


CH = 512


def mlp_forward(mid, w_ref, b1_ref, nv_ref, act_ref, slope_ref):
    hat, _ = norm_stats(mid)
    hid = (hat * nv_ref[2:3, :] + nv_ref[3:4, :]).astype(bf16)
    total = jnp.zeros((ROWS, D), f32)
    for m in range(2):
        for c in range(0, FFH, CH):
            col = m * FFH + c
            u = dot(hid, w_ref[m, :, c : c + CH]) + b1_ref[:, col : col + CH]
            phi = 0.5 + 0.5 * lax.erf(u * root_half)
            act = (u * phi).astype(bf16)
            act_ref[:, col : col + CH] = act
            slope_ref[:, col : col + CH] = (phi + u * jnp.exp(-0.5 * u * u) * inv_root_two_pi).astype(bf16)
            total += dot(act, w_ref[m, :, FFH + c : FFH + c + CH], 1, 1)
    return mid + total + nv_ref[5:6, :]


def mlp_backward(gout, mid, w_ref, nv_ref, slope_ref, gp, hid_s, gb_s, rows, b1_acc, nv_acc):
    hat, inv = norm_stats(mid)
    hid_s[rows, :] = (hat * nv_ref[2:3, :] + nv_ref[3:4, :]).astype(bf16)
    gb = gout.astype(bf16)
    gb_s[rows, :] = gb
    ghid = jnp.zeros((ROWS, D), f32)
    for m in range(2):
        for c in range(0, FFH, CH):
            col = m * FFH + c
            g = dot(gb, w_ref[m, :, FFH + c : FFH + c + CH]) * slope_ref[:, col : col + CH].astype(f32)
            b1_acc[:, col : col + CH] += row_sum(g)
            g = g.astype(bf16)
            gp[rows, col : col + CH] = g
            ghid += dot(g, w_ref[m, :, c : c + CH], 1, 1)
    gmid = gout + norm_back(ghid, hat, inv, nv_ref[2:3, :])
    nv_acc[2:3, :] += row_sum(ghid * hat)
    nv_acc[3:4, :] += row_sum(ghid)
    nv_acc[4:5, :] += row_sum(gmid)
    nv_acc[5:6, :] += row_sum(gout)
    return gmid


def attend_backward(gmid, x, w_ref, bias_ref, nv_ref, perm_ref, perm_t_ref, hm_ref, qkv_ref,
                    mperm, gmw, gqw, gq_s, mb_s, nb_s, rows, ds_acc, qv_acc, nv_acc, windows):
    hat, inv = norm_stats(x)
    nb_s[rows, :] = (hat * nv_ref[0:1, :] + nv_ref[1:2, :]).astype(bf16)
    mb_s[rows, :] = gmid.astype(bf16)
    to_window_rows(perm_ref[...], gmid, mperm)
    for m in range(2):
        gmw[:, m * HALF : (m + 1) * HALF] = dot(mperm[...], w_ref[m, :, QKV:]).astype(bf16)

    def body(w, carry):
        wrows = pl.ds(pl.multiple_of(w * WROW, WROW), WROW)
        wt = lax.rem(w, windows) if windows > 1 else 0
        for m in range(2):
            base = m * QKV
            q = qkv_ref[wrows, base : base + HALF]
            k = qkv_ref[wrows, base + HALF : base + 2 * HALF]
            v = qkv_ref[wrows, base + 2 * HALF : base + QKV]
            gm = gmw[wrows, m * HALF : (m + 1) * HALF]
            qx = expand_heads(q, hm_ref)
            gx = expand_heads(gm, hm_ref)
            pr = softmax_cols(k, qx, bias_ref[wt, m])
            dp = dot(v, gx, 1, 1)
            ds = pr * (dp - jnp.sum(pr * dp, 0, keepdims=True))
            ds_acc[m] += ds
            ds = ds.astype(bf16)
            gv = dot(pr.astype(bf16), gx)
            gk = dot(ds, qx) * score_scale
            gq = fold_heads(dot(ds, k, 0, 0)) * score_scale
            qv_acc[0:1, m * HALF : (m + 1) * HALF] += row_sum(gq)
            qv_acc[1:2, m * HALF : (m + 1) * HALF] += row_sum(gv)
            gqw[wrows, base : base + HALF] = gq.astype(bf16)
            gqw[wrows, base + HALF : base + 2 * HALF] = gk.astype(bf16)
            gqw[wrows, base + 2 * HALF : base + QKV] = gv.astype(bf16)
        return carry

    lax.fori_loop(0, 4 * PAIR, body, 0)
    gq = to_token_rows(perm_t_ref[...], gqw)
    gq_s[rows, :] = gq
    gnorm = dot(gq[:, :QKV], w_ref[0, :, :QKV], 1, 1) + dot(gq[:, QKV:], w_ref[1, :, :QKV], 1, 1)
    nv_acc[0:1, :] += row_sum(gnorm * hat)
    nv_acc[1:2, :] += row_sum(gnorm)
    return gmid + norm_back(gnorm, hat, inv, nv_ref[0:1, :])


def forward_kernel(first, last, windows, x_ref, wm_ref, wa_ref, bias_ref, qvb_ref, b1_ref, nv_ref,
                   perm_ref, perm_t_ref, hm_ref, y_ref, mid_ref, qkv_ref, mixed_ref, act_ref, slope_ref,
                   xs, nperm, mixw):
    if first:
        put_images(xs, x_ref)
        x = xs[...]
    else:
        x = x_ref[...]
    mid = attend_forward(x, wa_ref, bias_ref, qvb_ref, nv_ref, perm_ref, perm_t_ref, hm_ref,
                         qkv_ref, mixed_ref, nperm, mixw, windows)
    mid_ref[...] = mid
    y = mlp_forward(mid, wm_ref, b1_ref, nv_ref, act_ref, slope_ref)
    if last:
        for im in range(PAIR):
            y_ref[im] = y[im * SEQP : im * SEQP + SEQ]
    else:
        y_ref[...] = y


GW = 1024


def backward_kernel(first, last, windows, steps, g_ref, x_ref, mid_ref, wm_ref, wa_ref, bias_ref, nv_ref,
                    perm_ref, perm_t_ref, hm_ref, live_ref, qkv_ref, slope_ref, act_ref, mixed_ref,
                    gx_ref, gw_ref, qv_acc, b1_acc, ds_acc, nv_acc,
                    xs, gs, mperm, gmw, gqw, gp, gq_s, hid_s, gb_s, mb_s, nb_s):
    i = pl.program_id(0)

    @pl.when(i == 0)
    def _():
        for ref in (qv_acc, b1_acc, ds_acc, nv_acc):
            ref[...] = jnp.zeros_like(ref)

    @pl.when(i < steps)
    def _():
        rows = pl.ds(pl.multiple_of(i * ROWS, ROWS), ROWS)
        if last:
            for im in range(PAIR):
                flag = live_ref[im : im + 1, :]
                gs[im * SEQP : im * SEQP + SEQ, :] = g_ref[im] * jnp.concatenate([flag] * 4, 1)
                gs[im * SEQP + SEQ : (im + 1) * SEQP, :] = jnp.zeros((SEQP - SEQ, D), f32)
            gout = gs[...]
        else:
            gout = g_ref[...]
        if first:
            put_images(xs, x_ref)
            x = xs[...]
        else:
            x = x_ref[...]
        gmid = mlp_backward(gout, mid_ref[...], wm_ref, nv_ref, slope_ref, gp, hid_s, gb_s, rows, b1_acc, nv_acc)
        gin = attend_backward(gmid, x, wa_ref, bias_ref, nv_ref, perm_ref, perm_t_ref, hm_ref, qkv_ref,
                              mperm, gmw, gqw, gq_s, mb_s, nb_s, rows, ds_acc, qv_acc, nv_acc, windows)
        if first:
            for im in range(PAIR):
                gx_ref[im] = gin[im * SEQP : im * SEQP + SEQ]
        else:
            gx_ref[...] = gin

    for m in range(2):

        @pl.when(i == steps + 3 * m)
        def _():
            gw_ref[0] = dot(hid_s[...], gp[:, m * FFH : (m + 1) * FFH], 0, 0).astype(bf16)

        @pl.when(i == steps + 3 * m + 1)
        def _():
            gw_ref[0] = dot(gb_s[...], act_ref[:, m * FFH : (m + 1) * FFH], 0, 0).astype(bf16)

        @pl.when(i == steps + 3 * m + 2)
        def _():
            gw_ref[0, :, :QKV] = dot(nb_s[...], gq_s[:, m * QKV : (m + 1) * QKV], 0, 0).astype(bf16)
            gw_ref[0, :, QKV:] = dot(mb_s[...], mixed_ref[:, m * HALF : (m + 1) * HALF], 0, 0).astype(bf16)


def whole(shape, buffers=1):
    zero = (0,) * len(shape)
    return pl.BlockSpec(shape, lambda i: zero, pipeline_mode=pl.Buffered(buffers))


VLIM = 60 * 1024 * 1024


def forward_layer(layer, x, wg, bias, qvb, b1, nv, consts, steps):
    first, last = layer == 0, layer == LAYERS - 1
    shifted = layer % 2 == 1
    perm, perm_t, hm = consts
    nimg = steps * PAIR
    windows = bias.shape[0]
    img = lambda: pl.BlockSpec((PAIR, SEQ, D), lambda i: (i, 0, 0))
    row = lambda n: pl.BlockSpec((ROWS, n), lambda i: (i, 0))
    return pl.pallas_call(
        functools.partial(forward_kernel, first, last, windows),
        name=f"forward_{layer}",
        grid=(steps,),
        in_specs=[
            img() if first else row(D),
            pl.BlockSpec((2, D, ATT), lambda i: (0, 0, 0), pipeline_mode=pl.Buffered(1)),
            pl.BlockSpec((2, D, COLS - ATT), lambda i: (0, 0, ATT // (COLS - ATT)), pipeline_mode=pl.Buffered(1)),
            whole(bias.shape), whole(qvb.shape), whole(b1.shape), whole(nv.shape),
            whole(perm.shape), whole(perm_t.shape), whole(hm.shape),
        ],
        out_specs=[
            img() if last else row(D), row(D),
            pl.BlockSpec((WPAIR, 2 * QKV), lambda i: (i, 0)), row(D), row(2 * FFH), row(2 * FFH),
        ],
        out_shape=[
            jax.ShapeDtypeStruct((nimg, SEQ, D) if last else (nimg * SEQP, D), f32),
            jax.ShapeDtypeStruct((nimg * SEQP, D), f32),
            jax.ShapeDtypeStruct((steps * WPAIR, 2 * QKV), bf16),
            jax.ShapeDtypeStruct((nimg * SEQP, D), bf16),
            jax.ShapeDtypeStruct((nimg * SEQP, 2 * FFH), bf16),
            jax.ShapeDtypeStruct((nimg * SEQP, 2 * FFH), bf16),
        ],
        scratch_shapes=[
            pltpu.VMEM((ROWS, D), f32), pltpu.VMEM((WPAIR, D), bf16), pltpu.VMEM((WPAIR, D), bf16),
        ],
        compiler_params=pltpu.CompilerParams(vmem_limit_bytes=VLIM),
    )(x, wg, wg, bias, qvb, b1, nv, perm, perm_t, hm)


def backward_layer(layer, grad, x, saved, wg, bias, nv, consts, live, steps):
    first, last = layer == 0, layer == LAYERS - 1
    perm, perm_t, hm = consts
    mid, qkv, mixed, act, slope = saved
    nimg = steps * PAIR
    windows = bias.shape[0]
    top = steps - 1
    img = lambda: pl.BlockSpec((PAIR, SEQ, D), lambda i: (jnp.minimum(i, top), 0, 0))
    row = lambda n: pl.BlockSpec((ROWS, n), lambda i: (jnp.minimum(i, top), 0))
    total = nimg * SEQP

    def gmap(i):
        k = jnp.maximum(i - steps, 0)
        return (k // 3, 0, lax.rem(k, 3))

    return pl.pallas_call(
        functools.partial(backward_kernel, first, last, windows, steps),
        name=f"backward_{layer}",
        grid=(steps + 6,),
        in_specs=[
            img() if last else row(D), img() if first else row(D), row(D),
            pl.BlockSpec((2, D, ATT), lambda i: (0, 0, 0), pipeline_mode=pl.Buffered(1)),
            pl.BlockSpec((2, D, COLS - ATT), lambda i: (0, 0, ATT // (COLS - ATT)), pipeline_mode=pl.Buffered(1)),
            whole(bias.shape), whole(nv.shape), whole(perm.shape), whole(perm_t.shape), whole(hm.shape),
            pl.BlockSpec((None, PAIR, 128), lambda i: (jnp.minimum(i, top), 0, 0)),
            pl.BlockSpec((WPAIR, 2 * QKV), lambda i: (jnp.minimum(i, top), 0)), row(2 * FFH),
            whole(act.shape), whole(mixed.shape),
        ],
        out_specs=[
            img() if first else row(D),
            pl.BlockSpec((1, D, GW), gmap),
            whole((2, 2 * HALF)), whole((1, 2 * FFH)), whole((2, WROW, LANES)), whole((8, D)),
        ],
        out_shape=[
            jax.ShapeDtypeStruct((nimg, SEQ, D) if first else (total, D), f32),
            jax.ShapeDtypeStruct((2, D, COLS), bf16),
            jax.ShapeDtypeStruct((2, 2 * HALF), f32),
            jax.ShapeDtypeStruct((1, 2 * FFH), f32),
            jax.ShapeDtypeStruct((2, WROW, LANES), f32),
            jax.ShapeDtypeStruct((8, D), f32),
        ],
        scratch_shapes=[
            pltpu.VMEM((ROWS, D), f32), pltpu.VMEM((ROWS, D), f32),
            pltpu.VMEM((WPAIR, D), bf16), pltpu.VMEM((WPAIR, D), bf16), pltpu.VMEM((WPAIR, 2 * QKV), bf16),
            pltpu.VMEM((total, 2 * FFH), bf16), pltpu.VMEM((total, 2 * QKV), bf16),
            pltpu.VMEM((total, D), bf16), pltpu.VMEM((total, D), bf16),
            pltpu.VMEM((total, D), bf16), pltpu.VMEM((total, D), bf16),
        ],
        compiler_params=pltpu.CompilerParams(vmem_limit_bytes=VLIM),
    )(grad, x, mid, wg, wg, bias, nv, perm, perm_t, hm, live, qkv, slope, act, mixed)


def head_mask():
    return (np.arange(HALF)[None, :] // HD == np.arange(GROUP)[:, None]).astype(np.float32)


def bias_cols(onehot, table, shifted):
    picked = jnp.dot(table.T, onehot, precision=lax.Precision.HIGHEST).reshape(2, GROUP, WSEQ, WSEQ)
    by_j = picked.transpose(0, 3, 1, 2)
    by_j = jnp.pad(by_j, ((0, 0), (0, 0), (0, 0), (0, WROW - WSEQ)))
    by_j = jnp.pad(by_j, ((0, 0), (0, WROW - WSEQ), (0, 0), (0, 0)), constant_values=pad_fill)
    if shifted:
        by_j = by_j[None] + jnp.asarray(region_mask())[:, None, :, None, :]
    else:
        by_j = by_j[None]
    return by_j.reshape(-1, 2, WROW, LANES)


def adam_update(weight_in, moment_one, moment_two, grad_sum, decay):
    new_one = beta_one * moment_one + (1.0 - beta_one) * grad_sum
    new_two = beta_two * moment_two + (1.0 - beta_two) * grad_sum * grad_sum
    hat_one = new_one / (1.0 - beta_one**adam_step)
    hat_two = new_two / (1.0 - beta_two**adam_step)
    new_weight = weight_in - learn_rate * (hat_one / (jnp.sqrt(hat_two) + adam_eps) + decay * weight_in)
    return (new_weight, new_one, new_two)


def both_halves(mine, me):
    other = lax.ppermute(mine, "mp", [(0, 1), (1, 0)])
    low = jnp.where(me == 0, mine, other)
    high = jnp.where(me == 0, other, mine)
    return jnp.concatenate([low, high], 0)


def local(
    tokens, cotangent, image_count, rel_index,
    w_qkv, w_proj, w_fc_one, w_fc_two, qv_bias, fc_one_bias, rel_table, norm_vec,
    m_qkv, m_proj, m_fc_one, m_fc_two, m_qv_bias, m_fc_one_bias, m_rel_table, m_norm_vec,
    v_qkv, v_proj, v_fc_one, v_fc_two, v_qv_bias, v_fc_one_bias, v_rel_table, v_norm_vec,
):
    me = lax.axis_index("mp")
    images = tokens.shape[0]
    nimg = images // 2
    steps = nimg // PAIR
    part = w_qkv.shape[1]
    tok = lax.dynamic_slice_in_dim(tokens, me * nimg, nimg, 0)
    cot = lax.dynamic_slice_in_dim(cotangent, me * nimg, nimg, 0)
    live = (jnp.arange(nimg, dtype=jnp.int32) + me * nimg < image_count[0]).astype(f32)
    live = jnp.broadcast_to(live[:, None], (nimg, 128)).reshape(steps, PAIR, 128)

    packed = jnp.concatenate(
        [w_fc_one, w_fc_two.transpose(0, 2, 1), w_qkv.reshape(LAYERS, part, QKV), w_proj.transpose(0, 2, 1)], 2
    ).astype(bf16)
    gathered = lax.all_gather(packed, ("mp", "dp"))
    small = jnp.concatenate(
        [qv_bias.reshape(LAYERS, -1), fc_one_bias, rel_table.reshape(LAYERS, -1)], 1
    )
    small = lax.all_gather(small, "mp")
    qvb = small[:, :, : 2 * HALF].reshape(2, LAYERS, 2, HALF)
    b1 = small[:, :, 2 * HALF : 2 * HALF + FFH].transpose(1, 0, 2).reshape(LAYERS, 1, 2 * FFH)
    table = small[:, :, 2 * HALF + FFH :].reshape(2, LAYERS, TABLE, GROUP).transpose(1, 2, 0, 3)
    table = table.reshape(LAYERS, TABLE, 2 * GROUP)
    qvb = jnp.concatenate([qvb[:, :, 0], jnp.zeros_like(qvb[:, :, 0]), qvb[:, :, 1]], 2)

    onehot = (rel_index.reshape(1, WSEQ * WSEQ) == jnp.arange(TABLE, dtype=jnp.int32)[:, None]).astype(f32)
    hm = jnp.asarray(head_mask(), bf16)
    x, xs, saved, ctx = tok, [], [], []
    for layer in range(LAYERS):
        shifted = layer % 2 == 1

        wg = gathered.reshape(2, -1, LAYERS, part, COLS)[:, :, layer]
        wg = wg.reshape(2, D, COLS)
        bias = bias_cols(onehot, table[layer], shifted)
        p = permutation(shifted)
        consts = (jnp.asarray(p, bf16), jnp.asarray(p.T, bf16), hm)
        ctx.append((wg, bias, consts))
        xs.append(x)
        x, *kept = forward_layer(layer, x, wg, bias, qvb[:, layer], b1[layer], norm_vec[layer], consts, steps)
        saved.append(kept)
    out = both_halves(x, me)
    g = cot
    big, little = [None] * LAYERS, [None] * LAYERS
    for layer in reversed(range(LAYERS)):
        wg, bias, consts = ctx[layer]
        g, gw, gqv, gb1, ds, gnv = backward_layer(
            layer, g, xs[layer], saved[layer], wg, bias, norm_vec[layer], consts, live, steps
        )
        mine = lax.dynamic_index_in_dim(gw, me, 0, keepdims=False)
        other = lax.ppermute(lax.dynamic_index_in_dim(gw, 1 - me, 0, keepdims=False), "mp", [(0, 1), (1, 0)])
        total = (mine.astype(f32) + other.astype(f32)).astype(bf16)
        big[layer] = lax.psum_scatter(total, "dp", scatter_dimension=0, tiled=True).astype(f32)
        ds = ds.reshape(2, WROW, GROUP, WROW)[:, :WSEQ, :, :WSEQ].transpose(0, 2, 3, 1)
        gt = jnp.dot(ds.reshape(2 * GROUP, WSEQ * WSEQ), onehot.T, precision=lax.Precision.HIGHEST)
        little[layer] = jnp.concatenate([gqv.reshape(-1), gb1.reshape(-1), gt.reshape(-1), gnv[:6].reshape(-1)])
    x_grad = both_halves(g, me)
    little = lax.psum(jnp.stack(little), ("dp", "mp"))
    big = jnp.stack(big)
    one_grad = big[:, :, :FFH]
    two_grad = big[:, :, FFH:ATT].transpose(0, 2, 1)
    qkv_grad = big[:, :, ATT : ATT + QKV].reshape(LAYERS, part, 3, HALF)
    proj_grad = big[:, :, ATT + QKV :].transpose(0, 2, 1)
    cut = lambda a: lax.dynamic_index_in_dim(a, me, 1, keepdims=False)
    at = 2 * 2 * HALF
    qv_grad = cut(little[:, :at].reshape(LAYERS, 2, 2, HALF).transpose(0, 2, 1, 3))
    bias_grad = cut(little[:, at : at + 2 * FFH].reshape(LAYERS, 2, FFH))
    at += 2 * FFH
    table_grad = cut(little[:, at : at + 2 * GROUP * TABLE].reshape(LAYERS, 2, GROUP, TABLE)).transpose(0, 2, 1)
    at += 2 * GROUP * TABLE
    norm_grad = little[:, at:].reshape(LAYERS, 6, D)
    groups = [
        adam_update(w_qkv, m_qkv, v_qkv, qkv_grad, decay_rate),
        adam_update(w_proj, m_proj, v_proj, proj_grad, decay_rate),
        adam_update(w_fc_one, m_fc_one, v_fc_one, one_grad, decay_rate),
        adam_update(w_fc_two, m_fc_two, v_fc_two, two_grad, decay_rate),
        adam_update(qv_bias, m_qv_bias, v_qv_bias, qv_grad, 0.0),
        adam_update(fc_one_bias, m_fc_one_bias, v_fc_one_bias, bias_grad, 0.0),
        adam_update(rel_table, m_rel_table, v_rel_table, table_grad, 0.0),
        adam_update(norm_vec, m_norm_vec, v_norm_vec, norm_grad, 0.0),
    ]
    return (out, x_grad, *[grp[k] for k in range(3) for grp in groups])


def solution(mesh):
    params = (
        P(None, "dp", None, "mp"), P(None, "mp", "dp"), P(None, "dp", "mp"), P(None, "mp", "dp"),
        P(None, None, "mp"), P(None, "mp"), P(None, None, "mp"), P(),
    )
    act = (P("dp", None, None), P("dp", None, None))
    return jax.shard_map(
        local,
        mesh=mesh,
        in_specs=(*act, P("dp"), P(), *params, *params, *params),
        out_specs=(*act, *params, *params, *params),
        check_vma=False,
    )
```

```python
import functools

import jax
import jax.numpy as jnp
import numpy as np
from jax import lax
from jax.experimental import pallas as pl
from jax.experimental.pallas import tpu as pltpu
from jax.sharding import PartitionSpec as P

D = 512
HD = 32
SIDE = 14
WIN = 7
SHIFT = 3
SEQ = 196
WSEQ = 49
TABLE = 169
LAYERS = 2
SEQP = 200
PAIR = 2
ROWS = PAIR * SEQP
WROW = 64
WIMG = 4 * WROW
WPAIR = PAIR * WIMG
HALF = 256
GROUP = 8
LANES = GROUP * WROW
FFH = 1024
QKV = 3 * HALF
COLS = 2 * FFH + QKV + HALF
ATT = 2 * FFH

norm_eps = 1e-05
mask_fill = -100.0
pad_fill = -1e30
beta_one = 0.9
beta_two = 0.999
adam_eps = 1e-08
learn_rate = 0.02
decay_rate = 0.05
adam_step = 3.0
root_half = 0.7071067811865476
inv_root_two_pi = 0.3989422804014327
score_scale = HD**-0.5

f32 = jnp.float32
bf16 = jnp.bfloat16


def dot(a, b, ca=1, cb=0):
    return lax.dot_general(a, b, (((ca,), (cb,)), ((), ())), preferred_element_type=f32)


def window_tokens(shifted):
    off = SHIFT if shifted else 0
    out = np.zeros((4, WSEQ), np.int64)
    for wr in range(2):
        for wc in range(2):
            for p in range(WSEQ):
                r = (7 * wr + p // 7 + off) % SIDE
                c = (7 * wc + p % 7 + off) % SIDE
                out[wr * 2 + wc, p] = r * SIDE + c
    return out


def permutation(shifted):
    tok = window_tokens(shifted)
    perm = np.zeros((WIMG, SEQP), np.float32)
    for w in range(4):
        perm[w * WROW + np.arange(WSEQ), tok[w]] = 1.0
    return perm


def region_mask():
    pos = np.arange(SIDE)
    band = (pos >= SIDE - WIN).astype(int) + (pos >= SIDE - SHIFT).astype(int)
    region = 3 * band[:, None] + band[None, :]
    win = region.reshape(2, WIN, 2, WIN).transpose(0, 2, 1, 3).reshape(4, WSEQ)
    out = np.zeros((4, WROW, WROW), np.float32)
    out[:, :WSEQ, :WSEQ] = np.where(win[:, :, None] != win[:, None, :], mask_fill, 0.0)
    return out


def norm_stats(z):
    mean = jnp.mean(z, -1, keepdims=True)
    cen = z - mean
    var = jnp.mean(cen * cen, -1, keepdims=True)
    inv = lax.rsqrt(var + norm_eps)
    return cen * inv, inv


def norm_back(e, hat, inv, gain):
    s = e * gain
    return inv * (s - jnp.mean(s, -1, keepdims=True) - hat * jnp.mean(s * hat, -1, keepdims=True))


def row_sum(v):
    return jnp.sum(v, 0, keepdims=True)


def put_images(ref, blk):
    for im in range(PAIR):
        ref[im * SEQP : im * SEQP + SEQ, :] = blk[im].astype(f32)
        ref[im * SEQP + SEQ : (im + 1) * SEQP, :] = jnp.zeros((SEQP - SEQ, D), f32)


def to_window_rows(perm, rows, out_ref):
    for im in range(PAIR):
        part = rows[im * SEQP : (im + 1) * SEQP].astype(bf16)
        out_ref[im * WIMG : (im + 1) * WIMG, :] = dot(perm, part).astype(bf16)


def to_token_rows(perm_t, ref):
    return jnp.concatenate(
        [dot(perm_t, ref[im * WIMG : (im + 1) * WIMG, :]) for im in range(PAIR)], 0
    ).astype(bf16)


def expand_heads(x, hm_ref):
    return jnp.concatenate([x * hm_ref[h : h + 1, :] for h in range(GROUP)], 0)


def fold_heads(o):
    lane = lax.broadcasted_iota(jnp.int32, (WROW, HALF), 1) // HD
    acc = o[:WROW]
    for h in range(1, GROUP):
        acc = jnp.where(lane == h, o[h * WROW : (h + 1) * WROW], acc)
    return acc


def softmax_cols(k, qx, bias):
    s = dot(k, qx, 1, 1) * score_scale + bias
    e = jnp.exp(s - jnp.max(s, 0, keepdims=True))
    return e * (1.0 / jnp.sum(e, 0, keepdims=True))


def attend_forward(x, w_ref, bias_ref, qvb_ref, nv_ref, perm_ref, perm_t_ref, hm_ref,
                   qkv_ref, mixed_ref, nperm, mixw, windows):
    hat, _ = norm_stats(x)
    normed = hat * nv_ref[0:1, :] + nv_ref[1:2, :]
    to_window_rows(perm_ref[...], normed, nperm)
    for m in range(2):
        r = dot(nperm[...], w_ref[m, :, :QKV])
        qkv_ref[:, m * QKV : (m + 1) * QKV] = (r + qvb_ref[m : m + 1, :]).astype(bf16)

    def body(w, carry):
        rows = pl.ds(pl.multiple_of(w * WROW, WROW), WROW)
        wt = lax.rem(w, windows) if windows > 1 else 0
        for m in range(2):
            base = m * QKV
            q = qkv_ref[rows, base : base + HALF]
            k = qkv_ref[rows, base + HALF : base + 2 * HALF]
            v = qkv_ref[rows, base + 2 * HALF : base + QKV]
            pr = softmax_cols(k, expand_heads(q, hm_ref), bias_ref[wt, m])
            o = dot(pr.astype(bf16), v, 0, 0)
            mixw[rows, m * HALF : (m + 1) * HALF] = fold_heads(o).astype(bf16)
        return carry

    lax.fori_loop(0, 4 * PAIR, body, 0)
    mixed = to_token_rows(perm_t_ref[...], mixw)
    mixed_ref[...] = mixed
    attn = dot(mixed[:, :HALF], w_ref[0, :, QKV:], 1, 1) + dot(mixed[:, HALF:], w_ref[1, :, QKV:], 1, 1)
    return x + attn + nv_ref[4:5, :]


CH = 512


def mlp_forward(mid, w_ref, b1_ref, nv_ref, act_ref, slope_ref):
    hat, _ = norm_stats(mid)
    hid = (hat * nv_ref[2:3, :] + nv_ref[3:4, :]).astype(bf16)
    total = jnp.zeros((ROWS, D), f32)
    for m in range(2):
        for c in range(0, FFH, CH):
            col = m * FFH + c
            u = dot(hid, w_ref[m, :, c : c + CH]) + b1_ref[:, col : col + CH]
            phi = 0.5 + 0.5 * lax.erf(u * root_half)
            act = (u * phi).astype(bf16)
            act_ref[:, col : col + CH] = act
            slope_ref[:, col : col + CH] = (phi + u * jnp.exp(-0.5 * u * u) * inv_root_two_pi).astype(bf16)
            total += dot(act, w_ref[m, :, FFH + c : FFH + c + CH], 1, 1)
    return mid + total + nv_ref[5:6, :]


def mlp_backward(gout, mid, w_ref, nv_ref, slope_ref, gp, hid_s, gb_s, rows, b1_acc, nv_acc):
    hat, inv = norm_stats(mid)
    hid_s[rows, :] = (hat * nv_ref[2:3, :] + nv_ref[3:4, :]).astype(bf16)
    gb = gout.astype(bf16)
    gb_s[rows, :] = gb
    ghid = jnp.zeros((ROWS, D), f32)
    for m in range(2):
        for c in range(0, FFH, CH):
            col = m * FFH + c
            g = dot(gb, w_ref[m, :, FFH + c : FFH + c + CH]) * slope_ref[:, col : col + CH].astype(f32)
            b1_acc[:, col : col + CH] += row_sum(g)
            g = g.astype(bf16)
            gp[rows, col : col + CH] = g
            ghid += dot(g, w_ref[m, :, c : c + CH], 1, 1)
    gmid = gout + norm_back(ghid, hat, inv, nv_ref[2:3, :])
    nv_acc[2:3, :] += row_sum(ghid * hat)
    nv_acc[3:4, :] += row_sum(ghid)
    nv_acc[4:5, :] += row_sum(gmid)
    nv_acc[5:6, :] += row_sum(gout)
    return gmid


def attend_backward(gmid, x, w_ref, bias_ref, nv_ref, perm_ref, perm_t_ref, hm_ref, qkv_ref,
                    mperm, gmw, gqw, gq_s, mb_s, nb_s, rows, ds_acc, qv_acc, nv_acc, windows):
    hat, inv = norm_stats(x)
    nb_s[rows, :] = (hat * nv_ref[0:1, :] + nv_ref[1:2, :]).astype(bf16)
    mb_s[rows, :] = gmid.astype(bf16)
    to_window_rows(perm_ref[...], gmid, mperm)
    for m in range(2):
        gmw[:, m * HALF : (m + 1) * HALF] = dot(mperm[...], w_ref[m, :, QKV:]).astype(bf16)

    def body(w, carry):
        wrows = pl.ds(pl.multiple_of(w * WROW, WROW), WROW)
        wt = lax.rem(w, windows) if windows > 1 else 0
        for m in range(2):
            base = m * QKV
            q = qkv_ref[wrows, base : base + HALF]
            k = qkv_ref[wrows, base + HALF : base + 2 * HALF]
            v = qkv_ref[wrows, base + 2 * HALF : base + QKV]
            gm = gmw[wrows, m * HALF : (m + 1) * HALF]
            qx = expand_heads(q, hm_ref)
            gx = expand_heads(gm, hm_ref)
            pr = softmax_cols(k, qx, bias_ref[wt, m])
            dp = dot(v, gx, 1, 1)
            ds = pr * (dp - jnp.sum(pr * dp, 0, keepdims=True))
            ds_acc[m] += ds
            ds = ds.astype(bf16)
            gv = dot(pr.astype(bf16), gx)
            gk = dot(ds, qx) * score_scale
            gq = fold_heads(dot(ds, k, 0, 0)) * score_scale
            qv_acc[0:1, m * HALF : (m + 1) * HALF] += row_sum(gq)
            qv_acc[1:2, m * HALF : (m + 1) * HALF] += row_sum(gv)
            gqw[wrows, base : base + HALF] = gq.astype(bf16)
            gqw[wrows, base + HALF : base + 2 * HALF] = gk.astype(bf16)
            gqw[wrows, base + 2 * HALF : base + QKV] = gv.astype(bf16)
        return carry

    lax.fori_loop(0, 4 * PAIR, body, 0)
    gq = to_token_rows(perm_t_ref[...], gqw)
    gq_s[rows, :] = gq
    gnorm = dot(gq[:, :QKV], w_ref[0, :, :QKV], 1, 1) + dot(gq[:, QKV:], w_ref[1, :, :QKV], 1, 1)
    nv_acc[0:1, :] += row_sum(gnorm * hat)
    nv_acc[1:2, :] += row_sum(gnorm)
    return gmid + norm_back(gnorm, hat, inv, nv_ref[0:1, :])


def forward_kernel(first, last, windows, x_ref, wm_ref, wa_ref, bias_ref, qvb_ref, b1_ref, nv_ref,
                   perm_ref, perm_t_ref, hm_ref, y_ref, mid_ref, qkv_ref, mixed_ref, act_ref, slope_ref,
                   xs, nperm, mixw):
    if first:
        put_images(xs, x_ref)
        x = xs[...]
    else:
        x = x_ref[...]
    mid = attend_forward(x, wa_ref, bias_ref, qvb_ref, nv_ref, perm_ref, perm_t_ref, hm_ref,
                         qkv_ref, mixed_ref, nperm, mixw, windows)
    mid_ref[...] = mid
    y = mlp_forward(mid, wm_ref, b1_ref, nv_ref, act_ref, slope_ref)
    if last:
        for im in range(PAIR):
            y_ref[im] = y[im * SEQP : im * SEQP + SEQ]
    else:
        y_ref[...] = y


GW = 1024


def backward_kernel(first, last, windows, steps, g_ref, x_ref, mid_ref, wm_ref, wa_ref, bias_ref, nv_ref,
                    perm_ref, perm_t_ref, hm_ref, live_ref, qkv_ref, slope_ref, act_ref, mixed_ref,
                    gx_ref, gw_ref, qv_acc, b1_acc, ds_acc, nv_acc,
                    xs, gs, mperm, gmw, gqw, gp, gq_s, hid_s, gb_s, mb_s, nb_s):
    i = pl.program_id(0)

    @pl.when(i == 0)
    def _():
        for ref in (qv_acc, b1_acc, ds_acc, nv_acc):
            ref[...] = jnp.zeros_like(ref)

    @pl.when(i < steps)
    def _():
        rows = pl.ds(pl.multiple_of(i * ROWS, ROWS), ROWS)
        if last:
            for im in range(PAIR):
                flag = live_ref[im : im + 1, :]
                gs[im * SEQP : im * SEQP + SEQ, :] = g_ref[im] * jnp.concatenate([flag] * 4, 1)
                gs[im * SEQP + SEQ : (im + 1) * SEQP, :] = jnp.zeros((SEQP - SEQ, D), f32)
            gout = gs[...]
        else:
            gout = g_ref[...]
        if first:
            put_images(xs, x_ref)
            x = xs[...]
        else:
            x = x_ref[...]
        gmid = mlp_backward(gout, mid_ref[...], wm_ref, nv_ref, slope_ref, gp, hid_s, gb_s, rows, b1_acc, nv_acc)
        gin = attend_backward(gmid, x, wa_ref, bias_ref, nv_ref, perm_ref, perm_t_ref, hm_ref, qkv_ref,
                              mperm, gmw, gqw, gq_s, mb_s, nb_s, rows, ds_acc, qv_acc, nv_acc, windows)
        if first:
            for im in range(PAIR):
                gx_ref[im] = gin[im * SEQP : im * SEQP + SEQ]
        else:
            gx_ref[...] = gin

    for m in range(2):

        @pl.when(i == steps + 3 * m)
        def _():
            gw_ref[0] = dot(hid_s[...], gp[:, m * FFH : (m + 1) * FFH], 0, 0).astype(bf16)

        @pl.when(i == steps + 3 * m + 1)
        def _():
            gw_ref[0] = dot(gb_s[...], act_ref[:, m * FFH : (m + 1) * FFH], 0, 0).astype(bf16)

        @pl.when(i == steps + 3 * m + 2)
        def _():
            gw_ref[0, :, :QKV] = dot(nb_s[...], gq_s[:, m * QKV : (m + 1) * QKV], 0, 0).astype(bf16)
            gw_ref[0, :, QKV:] = dot(mb_s[...], mixed_ref[:, m * HALF : (m + 1) * HALF], 0, 0).astype(bf16)


def whole(shape, buffers=1):
    zero = (0,) * len(shape)
    return pl.BlockSpec(shape, lambda i: zero, pipeline_mode=pl.Buffered(buffers))


VLIM = 60 * 1024 * 1024


def forward_layer(layer, x, wg, bias, qvb, b1, nv, consts, steps):
    first, last = layer == 0, layer == LAYERS - 1
    shifted = layer % 2 == 1
    perm, perm_t, hm = consts
    nimg = steps * PAIR
    windows = bias.shape[0]
    img = lambda: pl.BlockSpec((PAIR, SEQ, D), lambda i: (i, 0, 0))
    row = lambda n: pl.BlockSpec((ROWS, n), lambda i: (i, 0))
    return pl.pallas_call(
        functools.partial(forward_kernel, first, last, windows),
        name=f"forward_{layer}",
        grid=(steps,),
        in_specs=[
            img() if first else row(D),
            pl.BlockSpec((2, D, ATT), lambda i: (0, 0, 0), pipeline_mode=pl.Buffered(1)),
            pl.BlockSpec((2, D, COLS - ATT), lambda i: (0, 0, ATT // (COLS - ATT)), pipeline_mode=pl.Buffered(1)),
            whole(bias.shape), whole(qvb.shape), whole(b1.shape), whole(nv.shape),
            whole(perm.shape), whole(perm_t.shape), whole(hm.shape),
        ],
        out_specs=[
            img() if last else row(D), row(D),
            pl.BlockSpec((WPAIR, 2 * QKV), lambda i: (i, 0)), row(D), row(2 * FFH), row(2 * FFH),
        ],
        out_shape=[
            jax.ShapeDtypeStruct((nimg, SEQ, D) if last else (nimg * SEQP, D), f32),
            jax.ShapeDtypeStruct((nimg * SEQP, D), f32),
            jax.ShapeDtypeStruct((steps * WPAIR, 2 * QKV), bf16),
            jax.ShapeDtypeStruct((nimg * SEQP, D), bf16),
            jax.ShapeDtypeStruct((nimg * SEQP, 2 * FFH), bf16),
            jax.ShapeDtypeStruct((nimg * SEQP, 2 * FFH), bf16),
        ],
        scratch_shapes=[
            pltpu.VMEM((ROWS, D), f32), pltpu.VMEM((WPAIR, D), bf16), pltpu.VMEM((WPAIR, D), bf16),
        ],
        compiler_params=pltpu.CompilerParams(vmem_limit_bytes=VLIM),
    )(x, wg, wg, bias, qvb, b1, nv, perm, perm_t, hm)


def backward_layer(layer, grad, x, saved, wg, bias, nv, consts, live, steps):
    first, last = layer == 0, layer == LAYERS - 1
    perm, perm_t, hm = consts
    mid, qkv, mixed, act, slope = saved
    nimg = steps * PAIR
    windows = bias.shape[0]
    top = steps - 1
    img = lambda: pl.BlockSpec((PAIR, SEQ, D), lambda i: (jnp.minimum(i, top), 0, 0))
    row = lambda n: pl.BlockSpec((ROWS, n), lambda i: (jnp.minimum(i, top), 0))
    total = nimg * SEQP

    def gmap(i):
        k = jnp.maximum(i - steps, 0)
        return (k // 3, 0, lax.rem(k, 3))

    return pl.pallas_call(
        functools.partial(backward_kernel, first, last, windows, steps),
        name=f"backward_{layer}",
        grid=(steps + 6,),
        in_specs=[
            img() if last else row(D), img() if first else row(D), row(D),
            pl.BlockSpec((2, D, ATT), lambda i: (0, 0, 0), pipeline_mode=pl.Buffered(1)),
            pl.BlockSpec((2, D, COLS - ATT), lambda i: (0, 0, ATT // (COLS - ATT)), pipeline_mode=pl.Buffered(1)),
            whole(bias.shape), whole(nv.shape), whole(perm.shape), whole(perm_t.shape), whole(hm.shape),
            pl.BlockSpec((None, PAIR, 128), lambda i: (jnp.minimum(i, top), 0, 0)),
            pl.BlockSpec((WPAIR, 2 * QKV), lambda i: (jnp.minimum(i, top), 0)), row(2 * FFH),
            whole(act.shape), whole(mixed.shape),
        ],
        out_specs=[
            img() if first else row(D),
            pl.BlockSpec((1, D, GW), gmap),
            whole((2, 2 * HALF)), whole((1, 2 * FFH)), whole((2, WROW, LANES)), whole((8, D)),
        ],
        out_shape=[
            jax.ShapeDtypeStruct((nimg, SEQ, D) if first else (total, D), f32),
            jax.ShapeDtypeStruct((2, D, COLS), bf16),
            jax.ShapeDtypeStruct((2, 2 * HALF), f32),
            jax.ShapeDtypeStruct((1, 2 * FFH), f32),
            jax.ShapeDtypeStruct((2, WROW, LANES), f32),
            jax.ShapeDtypeStruct((8, D), f32),
        ],
        scratch_shapes=[
            pltpu.VMEM((ROWS, D), f32), pltpu.VMEM((ROWS, D), f32),
            pltpu.VMEM((WPAIR, D), bf16), pltpu.VMEM((WPAIR, D), bf16), pltpu.VMEM((WPAIR, 2 * QKV), bf16),
            pltpu.VMEM((total, 2 * FFH), bf16), pltpu.VMEM((total, 2 * QKV), bf16),
            pltpu.VMEM((total, D), bf16), pltpu.VMEM((total, D), bf16),
            pltpu.VMEM((total, D), bf16), pltpu.VMEM((total, D), bf16),
        ],
        compiler_params=pltpu.CompilerParams(vmem_limit_bytes=VLIM),
    )(grad, x, mid, wg, wg, bias, nv, perm, perm_t, hm, live, qkv, slope, act, mixed)


def head_mask():
    return (np.arange(HALF)[None, :] // HD == np.arange(GROUP)[:, None]).astype(np.float32)


def bias_cols(onehot, table, shifted):
    picked = jnp.dot(table.T, onehot, precision=lax.Precision.HIGHEST).reshape(2, GROUP, WSEQ, WSEQ)
    by_j = picked.transpose(0, 3, 1, 2)
    by_j = jnp.pad(by_j, ((0, 0), (0, 0), (0, 0), (0, WROW - WSEQ)))
    by_j = jnp.pad(by_j, ((0, 0), (0, WROW - WSEQ), (0, 0), (0, 0)), constant_values=pad_fill)
    if shifted:
        by_j = by_j[None] + jnp.asarray(region_mask())[:, None, :, None, :]
    else:
        by_j = by_j[None]
    return by_j.reshape(-1, 2, WROW, LANES)

NZ, NY, NX = 4, 2, 2
PEERS = NZ * NY * NX
MESH_ID = pl.DeviceIdType.MESH


class Place:
    def __init__(self):
        d = lax.axis_index("dp")
        self.d, self.m = d, lax.axis_index("mp")
        self.z, self.y, self.x = d // 4, lax.rem(d // 2, 2), lax.rem(d, 2)

    def chip(self, z, y, x):
        return (z * NY + y) * NX + x

    def at(self, dz=0, y=None, x=None, m=None):
        y = self.y if y is None else y
        x = self.x if x is None else x
        return (self.chip(self.z + dz, y, x), self.m if m is None else m)

    def xn(self):
        return self.at(x=1 - self.x)

    def yn(self):
        return self.at(y=1 - self.y)

    def core(self):
        return self.at(m=1 - self.m)

    def zn(self, step):
        return self.at(dz=step)

    def has(self, step):
        return self.z < NZ - 1 if step > 0 else self.z > 0


def remote(src, dst, send, recv, to):
    return pltpu.make_async_remote_copy(
        src_ref=src, dst_ref=dst, send_sem=send, recv_sem=recv, device_id=to, device_id_type=MESH_ID
    )


def neighbour_barrier(p, far=False):
    sem = pltpu.get_barrier_semaphore()

    def tell(to):
        pl.semaphore_signal(sem, inc=1, device_id=to, device_id_type=MESH_ID)

    for to in (p.xn(), p.yn(), p.core()):
        tell(to)
    count = 3
    for step in (1, -1):
        pl.when(p.has(step))(lambda step=step: tell(p.zn(step)))
        count = count + p.has(step).astype(jnp.int32)
    if far:
        tell((p.chip((p.z + 2) % NZ, p.y, p.x), p.m))
        count = count + 1
    pl.semaphore_wait(sem, count)


class Gather:
    SEMS = 52
    BASE = {"z": 0, "xa": 8, "yb": 12, "ya0": 16, "ya1": 20, "xb0": 24, "xb1": 28,
            "own": 32, "ax": 36, "by": 40, "ar": 44, "br": 48}

    def __init__(self, own, full, send, recv, local, lo, hi):
        self.p, self.own, self.full = Place(), own, full
        self.send, self.recv, self.local = send, recv, local
        mid = (lo + hi) // 2
        self.all, self.a, self.b = pl.ds(lo, hi - lo), pl.ds(lo, mid - lo), pl.ds(mid, hi - mid)

    def region(self, kind, k, arrived):
        p = self.p
        oy, ox = 1 - p.y, 1 - p.x
        if kind == "z":
            return (p.m, k, p.y, p.x), self.all, None
        if kind == "xa":
            return (p.m, k, p.y, ox if arrived else p.x), self.a, p.xn()
        if kind == "yb":
            return (p.m, k, oy if arrived else p.y, p.x), self.b, p.yn()
        if kind in ("ya0", "ya1"):
            return (p.m, k, oy if arrived else p.y, p.x if kind == "ya0" else ox), self.a, p.yn()
        if kind in ("xb0", "xb1"):
            return (p.m, k, p.y if kind == "xb0" else oy, ox if arrived else p.x), self.b, p.xn()
        m = 1 - p.m if arrived else p.m
        if kind == "own":
            return (m, k, p.y, p.x), self.all, p.core()
        if kind == "ax":
            return (m, k, p.y, ox), self.a, p.core()
        if kind == "by":
            return (m, k, oy, p.x), self.b, p.core()
        if kind == "ar":
            return (m, k, oy, slice(None)), self.a, p.core()
        return (m, k, slice(None), ox), self.b, p.core()

    def copy(self, kind, k, own=False, arrived=False, step=0):
        at, cols, to = self.region(kind, k, arrived)
        dst = self.full.at[(*at, slice(None), cols)]
        src = self.own.at[:, cols] if own else dst
        s = self.BASE[kind] + k
        r = s
        if kind == "z":
            to = self.p.zn(step)
            s = s + (4 if step < 0 else 0)
        return remote(src, dst, self.send.at[s], self.recv.at[r], to)

    def keep(self):
        p = self.p
        return pltpu.make_async_copy(
            self.own.at[:, self.all], self.full.at[p.m, p.z, p.y, p.x, :, self.all], self.local.at[0]
        )

    def fan(self, k, own=False):
        for kind in ("xa", "yb", "ya0", "xb0", "own"):
            self.copy(kind, k, own).start()

    def stage(self, n):
        p = self.p
        if n == 0:
            self.keep().start()
            for step in (1, -1):
                pl.when(p.has(step))(lambda step=step: self.copy("z", p.z, True, step=step).start())
            self.fan(p.z, True)
        elif n <= 3:
            for step in (1, -1):
                k = p.z - step * n
                inside = k >= 0 if step > 0 else k < NZ

                @pl.when(inside)
                def _():
                    self.copy("z", k, arrived=True, step=step).wait_recv()
                    pl.when(p.has(step))(lambda: self.copy("z", k, step=step).start())
                    self.fan(k)
        elif n == 4:
            for k in range(NZ):
                self.copy("xa", k, arrived=True).wait_recv()
                for kind in ("ya1", "ax"):
                    self.copy(kind, k).start()
                self.copy("yb", k, arrived=True).wait_recv()
                for kind in ("xb1", "by"):
                    self.copy(kind, k).start()
        elif n == 5:
            for k in range(NZ):
                for kind, rest in (("ya", "ar"), ("xb", "br")):
                    for rel in ("0", "1"):
                        self.copy(kind + rel, k, arrived=True).wait_recv()
                    self.copy(rest, k).start()
        else:
            for k in range(NZ):
                for kind in ("own", "ax", "by", "ar", "br"):
                    self.copy(kind, k, arrived=True).wait_recv()
                for kind in self.BASE:
                    if kind != "z":
                        self.copy(kind, k).wait_send()
                pl.when((k <= p.z) & p.has(1))(lambda: self.copy("z", k, step=1).wait_send())
                pl.when((k >= p.z) & p.has(-1))(lambda: self.copy("z", k, step=-1).wait_send())
            self.keep().wait()

    STAGES = 7


def add_into(ref, at, other):
    ref[at] = (ref[at].astype(f32) + other.astype(f32)).astype(bf16)


class Scatter:
    SEMS = 32
    LOCAL = 4
    BASE = {"core": 0, "ya": 4, "xb": 8, "xa": 12, "yb": 16, "up": 20, "down": 24}

    @staticmethod
    def scratch(rows, cols):
        half = cols // 2
        return [
            pltpu.VMEM((NZ, NY, NX, rows, cols), bf16), pltpu.VMEM((NZ, NY, NX, rows, cols), bf16),
            pltpu.VMEM((NZ, NX, rows, half), bf16), pltpu.VMEM((NZ, NY, rows, half), bf16),
            pltpu.VMEM((NZ, rows, half), bf16), pltpu.VMEM((NZ, rows, half), bf16),
            pltpu.VMEM((NZ, rows, cols), bf16), pltpu.VMEM((NZ, rows, cols), bf16),
            pltpu.SemaphoreType.DMA((Scatter.SEMS,)), pltpu.SemaphoreType.DMA((Scatter.SEMS,)),
            pltpu.SemaphoreType.DMA((Scatter.LOCAL,)),
        ]

    def __init__(self, grad, part, other, ya, xb, xa, yb, up, down, send, recv, local):
        self.p, self.grad, self.part, self.other = Place(), grad, part, other
        self.land = {"ya": ya, "xb": xb, "xa": xa, "yb": yb, "up": up, "down": down}
        self.send, self.recv, self.local = send, recv, local
        half = part.shape[-1] // 2
        self.a, self.b = pl.ds(0, half), pl.ds(half, half)

    def copy(self, kind, k):
        p = self.p
        oy, ox = 1 - p.y, 1 - p.x
        full = slice(None)
        if kind == "core":
            src, dst, to = self.grad.at[1 - p.m, k], self.other.at[k], p.core()
        else:
            at, to = {
                "ya": ((k, oy, full, full, self.a), p.yn()),
                "xb": ((k, full, ox, full, self.b), p.xn()),
                "xa": ((k, p.y, ox, full, self.a), p.xn()),
                "yb": ((k, oy, p.x, full, self.b), p.yn()),
                "up": ((k, p.y, p.x, full, full), p.zn(1)),
                "down": ((k, p.y, p.x, full, full), p.zn(-1)),
            }[kind]
            src, dst = self.part.at[at], self.land[kind].at[k]
        s = self.BASE[kind] + k
        return remote(src, dst, self.send.at[s], self.recv.at[s], to)

    def load(self, k):
        return pltpu.make_async_copy(self.grad.at[self.p.m, k], self.part.at[k], self.local.at[k])

    def pass_on(self, step):
        p = self.p
        kind = "up" if step > 0 else "down"
        for dist in range(NZ - 1, 0, -1):
            k = p.z + step * dist

            @pl.when((k < NZ) & (k >= 0))
            def _():
                @pl.when(p.has(-step))
                def _():
                    self.copy(kind, k).wait_recv()
                    add_into(self.part, (k, p.y, p.x), self.land[kind][k])

                self.copy(kind, k).start()

    def stage(self, n):
        p = self.p
        oy, ox = 1 - p.y, 1 - p.x
        if n == 0:
            for k in range(NZ):
                self.copy("core", k).start()
                self.load(k).start()
        elif n == 1:
            for k in range(NZ):
                self.load(k).wait()
                self.copy("core", k).wait_recv()
                for y in range(NY):
                    for x in range(NX):
                        add_into(self.part, (k, y, x), self.other[k, y, x])
                self.copy("ya", k).start()
                self.copy("xb", k).start()
        elif n == 2:
            for k in range(NZ):
                self.copy("ya", k).wait_recv()
                for x in range(NX):
                    add_into(self.part, (k, p.y, x, slice(None), self.a), self.land["ya"][k, x])
                self.copy("xa", k).start()
                self.copy("xb", k).wait_recv()
                for y in range(NY):
                    add_into(self.part, (k, y, p.x, slice(None), self.b), self.land["xb"][k, y])
                self.copy("yb", k).start()
        elif n == 3:
            for k in range(NZ):
                self.copy("xa", k).wait_recv()
                add_into(self.part, (k, p.y, p.x, slice(None), self.a), self.land["xa"][k])
                self.copy("yb", k).wait_recv()
                add_into(self.part, (k, p.y, p.x, slice(None), self.b), self.land["yb"][k])
            pl.when(p.z == 0)(lambda: self.pass_on(1))
            pl.when(p.z == NZ - 1)(lambda: self.pass_on(-1))
        elif n in (4, 5):
            j = n - 3
            pl.when(p.z == j)(lambda: self.pass_on(1))
            pl.when(p.z == NZ - 1 - j)(lambda: self.pass_on(-1))
        else:
            for k in range(NZ):
                for kind in ("core", "ya", "xb", "xa", "yb"):
                    self.copy(kind, k).wait_send()
                pl.when(k > p.z)(lambda: self.copy("up", k).wait_send())
                pl.when(k < p.z)(lambda: self.copy("down", k).wait_send())

    STAGES = 7

    def result(self, out):
        p = self.p
        out[...] = self.part[p.z, p.y, p.x].astype(f32)
        for step, kind in ((1, "up"), (-1, "down")):

            @pl.when(p.has(-step))
            def _():
                self.copy(kind, p.z).wait_recv()
                out[...] += self.land[kind][p.z].astype(f32)


class Total:
    STEPS = 5

    @staticmethod
    def scratch(shape):
        return [
            pltpu.VMEM((Total.STEPS, *shape), f32), pltpu.VMEM((Total.STEPS, *shape), f32),
            pltpu.SemaphoreType.DMA((Total.STEPS,)), pltpu.SemaphoreType.DMA((Total.STEPS,)),
        ]

    def __init__(self, start, held, land, send, recv):
        self.p, self.start, self.held, self.land, self.send, self.recv = Place(), start, held, land, send, recv

    def copy(self, n):
        p = self.p
        pair = p.z + 1 - 2 * lax.rem(p.z, 2)
        far = lax.rem(p.z + 2, NZ)
        to = (p.core(), p.yn(), p.xn(), (p.chip(pair, p.y, p.x), p.m), (p.chip(far, p.y, p.x), p.m))[n]
        src = self.start if n == 0 else self.held.at[n - 1]
        return remote(src, self.land.at[n], self.send.at[n], self.recv.at[n], to)

    def stage(self, n):
        if n > 0:
            self.copy(n - 1).wait_recv()
            before = self.start[...] if n == 1 else self.held[n - 2]
            self.held[n - 1] = before + self.land[n - 1]
        if n < self.STEPS:
            self.copy(n).start()
        else:
            for k in range(self.STEPS):
                self.copy(k).wait_send()


def gather_kernel(own_ref, small_ref, full_a, full_b, both_ref, send, recv, local, ssend, srecv):
    p = Place()
    neighbour_barrier(p)
    swap = remote(small_ref, both_ref.at[p.m], ssend.at[0], srecv.at[0], p.core())
    swap.start()
    cols = own_ref.shape[-1]
    parts = []
    for layer, full in enumerate((full_a, full_b)):
        for lo, hi in ((ATT, COLS), (0, ATT)):
            n = len(parts)
            if cols != COLS:
                lo, hi = lo * cols // COLS, hi * cols // COLS
            parts.append(Gather(own_ref.at[layer], full, send.at[n], recv.at[n], local.at[n], lo, hi))
    for n in range(Gather.STAGES):
        for g in parts:
            g.stage(n)
    both_ref[p.m] = small_ref[...]
    swap.wait()


def gather_all(packed, small):
    rows, cols = packed.shape[1:]
    full = jax.ShapeDtypeStruct((2, NZ, NY, NX, rows, cols), bf16)
    n = 2 * LAYERS
    return pl.pallas_call(
        gather_kernel,
        name="gather",
        out_shape=[full, full, jax.ShapeDtypeStruct((2, *small.shape), f32)],
        in_specs=[pl.BlockSpec(memory_space=pltpu.VMEM)] * 2,
        out_specs=[pl.BlockSpec(memory_space=pl.ANY)] * 2 + [pl.BlockSpec(memory_space=pltpu.VMEM)],
        scratch_shapes=[
            pltpu.SemaphoreType.DMA((n, Gather.SEMS)), pltpu.SemaphoreType.DMA((n, Gather.SEMS)),
            pltpu.SemaphoreType.DMA((n, 1)), pltpu.SemaphoreType.DMA((1,)), pltpu.SemaphoreType.DMA((1,)),
        ],
        compiler_params=pltpu.CompilerParams(collective_id=1, has_side_effects=True),
    )(packed, small)


def scatter_kernel(with_small, grad_ref, *refs):
    if with_small:
        small_ref, out_ref, small_out, *rest = refs
        total = Total(small_ref, *rest[-4:])
        rest = rest[:-4]
    else:
        out_ref, *rest = refs
    p = Place()
    neighbour_barrier(p, far=with_small)
    s = Scatter(grad_ref, *rest)
    for n in range(Scatter.STAGES - 1):
        s.stage(n)
        if with_small:
            total.stage(n)
    s.result(out_ref)
    s.stage(Scatter.STAGES - 1)
    if with_small:
        small_out[...] = total.held[Total.STEPS - 1]


def scatter_sum(grad, small, ident):
    rows, cols = grad.shape[-2:]
    with_small = small is not None
    vm = pl.BlockSpec(memory_space=pltpu.VMEM)
    out = [jax.ShapeDtypeStruct((rows, cols), f32)]
    if with_small:
        out.append(jax.ShapeDtypeStruct(small.shape, f32))
    return pl.pallas_call(
        functools.partial(scatter_kernel, with_small),
        name=f"scatter_{ident}",
        out_shape=out,
        in_specs=[pl.BlockSpec(memory_space=pl.ANY)] + [vm] * with_small,
        out_specs=[vm] * len(out),
        scratch_shapes=Scatter.scratch(rows, cols) + (Total.scratch(small.shape) if with_small else []),
        compiler_params=pltpu.CompilerParams(collective_id=ident, has_side_effects=True, vmem_limit_bytes=VLIM),
    )(*((grad, small) if with_small else (grad,)))


def adam_update(weight_in, moment_one, moment_two, grad_sum, decay):
    new_one = beta_one * moment_one + (1.0 - beta_one) * grad_sum
    new_two = beta_two * moment_two + (1.0 - beta_two) * grad_sum * grad_sum
    hat_one = new_one / (1.0 - beta_one**adam_step)
    hat_two = new_two / (1.0 - beta_two**adam_step)
    new_weight = weight_in - learn_rate * (hat_one / (jnp.sqrt(hat_two) + adam_eps) + decay * weight_in)
    return (new_weight, new_one, new_two)


def both_halves(mine, me):
    other = lax.ppermute(mine, "mp", [(0, 1), (1, 0)])
    low = jnp.where(me == 0, mine, other)
    high = jnp.where(me == 0, other, mine)
    return jnp.concatenate([low, high], 0)


SMALL = 2 * HALF + FFH + TABLE * GROUP
LITTLE = 4 * HALF + 2 * FFH + 2 * GROUP * TABLE + 6 * D


def lanes_of(a):
    flat = a.reshape(-1)
    return jnp.pad(flat, (0, -flat.size % 1024)).reshape(-1, 128)


def local(
    fast, tokens, cotangent, image_count, rel_index,
    w_qkv, w_proj, w_fc_one, w_fc_two, qv_bias, fc_one_bias, rel_table, norm_vec,
    m_qkv, m_proj, m_fc_one, m_fc_two, m_qv_bias, m_fc_one_bias, m_rel_table, m_norm_vec,
    v_qkv, v_proj, v_fc_one, v_fc_two, v_qv_bias, v_fc_one_bias, v_rel_table, v_norm_vec,
):
    me = lax.axis_index("mp")
    images = tokens.shape[0]
    nimg = images // 2
    steps = nimg // PAIR
    part = w_qkv.shape[1]
    tok = lax.dynamic_slice_in_dim(tokens, me * nimg, nimg, 0)
    cot = lax.dynamic_slice_in_dim(cotangent, me * nimg, nimg, 0)
    live = (jnp.arange(nimg, dtype=jnp.int32) + me * nimg < image_count[0]).astype(f32)
    live = jnp.broadcast_to(live[:, None], (nimg, 128)).reshape(steps, PAIR, 128)

    packed = jnp.concatenate(
        [w_fc_one, w_fc_two.transpose(0, 2, 1), w_qkv.reshape(LAYERS, part, QKV), w_proj.transpose(0, 2, 1)], 2
    ).astype(bf16)
    small = jnp.concatenate(
        [qv_bias.reshape(LAYERS, -1), fc_one_bias, rel_table.reshape(LAYERS, -1)], 1
    )
    if fast:
        *weights, small = gather_all(packed, lanes_of(small))
        weights = [w.reshape(2, D, COLS) for w in weights]
        small = small.reshape(2, -1)[:, : LAYERS * SMALL].reshape(2, LAYERS, SMALL)
    else:
        weights = lax.all_gather(packed, ("mp", "dp")).reshape(2, -1, LAYERS, part, COLS)
        weights = [weights[:, :, layer].reshape(2, D, COLS) for layer in range(LAYERS)]
        small = lax.all_gather(small, "mp")
    qvb = small[:, :, : 2 * HALF].reshape(2, LAYERS, 2, HALF)
    b1 = small[:, :, 2 * HALF : 2 * HALF + FFH].transpose(1, 0, 2).reshape(LAYERS, 1, 2 * FFH)
    table = small[:, :, 2 * HALF + FFH :].reshape(2, LAYERS, TABLE, GROUP).transpose(1, 2, 0, 3)
    table = table.reshape(LAYERS, TABLE, 2 * GROUP)
    qvb = jnp.concatenate([qvb[:, :, 0], jnp.zeros_like(qvb[:, :, 0]), qvb[:, :, 1]], 2)

    onehot = (rel_index.reshape(1, WSEQ * WSEQ) == jnp.arange(TABLE, dtype=jnp.int32)[:, None]).astype(f32)
    hm = jnp.asarray(head_mask(), bf16)
    x, xs, saved, ctx = tok, [], [], []
    for layer in range(LAYERS):
        shifted = layer % 2 == 1

        wg = weights[layer]
        bias = bias_cols(onehot, table[layer], shifted)
        p = permutation(shifted)
        consts = (jnp.asarray(p, bf16), jnp.asarray(p.T, bf16), hm)
        ctx.append((wg, bias, consts))
        xs.append(x)
        x, *kept = forward_layer(layer, x, wg, bias, qvb[:, layer], b1[layer], norm_vec[layer], consts, steps)
        saved.append(kept)
    out = both_halves(x, me)
    g = cot
    big, little = [None] * LAYERS, [None] * LAYERS
    for layer in reversed(range(LAYERS)):
        wg, bias, consts = ctx[layer]
        g, gw, gqv, gb1, ds, gnv = backward_layer(
            layer, g, xs[layer], saved[layer], wg, bias, norm_vec[layer], consts, live, steps
        )
        ds = ds.reshape(2, WROW, GROUP, WROW)[:, :WSEQ, :, :WSEQ].transpose(0, 2, 3, 1)
        gt = jnp.dot(ds.reshape(2 * GROUP, WSEQ * WSEQ), onehot.T, precision=lax.Precision.HIGHEST)
        little[layer] = jnp.concatenate([gqv.reshape(-1), gb1.reshape(-1), gt.reshape(-1), gnv[:6].reshape(-1)])
        if fast:
            gw = gw.reshape(2, NZ, NY, NX, part, COLS)
            if layer > 0:
                (big[layer],) = scatter_sum(gw, None, 2 + layer)
            else:
                big[layer], total = scatter_sum(gw, lanes_of(jnp.stack(little)), 2 + layer)
                little = total.reshape(-1)[: LAYERS * LITTLE].reshape(LAYERS, LITTLE)
            continue
        mine = lax.dynamic_index_in_dim(gw, me, 0, keepdims=False)
        other = lax.ppermute(lax.dynamic_index_in_dim(gw, 1 - me, 0, keepdims=False), "mp", [(0, 1), (1, 0)])
        total = (mine.astype(f32) + other.astype(f32)).astype(bf16)
        big[layer] = lax.psum_scatter(total, "dp", scatter_dimension=0, tiled=True).astype(f32)
    x_grad = both_halves(g, me)
    if not fast:
        little = lax.psum(jnp.stack(little), ("dp", "mp"))
    big = jnp.stack(big)
    one_grad = big[:, :, :FFH]
    two_grad = big[:, :, FFH:ATT].transpose(0, 2, 1)
    qkv_grad = big[:, :, ATT : ATT + QKV].reshape(LAYERS, part, 3, HALF)
    proj_grad = big[:, :, ATT + QKV :].transpose(0, 2, 1)
    cut = lambda a: lax.dynamic_index_in_dim(a, me, 1, keepdims=False)
    at = 2 * 2 * HALF
    qv_grad = cut(little[:, :at].reshape(LAYERS, 2, 2, HALF).transpose(0, 2, 1, 3))
    bias_grad = cut(little[:, at : at + 2 * FFH].reshape(LAYERS, 2, FFH))
    at += 2 * FFH
    table_grad = cut(little[:, at : at + 2 * GROUP * TABLE].reshape(LAYERS, 2, GROUP, TABLE)).transpose(0, 2, 1)
    at += 2 * GROUP * TABLE
    norm_grad = little[:, at:].reshape(LAYERS, 6, D)
    groups = [
        adam_update(w_qkv, m_qkv, v_qkv, qkv_grad, decay_rate),
        adam_update(w_proj, m_proj, v_proj, proj_grad, decay_rate),
        adam_update(w_fc_one, m_fc_one, v_fc_one, one_grad, decay_rate),
        adam_update(w_fc_two, m_fc_two, v_fc_two, two_grad, decay_rate),
        adam_update(qv_bias, m_qv_bias, v_qv_bias, qv_grad, 0.0),
        adam_update(fc_one_bias, m_fc_one_bias, v_fc_one_bias, bias_grad, 0.0),
        adam_update(rel_table, m_rel_table, v_rel_table, table_grad, 0.0),
        adam_update(norm_vec, m_norm_vec, v_norm_vec, norm_grad, 0.0),
    ]
    return (out, x_grad, *[grp[k] for k in range(3) for grp in groups])


def solution(mesh):
    params = (
        P(None, "dp", None, "mp"), P(None, "mp", "dp"), P(None, "dp", "mp"), P(None, "mp", "dp"),
        P(None, None, "mp"), P(None, "mp"), P(None, None, "mp"), P(),
    )
    act = (P("dp", None, None), P("dp", None, None))
    return jax.shard_map(
        functools.partial(local, mesh.shape["dp"] == PEERS),
        mesh=mesh,
        in_specs=(*act, P("dp"), P(), *params, *params, *params),
        out_specs=(*act, *params, *params, *params),
        check_vma=False,
    )
```

```python
import functools

import jax
import jax.numpy as jnp
import numpy as np
from jax import lax
from jax.experimental import pallas as pl
from jax.experimental.pallas import tpu as pltpu
from jax.sharding import PartitionSpec as P

D = 512
HD = 32
SIDE = 14
WIN = 7
SHIFT = 3
SEQ = 196
WSEQ = 49
TABLE = 169
LAYERS = 2
SEQP = 200
PAIR = 2
ROWS = PAIR * SEQP
WROW = 64
WIMG = 4 * WROW
WPAIR = PAIR * WIMG
HALF = 256
GROUP = 8
LANES = GROUP * WROW
FFH = 1024
QKV = 3 * HALF
COLS = 2 * FFH + QKV + HALF
ATT = 2 * FFH

norm_eps = 1e-05
mask_fill = -100.0
pad_fill = -1e30
beta_one = 0.9
beta_two = 0.999
adam_eps = 1e-08
learn_rate = 0.02
decay_rate = 0.05
adam_step = 3.0
root_half = 0.7071067811865476
inv_root_two_pi = 0.3989422804014327
score_scale = HD**-0.5

f32 = jnp.float32
bf16 = jnp.bfloat16


def dot(a, b, ca=1, cb=0):
    return lax.dot_general(a, b, (((ca,), (cb,)), ((), ())), preferred_element_type=f32)


def window_tokens(shifted):
    off = SHIFT if shifted else 0
    out = np.zeros((4, WSEQ), np.int64)
    for wr in range(2):
        for wc in range(2):
            for p in range(WSEQ):
                r = (7 * wr + p // 7 + off) % SIDE
                c = (7 * wc + p % 7 + off) % SIDE
                out[wr * 2 + wc, p] = r * SIDE + c
    return out


def permutation(shifted):
    tok = window_tokens(shifted)
    perm = np.zeros((WIMG, SEQP), np.float32)
    for w in range(4):
        perm[w * WROW + np.arange(WSEQ), tok[w]] = 1.0
    return perm


def region_mask():
    pos = np.arange(SIDE)
    band = (pos >= SIDE - WIN).astype(int) + (pos >= SIDE - SHIFT).astype(int)
    region = 3 * band[:, None] + band[None, :]
    win = region.reshape(2, WIN, 2, WIN).transpose(0, 2, 1, 3).reshape(4, WSEQ)
    out = np.zeros((4, WROW, WROW), np.float32)
    out[:, :WSEQ, :WSEQ] = np.where(win[:, :, None] != win[:, None, :], mask_fill, 0.0)
    return out


def norm_stats(z):
    mean = jnp.mean(z, -1, keepdims=True)
    cen = z - mean
    var = jnp.mean(cen * cen, -1, keepdims=True)
    inv = lax.rsqrt(var + norm_eps)
    return cen * inv, inv


def norm_back(e, hat, inv, gain):
    s = e * gain
    return inv * (s - jnp.mean(s, -1, keepdims=True) - hat * jnp.mean(s * hat, -1, keepdims=True))


def row_sum(v):
    return jnp.sum(v, 0, keepdims=True)


def put_images(ref, blk):
    for im in range(PAIR):
        ref[im * SEQP : im * SEQP + SEQ, :] = blk[im].astype(f32)
        ref[im * SEQP + SEQ : (im + 1) * SEQP, :] = jnp.zeros((SEQP - SEQ, D), f32)


def to_window_rows(perm, rows, out_ref):
    for im in range(PAIR):
        part = rows[im * SEQP : (im + 1) * SEQP].astype(bf16)
        out_ref[im * WIMG : (im + 1) * WIMG, :] = dot(perm, part).astype(bf16)


def to_token_rows(perm_t, ref):
    return jnp.concatenate(
        [dot(perm_t, ref[im * WIMG : (im + 1) * WIMG, :]) for im in range(PAIR)], 0
    ).astype(bf16)


def expand_heads(x, hm_ref):
    return jnp.concatenate([x * hm_ref[h : h + 1, :] for h in range(GROUP)], 0)


def fold_heads(o):
    lane = lax.broadcasted_iota(jnp.int32, (WROW, HALF), 1) // HD
    acc = o[:WROW]
    for h in range(1, GROUP):
        acc = jnp.where(lane == h, o[h * WROW : (h + 1) * WROW], acc)
    return acc


def softmax_cols(k, qx, bias):
    s = dot(k, qx, 1, 1) * score_scale + bias
    e = jnp.exp(s - jnp.max(s, 0, keepdims=True))
    return e * (1.0 / jnp.sum(e, 0, keepdims=True))


def attend_forward(x, w_ref, bias_ref, qvb_ref, nv_ref, perm_ref, perm_t_ref, hm_ref,
                   qkv_ref, mixed_ref, nperm, mixw, windows):
    hat, _ = norm_stats(x)
    normed = hat * nv_ref[0:1, :] + nv_ref[1:2, :]
    to_window_rows(perm_ref[...], normed, nperm)
    for m in range(2):
        r = dot(nperm[...], w_ref[m, :, :QKV])
        qkv_ref[:, m * QKV : (m + 1) * QKV] = (r + qvb_ref[m : m + 1, :]).astype(bf16)

    def body(w, carry):
        rows = pl.ds(pl.multiple_of(w * WROW, WROW), WROW)
        wt = lax.rem(w, windows) if windows > 1 else 0
        for m in range(2):
            base = m * QKV
            q = qkv_ref[rows, base : base + HALF]
            k = qkv_ref[rows, base + HALF : base + 2 * HALF]
            v = qkv_ref[rows, base + 2 * HALF : base + QKV]
            pr = softmax_cols(k, expand_heads(q, hm_ref), bias_ref[wt, m])
            o = dot(pr.astype(bf16), v, 0, 0)
            mixw[rows, m * HALF : (m + 1) * HALF] = fold_heads(o).astype(bf16)
        return carry

    lax.fori_loop(0, 4 * PAIR, body, 0)
    mixed = to_token_rows(perm_t_ref[...], mixw)
    mixed_ref[...] = mixed
    attn = dot(mixed[:, :HALF], w_ref[0, :, QKV:], 1, 1) + dot(mixed[:, HALF:], w_ref[1, :, QKV:], 1, 1)
    return x + attn + nv_ref[4:5, :]


CH = 512


def mlp_forward(mid, w_ref, b1_ref, nv_ref, act_ref, slope_ref):
    hat, _ = norm_stats(mid)
    hid = (hat * nv_ref[2:3, :] + nv_ref[3:4, :]).astype(bf16)
    total = jnp.zeros((ROWS, D), f32)
    for m in range(2):
        for c in range(0, FFH, CH):
            col = m * FFH + c
            u = dot(hid, w_ref[m, :, c : c + CH]) + b1_ref[:, col : col + CH]
            phi = 0.5 + 0.5 * lax.erf(u * root_half)
            act = (u * phi).astype(bf16)
            act_ref[:, col : col + CH] = act
            slope_ref[:, col : col + CH] = (phi + u * jnp.exp(-0.5 * u * u) * inv_root_two_pi).astype(bf16)
            total += dot(act, w_ref[m, :, FFH + c : FFH + c + CH], 1, 1)
    return mid + total + nv_ref[5:6, :]


def mlp_backward(gout, mid, w_ref, nv_ref, slope_ref, gp, hid_s, gb_s, rows, b1_acc, nv_acc):
    hat, inv = norm_stats(mid)
    hid_s[rows, :] = (hat * nv_ref[2:3, :] + nv_ref[3:4, :]).astype(bf16)
    gb = gout.astype(bf16)
    gb_s[rows, :] = gb
    ghid = jnp.zeros((ROWS, D), f32)
    for m in range(2):
        for c in range(0, FFH, CH):
            col = m * FFH + c
            g = dot(gb, w_ref[m, :, FFH + c : FFH + c + CH]) * slope_ref[:, col : col + CH].astype(f32)
            b1_acc[:, col : col + CH] += row_sum(g)
            g = g.astype(bf16)
            gp[rows, col : col + CH] = g
            ghid += dot(g, w_ref[m, :, c : c + CH], 1, 1)
    gmid = gout + norm_back(ghid, hat, inv, nv_ref[2:3, :])
    nv_acc[2:3, :] += row_sum(ghid * hat)
    nv_acc[3:4, :] += row_sum(ghid)
    nv_acc[4:5, :] += row_sum(gmid)
    nv_acc[5:6, :] += row_sum(gout)
    return gmid


def attend_backward(gmid, x, w_ref, bias_ref, nv_ref, perm_ref, perm_t_ref, hm_ref, qkv_ref,
                    mperm, gmw, gqw, gq_s, mb_s, nb_s, rows, ds_acc, qv_acc, nv_acc, windows):
    hat, inv = norm_stats(x)
    nb_s[rows, :] = (hat * nv_ref[0:1, :] + nv_ref[1:2, :]).astype(bf16)
    mb_s[rows, :] = gmid.astype(bf16)
    to_window_rows(perm_ref[...], gmid, mperm)
    for m in range(2):
        gmw[:, m * HALF : (m + 1) * HALF] = dot(mperm[...], w_ref[m, :, QKV:]).astype(bf16)

    def body(w, carry):
        wrows = pl.ds(pl.multiple_of(w * WROW, WROW), WROW)
        wt = lax.rem(w, windows) if windows > 1 else 0
        for m in range(2):
            base = m * QKV
            q = qkv_ref[wrows, base : base + HALF]
            k = qkv_ref[wrows, base + HALF : base + 2 * HALF]
            v = qkv_ref[wrows, base + 2 * HALF : base + QKV]
            gm = gmw[wrows, m * HALF : (m + 1) * HALF]
            qx = expand_heads(q, hm_ref)
            gx = expand_heads(gm, hm_ref)
            pr = softmax_cols(k, qx, bias_ref[wt, m])
            dp = dot(v, gx, 1, 1)
            ds = pr * (dp - jnp.sum(pr * dp, 0, keepdims=True))
            ds_acc[m] += ds
            ds = ds.astype(bf16)
            gv = dot(pr.astype(bf16), gx)
            gk = dot(ds, qx) * score_scale
            gq = fold_heads(dot(ds, k, 0, 0)) * score_scale
            qv_acc[0:1, m * HALF : (m + 1) * HALF] += row_sum(gq)
            qv_acc[1:2, m * HALF : (m + 1) * HALF] += row_sum(gv)
            gqw[wrows, base : base + HALF] = gq.astype(bf16)
            gqw[wrows, base + HALF : base + 2 * HALF] = gk.astype(bf16)
            gqw[wrows, base + 2 * HALF : base + QKV] = gv.astype(bf16)
        return carry

    lax.fori_loop(0, 4 * PAIR, body, 0)
    gq = to_token_rows(perm_t_ref[...], gqw)
    gq_s[rows, :] = gq
    gnorm = dot(gq[:, :QKV], w_ref[0, :, :QKV], 1, 1) + dot(gq[:, QKV:], w_ref[1, :, :QKV], 1, 1)
    nv_acc[0:1, :] += row_sum(gnorm * hat)
    nv_acc[1:2, :] += row_sum(gnorm)
    return gmid + norm_back(gnorm, hat, inv, nv_ref[0:1, :])


def forward_kernel(first, last, windows, carry, x_ref, wm_ref, wa_ref, bias_ref, qvb_ref, b1_ref, nv_ref,
                   perm_ref, perm_t_ref, hm_ref, *refs):
    i = pl.program_id(0)
    if carry:
        own_ref, y_ref, mid_ref, qkv_ref, mixed_ref, act_ref, slope_ref, full_ref = refs[:8]
        xs, nperm, mixw, *sems = refs[8:]
        comm = Gather(own_ref, full_ref, *sems, 0, COLS)
        pl.when(i == 0)(lambda: neighbour_barrier(comm.p))
    else:
        y_ref, mid_ref, qkv_ref, mixed_ref, act_ref, slope_ref, xs, nperm, mixw = refs
        comm = None
    point(comm, i, 0)
    if first:
        put_images(xs, x_ref)
        x = xs[...]
    else:
        x = x_ref[...]
    mid = attend_forward(x, wa_ref, bias_ref, qvb_ref, nv_ref, perm_ref, perm_t_ref, hm_ref,
                         qkv_ref, mixed_ref, nperm, mixw, windows)
    mid_ref[...] = mid
    point(comm, i, 1)
    y = mlp_forward(mid, wm_ref, b1_ref, nv_ref, act_ref, slope_ref)
    if last:
        for im in range(PAIR):
            y_ref[im] = y[im * SEQP : im * SEQP + SEQ]
    else:
        y_ref[...] = y
    if carry:
        pl.when(i == 2)(lambda: comm.stage(6))


def point(comm, i, at):
    if comm is not None:
        for step in range(3):
            pl.when(i == step)(lambda step=step: comm.stage(2 * step + at))


GW = 1024


def backward_kernel(first, last, windows, steps, carry, g_ref, x_ref, mid_ref, wm_ref, wa_ref, bias_ref, nv_ref,
                    perm_ref, perm_t_ref, hm_ref, live_ref, qkv_ref, slope_ref, act_ref, mixed_ref, *refs):
    i = pl.program_id(0)
    if carry:
        prev_ref, *refs = refs
        sum_ref = refs.pop(6)
        comm = Scatter(prev_ref, *refs[17:])
        refs = refs[:17]
        pl.when(i == 0)(lambda: neighbour_barrier(comm.p))
    else:
        comm = None
    gx_ref, gw_ref, qv_acc, b1_acc, ds_acc, nv_acc, xs, gs, mperm, gmw, gqw, gp, gq_s, hid_s, gb_s, mb_s, nb_s = refs
    point(comm, i, 0)

    @pl.when(i == 0)
    def _():
        for ref in (qv_acc, b1_acc, ds_acc, nv_acc):
            ref[...] = jnp.zeros_like(ref)

    @pl.when(i < steps)
    def _():
        rows = pl.ds(pl.multiple_of(i * ROWS, ROWS), ROWS)
        if last:
            for im in range(PAIR):
                flag = live_ref[im : im + 1, :]
                gs[im * SEQP : im * SEQP + SEQ, :] = g_ref[im] * jnp.concatenate([flag] * 4, 1)
                gs[im * SEQP + SEQ : (im + 1) * SEQP, :] = jnp.zeros((SEQP - SEQ, D), f32)
            gout = gs[...]
        else:
            gout = g_ref[...]
        if first:
            put_images(xs, x_ref)
            x = xs[...]
        else:
            x = x_ref[...]
        gmid = mlp_backward(gout, mid_ref[...], wm_ref, nv_ref, slope_ref, gp, hid_s, gb_s, rows, b1_acc, nv_acc)
        point(comm, i, 1)
        gin = attend_backward(gmid, x, wa_ref, bias_ref, nv_ref, perm_ref, perm_t_ref, hm_ref, qkv_ref,
                              mperm, gmw, gqw, gq_s, mb_s, nb_s, rows, ds_acc, qv_acc, nv_acc, windows)
        if first:
            for im in range(PAIR):
                gx_ref[im] = gin[im * SEQP : im * SEQP + SEQ]
        else:
            gx_ref[...] = gin

    if carry:

        @pl.when(i == steps)
        def _():
            comm.result(sum_ref)
            comm.stage(6)

    for m in range(2):

        @pl.when(i == steps + 3 * m)
        def _():
            gw_ref[0] = dot(hid_s[...], gp[:, m * FFH : (m + 1) * FFH], 0, 0).astype(bf16)

        @pl.when(i == steps + 3 * m + 1)
        def _():
            gw_ref[0] = dot(gb_s[...], act_ref[:, m * FFH : (m + 1) * FFH], 0, 0).astype(bf16)

        @pl.when(i == steps + 3 * m + 2)
        def _():
            gw_ref[0, :, :QKV] = dot(nb_s[...], gq_s[:, m * QKV : (m + 1) * QKV], 0, 0).astype(bf16)
            gw_ref[0, :, QKV:] = dot(mb_s[...], mixed_ref[:, m * HALF : (m + 1) * HALF], 0, 0).astype(bf16)


def whole(shape, buffers=1):
    zero = (0,) * len(shape)
    return pl.BlockSpec(shape, lambda i: zero, pipeline_mode=pl.Buffered(buffers))


VLIM = 60 * 1024 * 1024


def forward_layer(layer, x, wg, bias, qvb, b1, nv, consts, steps, own=None):
    first, last = layer == 0, layer == LAYERS - 1
    shifted = layer % 2 == 1
    perm, perm_t, hm = consts
    nimg = steps * PAIR
    windows = bias.shape[0]
    img = lambda: pl.BlockSpec((PAIR, SEQ, D), lambda i: (i, 0, 0))
    row = lambda n: pl.BlockSpec((ROWS, n), lambda i: (i, 0))
    carry = own is not None
    more = dict(in_specs=[], out_specs=[], out_shape=[], scratch=[], params={})
    if carry:
        more = dict(
            in_specs=[whole(own.shape)],
            out_specs=[pl.BlockSpec(memory_space=pl.ANY)],
            out_shape=[jax.ShapeDtypeStruct((2, NZ, NY, NX, *own.shape), bf16)],
            scratch=[
                pltpu.SemaphoreType.DMA((Gather.SEMS,)), pltpu.SemaphoreType.DMA((Gather.SEMS,)),
                pltpu.SemaphoreType.DMA((1,)),
            ],
            params=dict(collective_id=8 + layer, has_side_effects=True),
        )
    return pl.pallas_call(
        functools.partial(forward_kernel, first, last, windows, carry),
        name=f"forward_{layer}",
        grid=(steps,),
        in_specs=[
            img() if first else row(D),
            pl.BlockSpec((2, D, ATT), lambda i: (0, 0, 0), pipeline_mode=pl.Buffered(1)),
            pl.BlockSpec((2, D, COLS - ATT), lambda i: (0, 0, ATT // (COLS - ATT)), pipeline_mode=pl.Buffered(1)),
            whole(bias.shape), whole(qvb.shape), whole(b1.shape), whole(nv.shape),
            whole(perm.shape), whole(perm_t.shape), whole(hm.shape),
        ] + more["in_specs"],
        out_specs=[
            img() if last else row(D), row(D),
            pl.BlockSpec((WPAIR, 2 * QKV), lambda i: (i, 0)), row(D), row(2 * FFH), row(2 * FFH),
        ] + more["out_specs"],
        out_shape=[
            jax.ShapeDtypeStruct((nimg, SEQ, D) if last else (nimg * SEQP, D), f32),
            jax.ShapeDtypeStruct((nimg * SEQP, D), f32),
            jax.ShapeDtypeStruct((steps * WPAIR, 2 * QKV), bf16),
            jax.ShapeDtypeStruct((nimg * SEQP, D), bf16),
            jax.ShapeDtypeStruct((nimg * SEQP, 2 * FFH), bf16),
            jax.ShapeDtypeStruct((nimg * SEQP, 2 * FFH), bf16),
        ] + more["out_shape"],
        scratch_shapes=[
            pltpu.VMEM((ROWS, D), f32), pltpu.VMEM((WPAIR, D), bf16), pltpu.VMEM((WPAIR, D), bf16),
        ] + more["scratch"],
        compiler_params=pltpu.CompilerParams(vmem_limit_bytes=VLIM, **more["params"]),
    )(x, wg, wg, bias, qvb, b1, nv, perm, perm_t, hm, *([own] if carry else []))


def backward_layer(layer, grad, x, saved, wg, bias, nv, consts, live, steps, prev=None):
    first, last = layer == 0, layer == LAYERS - 1
    perm, perm_t, hm = consts
    mid, qkv, mixed, act, slope = saved
    nimg = steps * PAIR
    windows = bias.shape[0]
    top = steps - 1
    img = lambda: pl.BlockSpec((PAIR, SEQ, D), lambda i: (jnp.minimum(i, top), 0, 0))
    row = lambda n: pl.BlockSpec((ROWS, n), lambda i: (jnp.minimum(i, top), 0))
    total = nimg * SEQP

    def gmap(i):
        k = jnp.maximum(i - steps, 0)
        return (k // 3, 0, lax.rem(k, 3))

    carry = prev is not None
    more = dict(in_specs=[], out_specs=[], out_shape=[], scratch=[], params={})
    if carry:
        rows, cols = prev.shape[-2:]
        more = dict(
            in_specs=[pl.BlockSpec(memory_space=pl.ANY)],
            out_specs=[whole((rows, cols))],
            out_shape=[jax.ShapeDtypeStruct((rows, cols), f32)],
            scratch=Scatter.scratch(rows, cols),
            params=dict(collective_id=10 + layer, has_side_effects=True),
        )
    return pl.pallas_call(
        functools.partial(backward_kernel, first, last, windows, steps, carry),
        name=f"backward_{layer}",
        grid=(steps + 6,),
        in_specs=[
            img() if last else row(D), img() if first else row(D), row(D),
            pl.BlockSpec((2, D, ATT), lambda i: (0, 0, 0), pipeline_mode=pl.Buffered(1)),
            pl.BlockSpec((2, D, COLS - ATT), lambda i: (0, 0, ATT // (COLS - ATT)), pipeline_mode=pl.Buffered(1)),
            whole(bias.shape), whole(nv.shape), whole(perm.shape), whole(perm_t.shape), whole(hm.shape),
            pl.BlockSpec((None, PAIR, 128), lambda i: (jnp.minimum(i, top), 0, 0)),
            pl.BlockSpec((WPAIR, 2 * QKV), lambda i: (jnp.minimum(i, top), 0)), row(2 * FFH),
            whole(act.shape), whole(mixed.shape),
        ] + more["in_specs"],
        out_specs=[
            img() if first else row(D),
            pl.BlockSpec((1, D, GW), gmap),
            whole((2, 2 * HALF)), whole((1, 2 * FFH)), whole((2, WROW, LANES)), whole((8, D)),
        ] + more["out_specs"],
        out_shape=[
            jax.ShapeDtypeStruct((nimg, SEQ, D) if first else (total, D), f32),
            jax.ShapeDtypeStruct((2, D, COLS), bf16),
            jax.ShapeDtypeStruct((2, 2 * HALF), f32),
            jax.ShapeDtypeStruct((1, 2 * FFH), f32),
            jax.ShapeDtypeStruct((2, WROW, LANES), f32),
            jax.ShapeDtypeStruct((8, D), f32),
        ] + more["out_shape"],
        scratch_shapes=[
            pltpu.VMEM((ROWS, D), f32), pltpu.VMEM((ROWS, D), f32),
            pltpu.VMEM((WPAIR, D), bf16), pltpu.VMEM((WPAIR, D), bf16), pltpu.VMEM((WPAIR, 2 * QKV), bf16),
            pltpu.VMEM((total, 2 * FFH), bf16), pltpu.VMEM((total, 2 * QKV), bf16),
            pltpu.VMEM((total, D), bf16), pltpu.VMEM((total, D), bf16),
            pltpu.VMEM((total, D), bf16), pltpu.VMEM((total, D), bf16),
        ] + more["scratch"],
        compiler_params=pltpu.CompilerParams(vmem_limit_bytes=VLIM, **more["params"]),
    )(grad, x, mid, wg, wg, bias, nv, perm, perm_t, hm, live, qkv, slope, act, mixed, *([prev] if carry else []))


def head_mask():
    return (np.arange(HALF)[None, :] // HD == np.arange(GROUP)[:, None]).astype(np.float32)


def bias_cols(onehot, table, shifted):
    picked = jnp.dot(table.T, onehot, precision=lax.Precision.HIGHEST).reshape(2, GROUP, WSEQ, WSEQ)
    by_j = picked.transpose(0, 3, 1, 2)
    by_j = jnp.pad(by_j, ((0, 0), (0, 0), (0, 0), (0, WROW - WSEQ)))
    by_j = jnp.pad(by_j, ((0, 0), (0, WROW - WSEQ), (0, 0), (0, 0)), constant_values=pad_fill)
    if shifted:
        by_j = by_j[None] + jnp.asarray(region_mask())[:, None, :, None, :]
    else:
        by_j = by_j[None]
    return by_j.reshape(-1, 2, WROW, LANES)

NZ, NY, NX = 4, 2, 2
PEERS = NZ * NY * NX
MESH_ID = pl.DeviceIdType.MESH


class Place:
    def __init__(self):
        d = lax.axis_index("dp")
        self.d, self.m = d, lax.axis_index("mp")
        self.z, self.y, self.x = d // 4, lax.rem(d // 2, 2), lax.rem(d, 2)

    def chip(self, z, y, x):
        return (z * NY + y) * NX + x

    def at(self, dz=0, y=None, x=None, m=None):
        y = self.y if y is None else y
        x = self.x if x is None else x
        return (self.chip(self.z + dz, y, x), self.m if m is None else m)

    def xn(self):
        return self.at(x=1 - self.x)

    def yn(self):
        return self.at(y=1 - self.y)

    def core(self):
        return self.at(m=1 - self.m)

    def zn(self, step):
        return self.at(dz=step)

    def has(self, step):
        return self.z < NZ - 1 if step > 0 else self.z > 0


def remote(src, dst, send, recv, to):
    return pltpu.make_async_remote_copy(
        src_ref=src, dst_ref=dst, send_sem=send, recv_sem=recv, device_id=to, device_id_type=MESH_ID
    )


def neighbour_barrier(p, far=False):
    sem = pltpu.get_barrier_semaphore()

    def tell(to):
        pl.semaphore_signal(sem, inc=1, device_id=to, device_id_type=MESH_ID)

    for to in (p.xn(), p.yn(), p.core()):
        tell(to)
    count = 3
    for step in (1, -1):
        pl.when(p.has(step))(lambda step=step: tell(p.zn(step)))
        count = count + p.has(step).astype(jnp.int32)
    if far:
        tell((p.chip((p.z + 2) % NZ, p.y, p.x), p.m))
        count = count + 1
    pl.semaphore_wait(sem, count)


class Gather:
    SEMS = 52
    BASE = {"z": 0, "xa": 8, "yb": 12, "ya0": 16, "ya1": 20, "xb0": 24, "xb1": 28,
            "own": 32, "ax": 36, "by": 40, "ar": 44, "br": 48}

    def __init__(self, own, full, send, recv, local, lo, hi):
        self.p, self.own, self.full = Place(), own, full
        self.send, self.recv, self.local = send, recv, local
        mid = (lo + hi) // 2
        self.all, self.a, self.b = pl.ds(lo, hi - lo), pl.ds(lo, mid - lo), pl.ds(mid, hi - mid)

    def region(self, kind, k, arrived):
        p = self.p
        oy, ox = 1 - p.y, 1 - p.x
        if kind == "z":
            return (p.m, k, p.y, p.x), self.all, None
        if kind == "xa":
            return (p.m, k, p.y, ox if arrived else p.x), self.a, p.xn()
        if kind == "yb":
            return (p.m, k, oy if arrived else p.y, p.x), self.b, p.yn()
        if kind in ("ya0", "ya1"):
            return (p.m, k, oy if arrived else p.y, p.x if kind == "ya0" else ox), self.a, p.yn()
        if kind in ("xb0", "xb1"):
            return (p.m, k, p.y if kind == "xb0" else oy, ox if arrived else p.x), self.b, p.xn()
        m = 1 - p.m if arrived else p.m
        if kind == "own":
            return (m, k, p.y, p.x), self.all, p.core()
        if kind == "ax":
            return (m, k, p.y, ox), self.a, p.core()
        if kind == "by":
            return (m, k, oy, p.x), self.b, p.core()
        if kind == "ar":
            return (m, k, oy, slice(None)), self.a, p.core()
        return (m, k, slice(None), ox), self.b, p.core()

    def copy(self, kind, k, own=False, arrived=False, step=0):
        at, cols, to = self.region(kind, k, arrived)
        dst = self.full.at[(*at, slice(None), cols)]
        src = self.own.at[:, cols] if own else dst
        s = self.BASE[kind] + k
        r = s
        if kind == "z":
            to = self.p.zn(step)
            s = s + (4 if step < 0 else 0)
        return remote(src, dst, self.send.at[s], self.recv.at[r], to)

    def keep(self):
        p = self.p
        return pltpu.make_async_copy(
            self.own.at[:, self.all], self.full.at[p.m, p.z, p.y, p.x, :, self.all], self.local.at[0]
        )

    def fan(self, k, own=False):
        for kind in ("xa", "yb", "ya0", "xb0", "own"):
            self.copy(kind, k, own).start()

    def stage(self, n):
        p = self.p
        if n == 0:
            self.keep().start()
            for step in (1, -1):
                pl.when(p.has(step))(lambda step=step: self.copy("z", p.z, True, step=step).start())
            self.fan(p.z, True)
        elif n <= 3:
            for step in (1, -1):
                k = p.z - step * n
                inside = k >= 0 if step > 0 else k < NZ

                @pl.when(inside)
                def _():
                    self.copy("z", k, arrived=True, step=step).wait_recv()
                    pl.when(p.has(step))(lambda: self.copy("z", k, step=step).start())
                    self.fan(k)
        elif n == 4:
            for k in range(NZ):
                self.copy("xa", k, arrived=True).wait_recv()
                for kind in ("ya1", "ax"):
                    self.copy(kind, k).start()
                self.copy("yb", k, arrived=True).wait_recv()
                for kind in ("xb1", "by"):
                    self.copy(kind, k).start()
        elif n == 5:
            for k in range(NZ):
                for kind, rest in (("ya", "ar"), ("xb", "br")):
                    for rel in ("0", "1"):
                        self.copy(kind + rel, k, arrived=True).wait_recv()
                    self.copy(rest, k).start()
        else:
            for k in range(NZ):
                for kind in ("own", "ax", "by", "ar", "br"):
                    self.copy(kind, k, arrived=True).wait_recv()
                for kind in self.BASE:
                    if kind != "z":
                        self.copy(kind, k).wait_send()
                pl.when((k <= p.z) & p.has(1))(lambda: self.copy("z", k, step=1).wait_send())
                pl.when((k >= p.z) & p.has(-1))(lambda: self.copy("z", k, step=-1).wait_send())
            self.keep().wait()

    STAGES = 7


def add_into(ref, at, other):
    ref[at] = (ref[at].astype(f32) + other.astype(f32)).astype(bf16)


class Scatter:
    SEMS = 32
    LOCAL = 4
    BASE = {"core": 0, "ya": 4, "xb": 8, "xa": 12, "yb": 16, "up": 20, "down": 24}

    @staticmethod
    def scratch(rows, cols):
        half = cols // 2
        return [
            pltpu.VMEM((NZ, NY, NX, rows, cols), bf16), pltpu.VMEM((NZ, NY, NX, rows, cols), bf16),
            pltpu.VMEM((NZ, NX, rows, half), bf16), pltpu.VMEM((NZ, NY, rows, half), bf16),
            pltpu.VMEM((NZ, rows, half), bf16), pltpu.VMEM((NZ, rows, half), bf16),
            pltpu.VMEM((NZ, rows, cols), bf16), pltpu.VMEM((NZ, rows, cols), bf16),
            pltpu.SemaphoreType.DMA((Scatter.SEMS,)), pltpu.SemaphoreType.DMA((Scatter.SEMS,)),
            pltpu.SemaphoreType.DMA((Scatter.LOCAL,)),
        ]

    def __init__(self, grad, part, other, ya, xb, xa, yb, up, down, send, recv, local):
        self.p, self.grad, self.part, self.other = Place(), grad, part, other
        self.land = {"ya": ya, "xb": xb, "xa": xa, "yb": yb, "up": up, "down": down}
        self.send, self.recv, self.local = send, recv, local
        half = part.shape[-1] // 2
        self.a, self.b = pl.ds(0, half), pl.ds(half, half)

    def copy(self, kind, k):
        p = self.p
        oy, ox = 1 - p.y, 1 - p.x
        full = slice(None)
        if kind == "core":
            src, dst, to = self.grad.at[1 - p.m, k], self.other.at[k], p.core()
        else:
            at, to = {
                "ya": ((k, oy, full, full, self.a), p.yn()),
                "xb": ((k, full, ox, full, self.b), p.xn()),
                "xa": ((k, p.y, ox, full, self.a), p.xn()),
                "yb": ((k, oy, p.x, full, self.b), p.yn()),
                "up": ((k, p.y, p.x, full, full), p.zn(1)),
                "down": ((k, p.y, p.x, full, full), p.zn(-1)),
            }[kind]
            src, dst = self.part.at[at], self.land[kind].at[k]
        s = self.BASE[kind] + k
        return remote(src, dst, self.send.at[s], self.recv.at[s], to)

    def load(self, k):
        return pltpu.make_async_copy(self.grad.at[self.p.m, k], self.part.at[k], self.local.at[k])

    def pass_on(self, step):
        p = self.p
        kind = "up" if step > 0 else "down"
        for dist in range(NZ - 1, 0, -1):
            k = p.z + step * dist

            @pl.when((k < NZ) & (k >= 0))
            def _():
                @pl.when(p.has(-step))
                def _():
                    self.copy(kind, k).wait_recv()
                    add_into(self.part, (k, p.y, p.x), self.land[kind][k])

                self.copy(kind, k).start()

    def stage(self, n):
        p = self.p
        oy, ox = 1 - p.y, 1 - p.x
        if n == 0:
            for k in range(NZ):
                self.copy("core", k).start()
                self.load(k).start()
        elif n == 1:
            for k in range(NZ):
                self.load(k).wait()
                self.copy("core", k).wait_recv()
                for y in range(NY):
                    for x in range(NX):
                        add_into(self.part, (k, y, x), self.other[k, y, x])
                self.copy("ya", k).start()
                self.copy("xb", k).start()
        elif n == 2:
            for k in range(NZ):
                self.copy("ya", k).wait_recv()
                for x in range(NX):
                    add_into(self.part, (k, p.y, x, slice(None), self.a), self.land["ya"][k, x])
                self.copy("xa", k).start()
                self.copy("xb", k).wait_recv()
                for y in range(NY):
                    add_into(self.part, (k, y, p.x, slice(None), self.b), self.land["xb"][k, y])
                self.copy("yb", k).start()
        elif n == 3:
            for k in range(NZ):
                self.copy("xa", k).wait_recv()
                add_into(self.part, (k, p.y, p.x, slice(None), self.a), self.land["xa"][k])
                self.copy("yb", k).wait_recv()
                add_into(self.part, (k, p.y, p.x, slice(None), self.b), self.land["yb"][k])
            pl.when(p.z == 0)(lambda: self.pass_on(1))
            pl.when(p.z == NZ - 1)(lambda: self.pass_on(-1))
        elif n in (4, 5):
            j = n - 3
            pl.when(p.z == j)(lambda: self.pass_on(1))
            pl.when(p.z == NZ - 1 - j)(lambda: self.pass_on(-1))
        else:
            for k in range(NZ):
                for kind in ("core", "ya", "xb", "xa", "yb"):
                    self.copy(kind, k).wait_send()
                pl.when(k > p.z)(lambda: self.copy("up", k).wait_send())
                pl.when(k < p.z)(lambda: self.copy("down", k).wait_send())

    STAGES = 7

    def result(self, out):
        p = self.p
        out[...] = self.part[p.z, p.y, p.x].astype(f32)
        for step, kind in ((1, "up"), (-1, "down")):

            @pl.when(p.has(-step))
            def _():
                self.copy(kind, p.z).wait_recv()
                out[...] += self.land[kind][p.z].astype(f32)


class Total:
    STEPS = 5

    @staticmethod
    def scratch(shape):
        return [
            pltpu.VMEM((Total.STEPS, *shape), f32), pltpu.VMEM((Total.STEPS, *shape), f32),
            pltpu.SemaphoreType.DMA((Total.STEPS,)), pltpu.SemaphoreType.DMA((Total.STEPS,)),
        ]

    def __init__(self, start, held, land, send, recv):
        self.p, self.start, self.held, self.land, self.send, self.recv = Place(), start, held, land, send, recv

    def copy(self, n):
        p = self.p
        pair = p.z + 1 - 2 * lax.rem(p.z, 2)
        far = lax.rem(p.z + 2, NZ)
        to = (p.core(), p.yn(), p.xn(), (p.chip(pair, p.y, p.x), p.m), (p.chip(far, p.y, p.x), p.m))[n]
        src = self.start if n == 0 else self.held.at[n - 1]
        return remote(src, self.land.at[n], self.send.at[n], self.recv.at[n], to)

    def stage(self, n):
        if n > 0:
            self.copy(n - 1).wait_recv()
            before = self.start[...] if n == 1 else self.held[n - 2]
            self.held[n - 1] = before + self.land[n - 1]
        if n < self.STEPS:
            self.copy(n).start()
        else:
            for k in range(self.STEPS):
                self.copy(k).wait_send()


def gather_kernel(own_ref, small_ref, full_ref, both_ref, send, recv, local, ssend, srecv):
    p = Place()
    neighbour_barrier(p)
    swap = remote(small_ref, both_ref.at[p.m], ssend.at[0], srecv.at[0], p.core())
    swap.start()
    parts = []
    for n, (lo, hi) in enumerate(((ATT, COLS), (0, ATT))):
        parts.append(Gather(own_ref, full_ref, send.at[n], recv.at[n], local.at[n], lo, hi))
    for n in range(Gather.STAGES):
        for g in parts:
            g.stage(n)
    both_ref[p.m] = small_ref[...]
    swap.wait()


def gather_all(packed, small):
    rows, cols = packed.shape
    full = jax.ShapeDtypeStruct((2, NZ, NY, NX, rows, cols), bf16)
    return pl.pallas_call(
        gather_kernel,
        name="gather",
        out_shape=[full, jax.ShapeDtypeStruct((2, *small.shape), f32)],
        in_specs=[pl.BlockSpec(memory_space=pltpu.VMEM)] * 2,
        out_specs=[pl.BlockSpec(memory_space=pl.ANY), pl.BlockSpec(memory_space=pltpu.VMEM)],
        scratch_shapes=[
            pltpu.SemaphoreType.DMA((2, Gather.SEMS)), pltpu.SemaphoreType.DMA((2, Gather.SEMS)),
            pltpu.SemaphoreType.DMA((2, 1)), pltpu.SemaphoreType.DMA((1,)), pltpu.SemaphoreType.DMA((1,)),
        ],
        compiler_params=pltpu.CompilerParams(collective_id=1, has_side_effects=True),
    )(packed, small)


def scatter_kernel(with_small, grad_ref, *refs):
    if with_small:
        small_ref, out_ref, small_out, *rest = refs
        total = Total(small_ref, *rest[-4:])
        rest = rest[:-4]
    else:
        out_ref, *rest = refs
    p = Place()
    neighbour_barrier(p, far=with_small)
    s = Scatter(grad_ref, *rest)
    for n in range(Scatter.STAGES - 1):
        s.stage(n)
        if with_small:
            total.stage(n)
    s.result(out_ref)
    s.stage(Scatter.STAGES - 1)
    if with_small:
        small_out[...] = total.held[Total.STEPS - 1]


def scatter_sum(grad, small, ident):
    rows, cols = grad.shape[-2:]
    with_small = small is not None
    vm = pl.BlockSpec(memory_space=pltpu.VMEM)
    out = [jax.ShapeDtypeStruct((rows, cols), f32)]
    if with_small:
        out.append(jax.ShapeDtypeStruct(small.shape, f32))
    return pl.pallas_call(
        functools.partial(scatter_kernel, with_small),
        name=f"scatter_{ident}",
        out_shape=out,
        in_specs=[pl.BlockSpec(memory_space=pl.ANY)] + [vm] * with_small,
        out_specs=[vm] * len(out),
        scratch_shapes=Scatter.scratch(rows, cols) + (Total.scratch(small.shape) if with_small else []),
        compiler_params=pltpu.CompilerParams(collective_id=ident, has_side_effects=True, vmem_limit_bytes=VLIM),
    )(*((grad, small) if with_small else (grad,)))


def adam_update(weight_in, moment_one, moment_two, grad_sum, decay):
    new_one = beta_one * moment_one + (1.0 - beta_one) * grad_sum
    new_two = beta_two * moment_two + (1.0 - beta_two) * grad_sum * grad_sum
    hat_one = new_one / (1.0 - beta_one**adam_step)
    hat_two = new_two / (1.0 - beta_two**adam_step)
    new_weight = weight_in - learn_rate * (hat_one / (jnp.sqrt(hat_two) + adam_eps) + decay * weight_in)
    return (new_weight, new_one, new_two)


def both_halves(mine, me):
    other = lax.ppermute(mine, "mp", [(0, 1), (1, 0)])
    low = jnp.where(me == 0, mine, other)
    high = jnp.where(me == 0, other, mine)
    return jnp.concatenate([low, high], 0)


SMALL = 2 * HALF + FFH + TABLE * GROUP
LITTLE = 4 * HALF + 2 * FFH + 2 * GROUP * TABLE + 6 * D


def lanes_of(a):
    flat = a.reshape(-1)
    return jnp.pad(flat, (0, -flat.size % 1024)).reshape(-1, 128)


def local(
    fast, tokens, cotangent, image_count, rel_index,
    w_qkv, w_proj, w_fc_one, w_fc_two, qv_bias, fc_one_bias, rel_table, norm_vec,
    m_qkv, m_proj, m_fc_one, m_fc_two, m_qv_bias, m_fc_one_bias, m_rel_table, m_norm_vec,
    v_qkv, v_proj, v_fc_one, v_fc_two, v_qv_bias, v_fc_one_bias, v_rel_table, v_norm_vec,
):
    me = lax.axis_index("mp")
    images = tokens.shape[0]
    nimg = images // 2
    steps = nimg // PAIR
    part = w_qkv.shape[1]
    tok = lax.dynamic_slice_in_dim(tokens, me * nimg, nimg, 0)
    cot = lax.dynamic_slice_in_dim(cotangent, me * nimg, nimg, 0)
    live = (jnp.arange(nimg, dtype=jnp.int32) + me * nimg < image_count[0]).astype(f32)
    live = jnp.broadcast_to(live[:, None], (nimg, 128)).reshape(steps, PAIR, 128)

    packed = jnp.concatenate(
        [w_fc_one, w_fc_two.transpose(0, 2, 1), w_qkv.reshape(LAYERS, part, QKV), w_proj.transpose(0, 2, 1)], 2
    ).astype(bf16)
    small = jnp.concatenate(
        [qv_bias.reshape(LAYERS, -1), fc_one_bias, rel_table.reshape(LAYERS, -1)], 1
    )
    if fast:
        weights, small = gather_all(packed[0], lanes_of(small))
        weights = [weights.reshape(2, D, COLS)]
        small = small.reshape(2, -1)[:, : LAYERS * SMALL].reshape(2, LAYERS, SMALL)
    else:
        weights = lax.all_gather(packed, ("mp", "dp")).reshape(2, -1, LAYERS, part, COLS)
        weights = [weights[:, :, layer].reshape(2, D, COLS) for layer in range(LAYERS)]
        small = lax.all_gather(small, "mp")
    qvb = small[:, :, : 2 * HALF].reshape(2, LAYERS, 2, HALF)
    b1 = small[:, :, 2 * HALF : 2 * HALF + FFH].transpose(1, 0, 2).reshape(LAYERS, 1, 2 * FFH)
    table = small[:, :, 2 * HALF + FFH :].reshape(2, LAYERS, TABLE, GROUP).transpose(1, 2, 0, 3)
    table = table.reshape(LAYERS, TABLE, 2 * GROUP)
    qvb = jnp.concatenate([qvb[:, :, 0], jnp.zeros_like(qvb[:, :, 0]), qvb[:, :, 1]], 2)

    onehot = (rel_index.reshape(1, WSEQ * WSEQ) == jnp.arange(TABLE, dtype=jnp.int32)[:, None]).astype(f32)
    hm = jnp.asarray(head_mask(), bf16)
    x, xs, saved, ctx = tok, [], [], []
    for layer in range(LAYERS):
        shifted = layer % 2 == 1

        wg = weights[layer]
        bias = bias_cols(onehot, table[layer], shifted)
        p = permutation(shifted)
        consts = (jnp.asarray(p, bf16), jnp.asarray(p.T, bf16), hm)
        ctx.append((wg, bias, consts))
        xs.append(x)
        own = packed[layer + 1] if fast and layer + 1 < LAYERS else None
        x, *kept = forward_layer(layer, x, wg, bias, qvb[:, layer], b1[layer], norm_vec[layer], consts, steps, own)
        if own is not None:
            weights.append(kept.pop().reshape(2, D, COLS))
        saved.append(kept)
    out = both_halves(x, me)
    g = cot
    waiting = None
    big, little = [None] * LAYERS, [None] * LAYERS
    for layer in reversed(range(LAYERS)):
        wg, bias, consts = ctx[layer]
        g, gw, gqv, gb1, ds, gnv, *done = backward_layer(
            layer, g, xs[layer], saved[layer], wg, bias, norm_vec[layer], consts, live, steps, waiting
        )
        if done:
            big[layer + 1] = done[0]
        ds = ds.reshape(2, WROW, GROUP, WROW)[:, :WSEQ, :, :WSEQ].transpose(0, 2, 3, 1)
        gt = jnp.dot(ds.reshape(2 * GROUP, WSEQ * WSEQ), onehot.T, precision=lax.Precision.HIGHEST)
        little[layer] = jnp.concatenate([gqv.reshape(-1), gb1.reshape(-1), gt.reshape(-1), gnv[:6].reshape(-1)])
        if fast:
            gw = gw.reshape(2, NZ, NY, NX, part, COLS)
            waiting = gw
            if layer == 0:
                big[layer], total = scatter_sum(gw, lanes_of(jnp.stack(little)), 2 + layer)
                little = total.reshape(-1)[: LAYERS * LITTLE].reshape(LAYERS, LITTLE)
            continue
        mine = lax.dynamic_index_in_dim(gw, me, 0, keepdims=False)
        other = lax.ppermute(lax.dynamic_index_in_dim(gw, 1 - me, 0, keepdims=False), "mp", [(0, 1), (1, 0)])
        total = (mine.astype(f32) + other.astype(f32)).astype(bf16)
        big[layer] = lax.psum_scatter(total, "dp", scatter_dimension=0, tiled=True).astype(f32)
    x_grad = both_halves(g, me)
    if not fast:
        little = lax.psum(jnp.stack(little), ("dp", "mp"))
    big = jnp.stack(big)
    one_grad = big[:, :, :FFH]
    two_grad = big[:, :, FFH:ATT].transpose(0, 2, 1)
    qkv_grad = big[:, :, ATT : ATT + QKV].reshape(LAYERS, part, 3, HALF)
    proj_grad = big[:, :, ATT + QKV :].transpose(0, 2, 1)
    cut = lambda a: lax.dynamic_index_in_dim(a, me, 1, keepdims=False)
    at = 2 * 2 * HALF
    qv_grad = cut(little[:, :at].reshape(LAYERS, 2, 2, HALF).transpose(0, 2, 1, 3))
    bias_grad = cut(little[:, at : at + 2 * FFH].reshape(LAYERS, 2, FFH))
    at += 2 * FFH
    table_grad = cut(little[:, at : at + 2 * GROUP * TABLE].reshape(LAYERS, 2, GROUP, TABLE)).transpose(0, 2, 1)
    at += 2 * GROUP * TABLE
    norm_grad = little[:, at:].reshape(LAYERS, 6, D)
    groups = [
        adam_update(w_qkv, m_qkv, v_qkv, qkv_grad, decay_rate),
        adam_update(w_proj, m_proj, v_proj, proj_grad, decay_rate),
        adam_update(w_fc_one, m_fc_one, v_fc_one, one_grad, decay_rate),
        adam_update(w_fc_two, m_fc_two, v_fc_two, two_grad, decay_rate),
        adam_update(qv_bias, m_qv_bias, v_qv_bias, qv_grad, 0.0),
        adam_update(fc_one_bias, m_fc_one_bias, v_fc_one_bias, bias_grad, 0.0),
        adam_update(rel_table, m_rel_table, v_rel_table, table_grad, 0.0),
        adam_update(norm_vec, m_norm_vec, v_norm_vec, norm_grad, 0.0),
    ]
    return (out, x_grad, *[grp[k] for k in range(3) for grp in groups])


def solution(mesh):
    params = (
        P(None, "dp", None, "mp"), P(None, "mp", "dp"), P(None, "dp", "mp"), P(None, "mp", "dp"),
        P(None, None, "mp"), P(None, "mp"), P(None, None, "mp"), P(),
    )
    act = (P("dp", None, None), P("dp", None, None))
    return jax.shard_map(
        functools.partial(local, mesh.shape["dp"] == PEERS),
        mesh=mesh,
        in_specs=(*act, P("dp"), P(), *params, *params, *params),
        out_specs=(*act, *params, *params, *params),
        check_vma=False,
    )
```

```python
import functools

import jax
import jax.numpy as jnp
import numpy as np
from jax import lax
from jax.experimental import pallas as pl
from jax.experimental.pallas import tpu as pltpu
from jax.sharding import PartitionSpec as P

D = 512
HD = 32
SIDE = 14
WIN = 7
SHIFT = 3
SEQ = 196
WSEQ = 49
TABLE = 169
LAYERS = 2
SEQP = 200
PAIR = 2
ROWS = PAIR * SEQP
WROW = 64
WIMG = 4 * WROW
WPAIR = PAIR * WIMG
HALF = 256
GROUP = 4
GROUPS = 4
QUAD = GROUP * HD
LANES = GROUP * WROW
FFH = 1024
QKV = 3 * HALF
COLS = 2 * FFH + QKV + HALF
ATT = 2 * FFH

norm_eps = 1e-05
mask_fill = -100.0
pad_fill = -1e30
beta_one = 0.9
beta_two = 0.999
adam_eps = 1e-08
learn_rate = 0.02
decay_rate = 0.05
adam_step = 3.0
root_half = 0.7071067811865476
inv_root_two_pi = 0.3989422804014327
score_scale = HD**-0.5
log2_e = 1.4426950408889634

f32 = jnp.float32
bf16 = jnp.bfloat16


def dot(a, b, ca=1, cb=0):
    return lax.dot_general(a, b, (((ca,), (cb,)), ((), ())), preferred_element_type=f32)


def window_tokens(shifted):
    off = SHIFT if shifted else 0
    out = np.zeros((4, WSEQ), np.int64)
    for wr in range(2):
        for wc in range(2):
            for p in range(WSEQ):
                r = (7 * wr + p // 7 + off) % SIDE
                c = (7 * wc + p % 7 + off) % SIDE
                out[wr * 2 + wc, p] = r * SIDE + c
    return out


def permutation(shifted):
    tok = window_tokens(shifted)
    perm = np.zeros((WIMG, SEQP), np.float32)
    for w in range(4):
        perm[w * WROW + np.arange(WSEQ), tok[w]] = 1.0
    return perm


def region_mask():
    pos = np.arange(SIDE)
    band = (pos >= SIDE - WIN).astype(int) + (pos >= SIDE - SHIFT).astype(int)
    region = 3 * band[:, None] + band[None, :]
    win = region.reshape(2, WIN, 2, WIN).transpose(0, 2, 1, 3).reshape(4, WSEQ)
    out = np.zeros((4, WROW, WROW), np.float32)
    out[:, :WSEQ, :WSEQ] = np.where(win[:, :, None] != win[:, None, :], mask_fill, 0.0)
    return out


def norm_stats(z):
    mean = jnp.mean(z, -1, keepdims=True)
    cen = z - mean
    var = jnp.mean(cen * cen, -1, keepdims=True)
    inv = lax.rsqrt(var + norm_eps)
    return cen * inv, inv


def norm_back(e, hat, inv, gain):
    s = e * gain
    return inv * (s - jnp.mean(s, -1, keepdims=True) - hat * jnp.mean(s * hat, -1, keepdims=True))


def row_sum(v):
    return jnp.sum(v, 0, keepdims=True)


def put_images(ref, rows, blk, scale=lambda im, v: v):
    part = ref.at[rows, :]
    for im in range(PAIR):
        part[im * SEQP : im * SEQP + SEQ, :] = scale(im, blk[im].astype(f32))
        part[im * SEQP + SEQ : (im + 1) * SEQP, :] = jnp.zeros((SEQP - SEQ, D), f32)


def flat(v):
    return v.reshape(D, v.shape[-1])


def to_window_rows(perm, rows, out_ref):
    for im in range(PAIR):
        part = rows[im * SEQP : (im + 1) * SEQP].astype(bf16)
        out_ref[im * WIMG : (im + 1) * WIMG, :] = dot(perm, part).astype(bf16)


def to_token_rows(perm_t, ref):
    return jnp.concatenate(
        [dot(perm_t, ref[im * WIMG : (im + 1) * WIMG, :]) for im in range(PAIR)], 0
    ).astype(bf16)


def expand_heads(x, hm_ref):
    return jnp.concatenate([x * hm_ref[h : h + 1, :] for h in range(GROUP)], 0)


def fold_heads(o):
    lane = lax.broadcasted_iota(jnp.int32, (WROW, QUAD), 1) // HD
    acc = o[:WROW]
    for h in range(1, GROUP):
        acc = jnp.where(lane == h, o[h * WROW : (h + 1) * WROW], acc)
    return acc


def staged(stages, count, lag):
    for t in range(count + lag * (len(stages) - 1)):
        for n, stage in enumerate(stages):
            if 0 <= t - lag * n < count:
                stage(t - lag * n)


def softmax_cols(s):
    e = jnp.exp2((s - jnp.max(s, 0, keepdims=True)) * (score_scale * log2_e))
    return e * (1.0 / jnp.sum(e, 0, keepdims=True))


def group_cols(g):
    base = (g // 2) * QKV + (g % 2) * QUAD
    return [slice(base + t * HALF, base + t * HALF + QUAD) for t in range(3)]


def attend_forward(x, wa, bias_ref, layer, qvb_ref, nv_ref, perm, perm_t, hm_ref, qkv_ref, mixed_ref,
                   nperm, mixw, sc, prc, at):
    hat, _ = norm_stats(x)
    normed = hat * nv_ref[0:1, :] + nv_ref[1:2, :]
    to_window_rows(perm, normed, nperm)
    for m in range(2):
        r = dot(nperm[...], flat(wa[m, ..., :QKV]))
        qkv_ref[:, m * QKV : (m + 1) * QKV] = (r + qvb_ref[m : m + 1, :]).astype(bf16)
    at("attend", 1)
    units = [(w, g) for w in range(4 * PAIR) for g in range(GROUPS)]

    def scores(t):
        w, g = units[t]
        r = slice(w * WROW, (w + 1) * WROW)
        cq, ck, _ = group_cols(g)
        sc[t % SLOTS] = dot(qkv_ref[r, ck], expand_heads(qkv_ref[r, cq], hm_ref), 1, 1) + bias_ref[layer * (1 + w % 4), g]

    def middle(t):
        prc[t % SLOTS] = softmax_cols(sc[t % SLOTS]).astype(bf16)

    def mix(t):
        w, g = units[t]
        r = slice(w * WROW, (w + 1) * WROW)
        o = dot(prc[t % SLOTS], qkv_ref[r, group_cols(g)[2]], 0, 0)
        mixw[r, g * QUAD : (g + 1) * QUAD] = fold_heads(o).astype(bf16)

    staged((scores, middle, mix), len(units), LAG)
    mixed = to_token_rows(perm_t, mixw)
    mixed_ref[...] = mixed
    attn = dot(mixed[:, :HALF], flat(wa[0, ..., QKV:]), 1, 1) + dot(mixed[:, HALF:], flat(wa[1, ..., QKV:]), 1, 1)
    return x + attn + nv_ref[4:5, :]


CH = 512
SLOTS = 8
LAG = 2


def mlp_forward(mid, wm, b1_ref, nv_ref, act_ref, slope_ref, at):
    hat, _ = norm_stats(mid)
    hid = (hat * nv_ref[2:3, :] + nv_ref[3:4, :]).astype(bf16)
    total = jnp.zeros((ROWS, D), f32)
    for m in range(2):
        for c in range(0, FFH, CH):
            col = m * FFH + c
            u = dot(hid, flat(wm[m, ..., c : c + CH])) + b1_ref[:, col : col + CH]
            t = u * root_half
            phi = 0.5 + 0.5 * lax.erf(t)
            act = (u * phi).astype(bf16)
            act_ref[:, col : col + CH] = act
            slope_ref[:, col : col + CH] = (phi + u * (jnp.exp2(t * t * -log2_e) * inv_root_two_pi)).astype(bf16)
            total += dot(act, flat(wm[m, ..., FFH + c : FFH + c + CH]), 1, 1)
        if m == 0:
            at("mlp", 1)
    return mid + total + nv_ref[5:6, :]


def mlp_backward(g_s, mid, wm, nv_ref, gp, hid_s, gb_s, rows, b1_acc, nv_acc, at):
    gout = g_s[rows, :]
    hat, inv = norm_stats(mid)
    hid_s[rows, :] = (hat * nv_ref[2:3, :] + nv_ref[3:4, :]).astype(bf16)
    gb = gout.astype(bf16)
    gb_s[rows, :] = gb
    ghid = jnp.zeros((ROWS, D), f32)
    for m in range(2):
        for c in range(0, FFH, CH):
            col = m * FFH + c
            g = dot(gb, flat(wm[m, ..., FFH + c : FFH + c + CH])) * gp[rows, col : col + CH].astype(f32)
            b1_acc[:, col : col + CH] += row_sum(g)
            g = g.astype(bf16)
            gp[rows, col : col + CH] = g
            ghid += dot(g, flat(wm[m, ..., c : c + CH]), 1, 1)
        if m == 0:
            at("mlp", 1)
    gmid = gout + norm_back(ghid, hat, inv, nv_ref[2:3, :])
    nv_acc[2:3, :] += row_sum(ghid * hat)
    nv_acc[3:4, :] += row_sum(ghid)
    nv_acc[4:5, :] += row_sum(gmid)
    nv_acc[5:6, :] += row_sum(gout)
    g_s[rows, :] = gmid


def attend_backward(g_s, x, wa, bias_ref, layer, nv_ref, perm, perm_t, hm_ref, qkv_ref,
                    mperm, gmw, gqw, gq_s, mb_s, nb_s, rows, ds_acc, qv_acc, nv_acc, sc, dpc, prc, dsc, at):
    gmid = g_s[rows, :]
    hat, inv = norm_stats(x)
    nb_s[rows, :] = (hat * nv_ref[0:1, :] + nv_ref[1:2, :]).astype(bf16)
    mb_s[rows, :] = gmid.astype(bf16)
    to_window_rows(perm, gmid, mperm)
    for m in range(2):
        gmw[:, m * HALF : (m + 1) * HALF] = dot(mperm[...], flat(wa[m, ..., QKV:])).astype(bf16)
    at("attend", 1)
    units = [(w, g) for w in range(4 * PAIR) for g in range(GROUPS)]

    def scores(t):
        w, g = units[t]
        r = slice(w * WROW, (w + 1) * WROW)
        cq, ck, cv = group_cols(g)
        sc[t % SLOTS] = dot(qkv_ref[r, ck], expand_heads(qkv_ref[r, cq], hm_ref), 1, 1) + bias_ref[layer * (1 + w % 4), g]
        dpc[t % SLOTS] = dot(qkv_ref[r, cv], expand_heads(gmw[r, g * QUAD : (g + 1) * QUAD], hm_ref), 1, 1)

    def middle(t):
        g = units[t][1]
        pr = softmax_cols(sc[t % SLOTS])
        prc[t % SLOTS] = pr.astype(bf16)
        dp = dpc[t % SLOTS]
        ds = pr * (dp - jnp.sum(pr * dp, 0, keepdims=True))
        ds_acc[g] += ds
        dsc[t % SLOTS] = ds.astype(bf16)

    def grads(t):
        w, g = units[t]
        r = slice(w * WROW, (w + 1) * WROW)
        cq, ck, cv = group_cols(g)
        own = slice(g * QUAD, (g + 1) * QUAD)
        gv = dot(prc[t % SLOTS], expand_heads(gmw[r, own], hm_ref))
        gk = dot(dsc[t % SLOTS], expand_heads(qkv_ref[r, cq], hm_ref)) * score_scale
        gq = fold_heads(dot(dsc[t % SLOTS], qkv_ref[r, ck], 0, 0)) * score_scale
        qv_acc[0:1, own] += row_sum(gq)
        qv_acc[1:2, own] += row_sum(gv)
        gqw[r, cq] = gq.astype(bf16)
        gqw[r, ck] = gk.astype(bf16)
        gqw[r, cv] = gv.astype(bf16)

    staged((scores, middle, grads), len(units), LAG)
    at("attend", 2)
    gq = to_token_rows(perm_t, gqw)
    gq_s[rows, :] = gq
    gnorm = dot(gq[:, :QKV], flat(wa[0, ..., :QKV]), 1, 1) + dot(gq[:, QKV:], flat(wa[1, ..., :QKV]), 1, 1)
    nv_acc[0:1, :] += row_sum(gnorm * hat)
    nv_acc[1:2, :] += row_sum(gnorm)
    g_s[rows, :] = g_s[rows, :] + norm_back(gnorm, hat, inv, nv_ref[0:1, :])


def forward_kernel(fast, steps, tok_ref, wa_in, wm_in, bias_ref, qvb_ref, b1_ref, nv_ref, perm_ref, perm_t_ref, hm_ref,
                   out_ref, ys_ref, mid_ref, qkv_ref, mixed_ref, act_ref, slope_ref, wa_out, wm_out,
                   xs, mids, wa, wm, nperm, mixw, sc, prc, local, *sems):
    s = pl.program_id(0)
    per = 2 * steps
    layer, r = s // per, lax.rem(s, per)
    pair = lax.rem(r, steps)
    rows = pl.ds(pl.multiple_of(pair * ROWS, ROWS), ROWS)
    weights = (wa, wm)
    if fast:
        send, recv = sems
        own = (wa_in, wm_in)
        gathers = [
            Gather(own[n % 2].at[n // 2], weights[n % 2].at[n // 2], send.at[n], recv.at[n], local.at[n])
            for n in range(2 * LAYERS)
        ]

    def keep(n):
        return pltpu.make_async_copy(weights[n % 2].at[n // 2], (wa_out, wm_out)[n % 2].at[n // 2], local.at[4 + n])

    def at(step, point):
        if not fast:
            return
        for key, todo in FORWARD_PLAN.items():
            if key[1] == point and (key[0] % per < steps) == (step == "attend"):

                @pl.when(s == key[0])
                def _():
                    for n, stage in todo:
                        gathers[n].stage(stage)
                        if stage == Gather.STAGES - 1:
                            keep(n).start()

    @pl.when(s == 0)
    def _():
        if fast:
            neighbour_barrier(Place())
        else:
            for n in range(2 * LAYERS):
                src = (wa_in, wm_in)[n % 2].at[n // 2]
                cp = pltpu.make_async_copy(src, weights[n % 2].at[n // 2], local.at[n])
                cp.start()
                cp.wait()

    @pl.when(r < steps)
    def _():
        at("attend", 0)

        @pl.when(s < steps)
        def _():
            put_images(xs, rows, tok_ref)

        mid = attend_forward(xs[rows, :], wa.at[layer], bias_ref, layer, qvb_ref.at[layer], nv_ref.at[layer],
                             perm_ref[layer], perm_t_ref[layer], hm_ref, qkv_ref, mixed_ref, nperm, mixw, sc, prc, at)
        mid_ref[...] = mid
        mids[rows, :] = mid
        at("attend", 2)

    @pl.when(r >= steps)
    def _():
        at("mlp", 0)
        y = mlp_forward(mids[rows, :], wm.at[layer], b1_ref.at[layer], nv_ref.at[layer], act_ref, slope_ref, at)

        @pl.when(layer < LAYERS - 1)
        def _():
            xs[rows, :] = y
            ys_ref[...] = y

        @pl.when(layer == LAYERS - 1)
        def _():
            for im in range(PAIR):
                out_ref[im] = y[im * SEQP : im * SEQP + SEQ]

    @pl.when(s == LAYERS * per - 1)
    def _():
        if fast:
            for n in range(2 * LAYERS):
                keep(n).wait()


FORWARD_PLAN = {
    (0, 0): [(0, 0), (0, 1), (0, 2), (0, 3), (0, 4), (0, 5), (1, 0), (0, 6)],
    (0, 1): [(1, 1)],
    (0, 2): [(1, 2)],
    (1, 1): [(1, 3)],
    (2, 1): [(1, 4)],
    (2, 2): [(1, 5)],
    (3, 0): [(2, 0), (1, 6)],
    (3, 1): [(2, 1)],
    (4, 0): [(2, 2)],
    (4, 1): [(2, 3), (3, 0)],
    (5, 0): [(2, 4), (3, 1)],
    (5, 1): [(2, 5), (3, 2)],
    (6, 0): [(2, 6)],
    (6, 1): [(3, 3)],
    (7, 1): [(3, 4)],
    (8, 1): [(3, 5)],
    (9, 0): [(3, 6)],
}


def backward_kernel(fast, steps, cot_ref, tok_ref, ys_ref, mid_ref, qkv_ref, act_in, slope_in, mixed_in, wa_in, wm_in,
                    bias_ref, nv_ref, perm_ref, perm_t_ref, hm_ref, live_ref, *refs):
    if fast:
        gx_ref, ga_out, sum_m, sum_a, *refs = refs
    else:
        gx_ref, ga_out, gm_out, *refs = refs
    (qv_all, b1_all, ds_all, nv_all, g_s, xs, mperm, gmw, gqw, gp, gq_s, hid_s, gb_s, mb_s, nb_s, act_s, mixed_s,
     wa, wm, gwm, gwa, sc, dpc, prc, dsc, local, *comm) = refs
    s = pl.program_id(0)
    per = 2 * steps + 6
    turn, r = s // per, lax.rem(s, per)
    layer = LAYERS - 1 - turn
    first_g, first_a, last_g = steps, steps + 4, 2 * steps + 4
    pair = jnp.where(r < first_a, jnp.minimum(r, steps - 1), jnp.minimum(r - first_a, steps - 1))
    rows = pl.ds(pl.multiple_of(pair * ROWS, ROWS), ROWS)
    total = steps * ROWS
    qv_acc, b1_acc, ds_acc, nv_acc, nv_ref = (
        ref.at[layer] for ref in (qv_all, b1_all, ds_all, nv_all, nv_ref)
    )
    me = lax.axis_index("mp")
    if fast:
        scatters = (Scatter(gwm.at[0], gwm.at[1], *comm[:9]), Scatter(gwa.at[0], gwa.at[1], *comm[9:]))
        sums = (sum_m, sum_a)
        pl.when(s == 0)(lambda: neighbour_barrier(Place()))

    def at(step, point):
        if not fast:
            return
        spans = {"mlp": (0, first_g), "g": (first_g, first_a), "attend": (first_a, last_g), "ga": (last_g, per)}
        for key, todo in BACKWARD_PLAN.items():
            lo, hi = spans[step]
            if key[1] == point and lo <= key[0] % per < hi:

                @pl.when(s == key[0])
                def _():
                    for n, stage in todo:
                        if stage == Scatter.STAGES - 1:
                            scatters[n].result(sums[n].at[LAYERS - 1 - (key[0] - 1) // per if n == 0 else 0])
                        scatters[n].stage(stage)

    def rows_of(l):
        return pl.ds(l * total, total)

    def load(name, l):
        src, dst, n = {
            "wm": (wm_in.at[l], wm, 0), "wa": (wa_in.at[l], wa, 1), "act": (act_in.at[rows_of(l)], act_s, 2),
            "mixed": (mixed_in.at[rows_of(l)], mixed_s, 3), "slope": (slope_in.at[rows_of(l)], gp, 4),
        }[name]
        return pltpu.make_async_copy(src, dst, local.at[n])

    top = LAYERS - 1

    @pl.when(s == 0)
    def _():
        for name in ("wm", "slope", "wa", "act", "mixed"):
            load(name, top).start()

    for l in range(top, -1, -1):
        base = (top - l) * per
        for name, step in (("wm", 0), ("slope", 0), ("act", first_g), ("wa", first_a), ("mixed", last_g)):
            pl.when(s == base + step)(lambda name=name, l=l: load(name, l).wait())
        if l > 0:
            for name, step in (("wm", first_g), ("slope", first_a), ("act", first_a), ("wa", last_g), ("mixed", per)):
                pl.when(s == base + step)(lambda name=name, l=l: load(name, l - 1).start())

    @pl.when(r == 0)
    def _():
        for ref in (qv_acc, b1_acc, ds_acc, nv_acc):
            ref[...] = jnp.zeros(ref.shape, f32)

    @pl.when(r < first_g)
    def _():
        at("mlp", 0)

        @pl.when(turn == 0)
        def _():
            put_images(g_s, rows, cot_ref, lambda im, v: v * jnp.concatenate([live_ref[im : im + 1, :]] * 4, 1))

        mlp_backward(g_s, mid_ref[...], wm, nv_ref, gp, hid_s, gb_s, rows, b1_acc, nv_acc, at)

    def gradient(left, right, lo, width):
        cols = pl.ds(pl.multiple_of(lo, width), width)
        return dot(left[...], right[:, cols], 0, 0).astype(bf16).reshape(*gwm.shape[1:-1], width)

    @pl.when((r >= first_g) & (r < first_a))
    def _():
        at("g", 0)
        q = r - first_g
        own = q // 2
        half = jnp.where(own == 1, me, 1 - me)

        @pl.when(lax.rem(q, 2) == 0)
        def _():
            gwm[own, ..., :FFH] = gradient(hid_s, gp, half * FFH, FFH)

        @pl.when(lax.rem(q, 2) == 1)
        def _():
            gwm[own, ..., FFH:] = gradient(gb_s, act_s, half * FFH, FFH)

        at("g", 1)

    @pl.when((r >= first_a) & (r < last_g))
    def _():
        at("attend", 0)

        @pl.when(layer == 0)
        def _():
            put_images(xs, slice(None), tok_ref)

        @pl.when(layer > 0)
        def _():
            xs[...] = ys_ref[...]

        attend_backward(g_s, xs[...], wa, bias_ref, layer, nv_ref, perm_ref[layer], perm_t_ref[layer], hm_ref,
                        qkv_ref, mperm, gmw, gqw, gq_s, mb_s, nb_s, rows, ds_acc, qv_acc, nv_acc, sc, dpc, prc, dsc, at)

        @pl.when(layer == 0)
        def _():
            for im in range(PAIR):
                gx_ref[im] = g_s.at[rows, :][im * SEQP : im * SEQP + SEQ]

    @pl.when(r >= last_g)
    def _():
        at("ga", 0)
        own = r - last_g
        half = jnp.where(own == 1, me, 1 - me)
        gwa[own, ..., :QKV] = gradient(nb_s, gq_s, half * QKV, QKV)
        gwa[own, ..., QKV:] = gradient(mb_s, mixed_s, half * HALF, HALF)
        at("ga", 1)

    def flush(src, dst):
        cp = pltpu.make_async_copy(src, dst, local.at[5])
        cp.start()
        cp.wait()

    if fast:
        pl.when(s == LAYERS * per - 1)(lambda: flush(gwa, ga_out))
    else:
        pl.when(r == first_a)(lambda: flush(gwm, gm_out.at[layer]))
        pl.when(r == per - 1)(lambda: flush(gwa, ga_out.at[layer]))


BACKWARD_PLAN = {
    (5, 0): [(0, 0)],
    (7, 0): [(0, 1)],
    (8, 1): [(0, 2)],
    (9, 1): [(0, 3)],
    (10, 0): [(0, 4)],
    (11, 0): [(1, 0), (0, 5)],
    (12, 0): [(1, 1), (0, 6)],
    (13, 1): [(1, 2)],
    (14, 1): [(1, 3)],
    (15, 0): [(1, 4)],
    (16, 0): [(1, 5)],
    (17, 0): [(0, 0), (1, 6)],
    (19, 0): [(0, 1)],
    (20, 1): [(0, 2)],
    (21, 1): [(0, 3)],
    (21, 2): [(0, 4)],
    (22, 0): [(0, 5)],
    (23, 0): [(0, 6)],
}


def whole(shape, buffers=1):
    zero = (0,) * len(shape)
    return pl.BlockSpec(shape, lambda i: zero, pipeline_mode=pl.Buffered(buffers))


VLIM = 65000000


def forward(tok, wa, wm, bias, qvb, b1, nv, perm, perm_t, hm, fast, steps):
    per = 2 * steps
    rows = steps * ROWS
    slots = (2, NZ, NY, NX, D // PEERS) if fast else (2, 1, 1, 1, D)
    wide = (COLS - ATT, ATT)
    any_ = pl.BlockSpec(memory_space=pl.ANY)

    def attend(s):
        return s // per * steps + jnp.minimum(lax.rem(s, per), steps - 1)

    def mlp(s):
        return s // per * steps + jnp.maximum(lax.rem(s, per) - steps, 0)

    sems = [pltpu.SemaphoreType.DMA((2 * LAYERS, Gather.SEMS))] * 2 if fast else []
    params = dict(collective_id=1, has_side_effects=True) if fast else {}
    return pl.pallas_call(
        functools.partial(forward_kernel, fast, steps),
        name="forward",
        grid=(LAYERS * per,),
        in_specs=[
            pl.BlockSpec((PAIR, SEQ, D), lambda s: (jnp.minimum(s, steps - 1), 0, 0)),
            whole(wa.shape) if fast else any_, whole(wm.shape) if fast else any_,
            *(whole(a.shape) for a in (bias, qvb, b1, nv, perm, perm_t, hm)),
        ],
        out_specs=[
            pl.BlockSpec((PAIR, SEQ, D), lambda s: (jnp.maximum(s - (LAYERS * per - steps), 0), 0, 0)),
            pl.BlockSpec((ROWS, D), lambda s: (jnp.clip(s - steps, 0, steps - 1), 0)),
            pl.BlockSpec((ROWS, D), lambda s: (attend(s), 0)),
            pl.BlockSpec((WPAIR, 2 * QKV), lambda s: (attend(s), 0)),
            pl.BlockSpec((ROWS, D), lambda s: (attend(s), 0)),
            pl.BlockSpec((ROWS, 2 * FFH), lambda s: (mlp(s), 0)),
            pl.BlockSpec((ROWS, 2 * FFH), lambda s: (mlp(s), 0)),
            any_, any_,
        ],
        out_shape=[
            jax.ShapeDtypeStruct((steps * PAIR, SEQ, D), f32),
            jax.ShapeDtypeStruct((rows, D), f32),
            jax.ShapeDtypeStruct((LAYERS * rows, D), f32),
            jax.ShapeDtypeStruct((LAYERS * steps * WPAIR, 2 * QKV), bf16),
            jax.ShapeDtypeStruct((LAYERS * rows, D), bf16),
            jax.ShapeDtypeStruct((LAYERS * rows, 2 * FFH), bf16),
            jax.ShapeDtypeStruct((LAYERS * rows, 2 * FFH), bf16),
            *(jax.ShapeDtypeStruct((LAYERS, *slots, n), bf16) for n in wide),
        ],
        scratch_shapes=[
            pltpu.VMEM((rows, D), f32), pltpu.VMEM((rows, D), f32),
            *(pltpu.VMEM((LAYERS, *slots, n), bf16) for n in wide),
            pltpu.VMEM((WPAIR, D), bf16), pltpu.VMEM((WPAIR, D), bf16),
            pltpu.VMEM((SLOTS, WROW, LANES), f32), pltpu.VMEM((SLOTS, WROW, LANES), bf16),
            pltpu.SemaphoreType.DMA((8,)), *sems,
        ],
        compiler_params=pltpu.CompilerParams(vmem_limit_bytes=VLIM, **params),
    )(tok, wa, wm, bias, qvb, b1, nv, perm, perm_t, hm)


def backward(cot, tok, saved, weights, bias, nv, perm, perm_t, hm, live, fast, steps):
    ys, mid, qkv, mixed, act, slope = saved
    wa, wm = weights
    per = 2 * steps + 6
    rows = steps * ROWS
    slots = wa.shape[1:-1]
    rest = slots[1:]
    any_ = pl.BlockSpec(memory_space=pl.ANY)

    def clip(v):
        return jnp.clip(v, 0, steps - 1)

    def layer(s):
        return LAYERS - 1 - s // per

    attend0 = (LAYERS - 1) * per + steps + 4
    img = lambda at: pl.BlockSpec((PAIR, SEQ, D), lambda s: (clip(s - at), 0, 0))
    wide = (COLS - ATT, ATT)
    part = rest[-1]
    if fast:
        outs = [
            jax.ShapeDtypeStruct((2, *rest, COLS - ATT), bf16),
            jax.ShapeDtypeStruct((LAYERS, part, ATT), f32), jax.ShapeDtypeStruct((1, part, COLS - ATT), f32),
        ]
        specs = [any_, whole(outs[1].shape), whole(outs[2].shape)]
        comm = Scatter.landing(part, ATT) + Scatter.landing(part, COLS - ATT)
        params = dict(collective_id=2, has_side_effects=True)
    else:
        outs = [jax.ShapeDtypeStruct((LAYERS, 2, *rest, n), bf16) for n in wide]
        specs, comm, params = [any_, any_], [], {}
    small = [(LAYERS, 2, 2 * HALF), (LAYERS, 1, 2 * FFH), (LAYERS, GROUPS, WROW, LANES), (LAYERS, 8, D)]
    return pl.pallas_call(
        functools.partial(backward_kernel, fast, steps),
        name="backward",
        grid=(LAYERS * per,),
        in_specs=[
            img(0), img(attend0),
            pl.BlockSpec((ROWS, D), lambda s: (clip(s - steps - 4), 0)),
            pl.BlockSpec((ROWS, D), lambda s: (layer(s) * steps + clip(lax.rem(s, per)), 0)),
            pl.BlockSpec((WPAIR, 2 * QKV), lambda s: (layer(s) * steps + clip(lax.rem(s, per) - steps - 4), 0)),
            any_, any_, any_, any_, any_,
            *(whole(a.shape) for a in (bias, nv, perm, perm_t, hm)),
            pl.BlockSpec((None, PAIR, 128), lambda s: (clip(s), 0, 0)),
        ],
        out_specs=[img(attend0), *specs, *(whole(n) for n in small)],
        out_shape=[
            jax.ShapeDtypeStruct((steps * PAIR, SEQ, D), f32), *outs, *(jax.ShapeDtypeStruct(n, f32) for n in small),
        ],
        scratch_shapes=[
            pltpu.VMEM((rows, D), f32), pltpu.VMEM((ROWS, D), f32),
            pltpu.VMEM((WPAIR, D), bf16), pltpu.VMEM((WPAIR, D), bf16), pltpu.VMEM((WPAIR, 2 * QKV), bf16),
            pltpu.VMEM((rows, 2 * FFH), bf16), pltpu.VMEM((rows, 2 * QKV), bf16),
            *[pltpu.VMEM((rows, D), bf16)] * 4,
            pltpu.VMEM((rows, 2 * FFH), bf16), pltpu.VMEM((rows, D), bf16),
            *(pltpu.VMEM((*slots, n), bf16) for n in wide),
            pltpu.VMEM((2, *rest, ATT), bf16), pltpu.VMEM((2, *rest, COLS - ATT), bf16),
            *[pltpu.VMEM((SLOTS, WROW, LANES), f32)] * 2, *[pltpu.VMEM((SLOTS, WROW, LANES), bf16)] * 2,
            pltpu.SemaphoreType.DMA((8,)), *comm,
        ],
        compiler_params=pltpu.CompilerParams(vmem_limit_bytes=VLIM, **params),
    )(cot, tok, ys, mid, qkv, act, slope, mixed, wa, wm, bias, nv, perm, perm_t, hm, live)


def head_mask():
    return (np.arange(QUAD)[None, :] // HD == np.arange(GROUP)[:, None]).astype(np.float32)


def bias_cols(onehot, table):
    picked = jnp.einsum("jti,mlth->lmjhi", onehot, table, precision=lax.Precision.HIGHEST)
    picked = picked.reshape(LAYERS, 2, WROW, 2, GROUP, WROW).transpose(0, 1, 3, 2, 4, 5)
    picked = picked.reshape(LAYERS, GROUPS, WROW, GROUP, WROW)
    apart = np.concatenate([np.zeros((1, WROW, WROW), np.float32), region_mask()])
    apart[:, WSEQ:] = pad_fill
    both = jnp.concatenate([picked[:1], jnp.broadcast_to(picked[1:], (4, *picked.shape[1:]))])
    both = (both + jnp.asarray(apart)[:, None, :, None, :]) * (1.0 / score_scale)
    return both.reshape(-1, GROUPS, WROW, LANES)

NZ, NY, NX = 4, 2, 2
PEERS = NZ * NY * NX
MESH_ID = pl.DeviceIdType.MESH


class Place:
    def __init__(self):
        d = lax.axis_index("dp")
        self.d, self.m = d, lax.axis_index("mp")
        self.z, self.y, self.x = d // 4, lax.rem(d // 2, 2), lax.rem(d, 2)

    def chip(self, z, y, x):
        return (z * NY + y) * NX + x

    def at(self, dz=0, y=None, x=None, m=None):
        y = self.y if y is None else y
        x = self.x if x is None else x
        return (self.chip(self.z + dz, y, x), self.m if m is None else m)

    def xn(self):
        return self.at(x=1 - self.x)

    def yn(self):
        return self.at(y=1 - self.y)

    def core(self):
        return self.at(m=1 - self.m)

    def zn(self, step):
        return self.at(dz=step)

    def has(self, step):
        return self.z < NZ - 1 if step > 0 else self.z > 0


def remote(src, dst, send, recv, to):
    return pltpu.make_async_remote_copy(
        src_ref=src, dst_ref=dst, send_sem=send, recv_sem=recv, device_id=to, device_id_type=MESH_ID
    )


def neighbour_barrier(p, far=False):
    sem = pltpu.get_barrier_semaphore()

    def tell(to):
        pl.semaphore_signal(sem, inc=1, device_id=to, device_id_type=MESH_ID)

    for to in (p.xn(), p.yn(), p.core()):
        tell(to)
    count = 3
    for step in (1, -1):
        pl.when(p.has(step))(lambda step=step: tell(p.zn(step)))
        count = count + p.has(step).astype(jnp.int32)
    if far:
        tell((p.chip((p.z + 2) % NZ, p.y, p.x), p.m))
        count = count + 1
    pl.semaphore_wait(sem, count)


class Gather:
    SEMS = 52
    BASE = {"z": 0, "xa": 8, "yb": 12, "ya0": 16, "ya1": 20, "xb0": 24, "xb1": 28,
            "own": 32, "ax": 36, "by": 40, "ar": 44, "br": 48}

    def __init__(self, own, full, send, recv, local):
        self.p, self.own, self.full = Place(), own, full
        self.send, self.recv, self.local = send, recv, local
        half = full.shape[-1] // 2
        self.all, self.a, self.b = pl.ds(0, 2 * half), pl.ds(0, half), pl.ds(half, half)

    def region(self, kind, k, arrived):
        p = self.p
        oy, ox = 1 - p.y, 1 - p.x
        if kind == "z":
            return (p.m, k, p.y, p.x), self.all, None
        if kind == "xa":
            return (p.m, k, p.y, ox if arrived else p.x), self.a, p.xn()
        if kind == "yb":
            return (p.m, k, oy if arrived else p.y, p.x), self.b, p.yn()
        if kind in ("ya0", "ya1"):
            return (p.m, k, oy if arrived else p.y, p.x if kind == "ya0" else ox), self.a, p.yn()
        if kind in ("xb0", "xb1"):
            return (p.m, k, p.y if kind == "xb0" else oy, ox if arrived else p.x), self.b, p.xn()
        m = 1 - p.m if arrived else p.m
        if kind == "own":
            return (m, k, p.y, p.x), self.all, p.core()
        if kind == "ax":
            return (m, k, p.y, ox), self.a, p.core()
        if kind == "by":
            return (m, k, oy, p.x), self.b, p.core()
        if kind == "ar":
            return (m, k, oy, slice(None)), self.a, p.core()
        return (m, k, slice(None), ox), self.b, p.core()

    def copy(self, kind, k, own=False, arrived=False, step=0):
        at, cols, to = self.region(kind, k, arrived)
        dst = self.full.at[(*at, slice(None), cols)]
        src = self.own.at[:, cols] if own else dst
        s = self.BASE[kind] + k
        r = s
        if kind == "z":
            to = self.p.zn(step)
            s = s + (4 if step < 0 else 0)
        return remote(src, dst, self.send.at[s], self.recv.at[r], to)

    def keep(self):
        p = self.p
        return pltpu.make_async_copy(
            self.own.at[:, self.all], self.full.at[p.m, p.z, p.y, p.x, :, self.all], self.local
        )

    def fan(self, k, own=False):
        for kind in ("xa", "yb", "ya0", "xb0", "own"):
            self.copy(kind, k, own).start()

    def stage(self, n):
        p = self.p
        if n == 0:
            self.keep().start()
            for step in (1, -1):
                pl.when(p.has(step))(lambda step=step: self.copy("z", p.z, True, step=step).start())
            self.fan(p.z, True)
        elif n <= 3:
            for step in (1, -1):
                k = p.z - step * n
                inside = k >= 0 if step > 0 else k < NZ

                @pl.when(inside)
                def _():
                    self.copy("z", k, arrived=True, step=step).wait_recv()
                    pl.when(p.has(step))(lambda: self.copy("z", k, step=step).start())
                    self.fan(k)
        elif n == 4:
            for k in range(NZ):
                self.copy("xa", k, arrived=True).wait_recv()
                for kind in ("ya1", "ax"):
                    self.copy(kind, k).start()
                self.copy("yb", k, arrived=True).wait_recv()
                for kind in ("xb1", "by"):
                    self.copy(kind, k).start()
        elif n == 5:
            for k in range(NZ):
                for kind, rest in (("ya", "ar"), ("xb", "br")):
                    for rel in ("0", "1"):
                        self.copy(kind + rel, k, arrived=True).wait_recv()
                    self.copy(rest, k).start()
        else:
            for k in range(NZ):
                for kind in ("own", "ax", "by", "ar", "br"):
                    self.copy(kind, k, arrived=True).wait_recv()
                for kind in self.BASE:
                    if kind != "z":
                        self.copy(kind, k).wait_send()
                pl.when((k <= p.z) & p.has(1))(lambda: self.copy("z", k, step=1).wait_send())
                pl.when((k >= p.z) & p.has(-1))(lambda: self.copy("z", k, step=-1).wait_send())
            self.keep().wait()

    STAGES = 7


def add_into(ref, at, other):
    ref[at] = (ref[at].astype(f32) + other.astype(f32)).astype(bf16)


class Scatter:
    SEMS = 28
    BASE = {"core": 0, "ya": 4, "xb": 8, "xa": 12, "yb": 16, "up": 20, "down": 24}

    @staticmethod
    def landing(rows, cols):
        half = cols // 2
        return [
            pltpu.VMEM((NZ, NY, NX, rows, cols), bf16),
            pltpu.VMEM((NZ, NX, rows, half), bf16), pltpu.VMEM((NZ, NY, rows, half), bf16),
            pltpu.VMEM((NZ, rows, half), bf16), pltpu.VMEM((NZ, rows, half), bf16),
            pltpu.VMEM((NZ, rows, cols), bf16), pltpu.VMEM((NZ, rows, cols), bf16),
            pltpu.SemaphoreType.DMA((Scatter.SEMS,)), pltpu.SemaphoreType.DMA((Scatter.SEMS,)),
        ]

    def __init__(self, give, part, other, ya, xb, xa, yb, up, down, send, recv):
        self.p, self.give, self.part, self.other = Place(), give, part, other
        self.land = {"ya": ya, "xb": xb, "xa": xa, "yb": yb, "up": up, "down": down}
        self.send, self.recv = send, recv
        half = part.shape[-1] // 2
        self.a, self.b = pl.ds(0, half), pl.ds(half, half)

    def copy(self, kind, k):
        p = self.p
        oy, ox = 1 - p.y, 1 - p.x
        full = slice(None)
        if kind == "core":
            src, dst, to = self.give.at[k], self.other.at[k], p.core()
        else:
            at, to = {
                "ya": ((k, oy, full, full, self.a), p.yn()),
                "xb": ((k, full, ox, full, self.b), p.xn()),
                "xa": ((k, p.y, ox, full, self.a), p.xn()),
                "yb": ((k, oy, p.x, full, self.b), p.yn()),
                "up": ((k, p.y, p.x, full, full), p.zn(1)),
                "down": ((k, p.y, p.x, full, full), p.zn(-1)),
            }[kind]
            src, dst = self.part.at[at], self.land[kind].at[k]
        s = self.BASE[kind] + k
        return remote(src, dst, self.send.at[s], self.recv.at[s], to)

    def pass_on(self, step):
        p = self.p
        kind = "up" if step > 0 else "down"
        for dist in range(NZ - 1, 0, -1):
            k = p.z + step * dist

            @pl.when((k < NZ) & (k >= 0))
            def _():
                @pl.when(p.has(-step))
                def _():
                    self.copy(kind, k).wait_recv()
                    add_into(self.part, (k, p.y, p.x), self.land[kind][k])

                self.copy(kind, k).start()

    def stage(self, n):
        p = self.p
        oy, ox = 1 - p.y, 1 - p.x
        if n == 0:
            for k in range(NZ):
                self.copy("core", k).start()
        elif n == 1:
            for k in range(NZ):
                self.copy("core", k).wait_recv()
                for y in range(NY):
                    for x in range(NX):
                        add_into(self.part, (k, y, x), self.other[k, y, x])
                self.copy("ya", k).start()
                self.copy("xb", k).start()
        elif n == 2:
            for k in range(NZ):
                self.copy("ya", k).wait_recv()
                for x in range(NX):
                    add_into(self.part, (k, p.y, x, slice(None), self.a), self.land["ya"][k, x])
                self.copy("xa", k).start()
                self.copy("xb", k).wait_recv()
                for y in range(NY):
                    add_into(self.part, (k, y, p.x, slice(None), self.b), self.land["xb"][k, y])
                self.copy("yb", k).start()
        elif n == 3:
            for k in range(NZ):
                self.copy("xa", k).wait_recv()
                add_into(self.part, (k, p.y, p.x, slice(None), self.a), self.land["xa"][k])
                self.copy("yb", k).wait_recv()
                add_into(self.part, (k, p.y, p.x, slice(None), self.b), self.land["yb"][k])
            pl.when(p.z == 0)(lambda: self.pass_on(1))
            pl.when(p.z == NZ - 1)(lambda: self.pass_on(-1))
        elif n in (4, 5):
            j = n - 3
            pl.when(p.z == j)(lambda: self.pass_on(1))
            pl.when(p.z == NZ - 1 - j)(lambda: self.pass_on(-1))
        else:
            for k in range(NZ):
                for kind in ("core", "ya", "xb", "xa", "yb"):
                    self.copy(kind, k).wait_send()
                pl.when(k > p.z)(lambda: self.copy("up", k).wait_send())
                pl.when(k < p.z)(lambda: self.copy("down", k).wait_send())

    STAGES = 7

    def result(self, out):
        p = self.p
        out[...] = self.part[p.z, p.y, p.x].astype(f32)
        for step, kind in ((1, "up"), (-1, "down")):

            @pl.when(p.has(-step))
            def _():
                self.copy(kind, p.z).wait_recv()
                out[...] += self.land[kind][p.z].astype(f32)


class Total:
    STEPS = 5

    @staticmethod
    def scratch(shape):
        return [
            pltpu.VMEM((Total.STEPS, *shape), f32), pltpu.VMEM((Total.STEPS, *shape), f32),
            pltpu.SemaphoreType.DMA((Total.STEPS,)), pltpu.SemaphoreType.DMA((Total.STEPS,)),
        ]

    def __init__(self, start, held, land, send, recv):
        self.p, self.start, self.held, self.land, self.send, self.recv = Place(), start, held, land, send, recv

    def copy(self, n):
        p = self.p
        pair = p.z + 1 - 2 * lax.rem(p.z, 2)
        far = lax.rem(p.z + 2, NZ)
        to = (p.core(), p.yn(), p.xn(), (p.chip(pair, p.y, p.x), p.m), (p.chip(far, p.y, p.x), p.m))[n]
        src = self.start if n == 0 else self.held.at[n - 1]
        return remote(src, self.land.at[n], self.send.at[n], self.recv.at[n], to)

    def stage(self, n):
        if n > 0:
            self.copy(n - 1).wait_recv()
            before = self.start[...] if n == 1 else self.held[n - 2]
            self.held[n - 1] = before + self.land[n - 1]
        if n < self.STEPS:
            self.copy(n).start()
        else:
            for k in range(self.STEPS):
                self.copy(k).wait_send()


def tail_kernel(grad_ref, small_ref, out_ref, small_out, part, *refs):
    neighbour_barrier(Place(), far=True)
    total = Total(small_ref, *refs[-4:])
    s = Scatter(grad_ref.at[0], part, *refs[:-4])
    part[...] = grad_ref[1]
    for n in range(Scatter.STAGES - 1):
        s.stage(n)
        total.stage(n)
    s.result(out_ref)
    s.stage(Scatter.STAGES - 1)
    small_out[...] = total.held[Total.STEPS - 1]


def tail(grad, small):
    rows, cols = grad.shape[-2:]
    vm = pl.BlockSpec(memory_space=pltpu.VMEM)
    return pl.pallas_call(
        tail_kernel,
        name="tail",
        out_shape=[jax.ShapeDtypeStruct((rows, cols), f32), jax.ShapeDtypeStruct(small.shape, f32)],
        in_specs=[vm] * 2,
        out_specs=[vm] * 2,
        scratch_shapes=[pltpu.VMEM(grad.shape[1:], bf16)] + Scatter.landing(rows, cols) + Total.scratch(small.shape),
        compiler_params=pltpu.CompilerParams(collective_id=3, has_side_effects=True, vmem_limit_bytes=VLIM),
    )(grad, small)


def adam_update(weight_in, moment_one, moment_two, grad_sum, decay):
    new_one = beta_one * moment_one + (1.0 - beta_one) * grad_sum
    new_two = beta_two * moment_two + (1.0 - beta_two) * grad_sum * grad_sum
    hat_one = new_one / (1.0 - beta_one**adam_step)
    hat_two = new_two / (1.0 - beta_two**adam_step)
    new_weight = weight_in - learn_rate * (hat_one / (jnp.sqrt(hat_two) + adam_eps) + decay * weight_in)
    return (new_weight, new_one, new_two)


def both_halves(mine, me):
    other = lax.ppermute(mine, "mp", [(0, 1), (1, 0)])
    low = jnp.where(me == 0, mine, other)
    high = jnp.where(me == 0, other, mine)
    return jnp.concatenate([low, high], 0)


HEADS = GROUPS * GROUP
LITTLE = 4 * HALF + 2 * FFH + HEADS * TABLE + 6 * D


def lanes_of(a):
    flat = a.reshape(-1)
    return jnp.pad(flat, (0, -flat.size % 1024)).reshape(-1, 128)


def sum_of_all(a):
    a = a.reshape(LAYERS, 2, D, a.shape[-1])
    total = a[:, 1].astype(f32) + lax.ppermute(a[:, 0], "mp", [(0, 1), (1, 0)]).astype(f32)
    return lax.psum_scatter(total.astype(bf16), "dp", scatter_dimension=1, tiled=True).astype(f32)


def pair_onehot(rel_index):
    index = jnp.pad(rel_index.T, ((0, WROW - WSEQ), (0, WROW - WSEQ)), constant_values=-1)
    return (index[:, None, :] == jnp.arange(TABLE, dtype=jnp.int32)[None, :, None]).astype(f32)


def local(
    fast, tokens, cotangent, image_count, rel_index,
    w_qkv, w_proj, w_fc_one, w_fc_two, qv_bias, fc_one_bias, rel_table, norm_vec,
    m_qkv, m_proj, m_fc_one, m_fc_two, m_qv_bias, m_fc_one_bias, m_rel_table, m_norm_vec,
    v_qkv, v_proj, v_fc_one, v_fc_two, v_qv_bias, v_fc_one_bias, v_rel_table, v_norm_vec,
):
    me = lax.axis_index("mp")
    images = tokens.shape[0]
    nimg = images // 2
    steps = nimg // PAIR
    part = w_qkv.shape[1]
    tok = lax.dynamic_slice_in_dim(tokens, me * nimg, nimg, 0)
    cot = lax.dynamic_slice_in_dim(cotangent, me * nimg, nimg, 0)
    live = (jnp.arange(nimg, dtype=jnp.int32) + me * nimg < image_count[0]).astype(f32)
    live = jnp.broadcast_to(live[:, None], (nimg, 128)).reshape(steps, PAIR, 128)

    wm = jnp.concatenate([w_fc_one, w_fc_two.transpose(0, 2, 1)], 2).astype(bf16)
    wa = jnp.concatenate([w_qkv.reshape(LAYERS, part, QKV), w_proj.transpose(0, 2, 1)], 2).astype(bf16)
    small = jnp.concatenate(
        [qv_bias.reshape(LAYERS, -1), fc_one_bias, rel_table.reshape(LAYERS, -1)], 1
    )
    small = both_halves(small[None], me)
    if not fast:
        wa, wm = (
            lax.all_gather(w, ("mp", "dp")).reshape(2, -1, LAYERS, part, w.shape[-1]).transpose(2, 0, 1, 3, 4)
            .reshape(LAYERS, 2, 1, 1, 1, D, w.shape[-1])
            for w in (wa, wm)
        )
    qvb = small[:, :, : 2 * HALF].reshape(2, LAYERS, 2, HALF).transpose(1, 0, 2, 3)
    b1 = small[:, :, 2 * HALF : 2 * HALF + FFH].transpose(1, 0, 2).reshape(LAYERS, 1, 2 * FFH)
    table = small[:, :, 2 * HALF + FFH :].reshape(2, LAYERS, TABLE, HEADS // 2)
    qvb = jnp.concatenate([qvb[:, :, 0], jnp.zeros_like(qvb[:, :, 0]), qvb[:, :, 1]], 2)

    onehot = pair_onehot(rel_index)
    bias = bias_cols(onehot, table)
    hm = jnp.asarray(head_mask(), bf16)
    perms = np.stack([permutation(layer % 2 == 1) for layer in range(LAYERS)])
    perm, perm_t = jnp.asarray(perms, bf16), jnp.asarray(perms.transpose(0, 2, 1), bf16)
    out, *saved, all_wa, all_wm = forward(tok, wa, wm, bias, qvb, b1, norm_vec, perm, perm_t, hm, fast, steps)
    if fast:
        wa, wm = all_wa, all_wm
    out = both_halves(out, me)
    g, *grads, gqv, gb1, ds, gnv = backward(
        cot, tok, saved, (wa, wm), bias, norm_vec, perm, perm_t, hm, live, fast, steps
    )
    x_grad = both_halves(g, me)
    ds = ds.reshape(LAYERS, GROUPS, WROW, GROUP, WROW)
    gt = jnp.einsum("lgjhi,jti->lght", ds, onehot, precision=lax.Precision.HIGHEST)
    little = jnp.concatenate([a.reshape(LAYERS, -1) for a in (gqv, gb1, gt, gnv[:, :6])], 1)
    if fast:
        ga, sum_m, sum_a = grads
        last, total = tail(ga, lanes_of(little))
        big_a, big_m = jnp.stack([last, sum_a[0]]), sum_m
        little = total.reshape(-1)[: LAYERS * LITTLE].reshape(LAYERS, LITTLE)
    else:
        big_a, big_m = (sum_of_all(a) for a in grads)
        little = lax.psum(little, ("dp", "mp"))
    one_grad = big_m[:, :, :FFH]
    two_grad = big_m[:, :, FFH:].transpose(0, 2, 1)
    qkv_grad = big_a[:, :, :QKV].reshape(LAYERS, part, 3, HALF)
    proj_grad = big_a[:, :, QKV:].transpose(0, 2, 1)
    cut = lambda a: lax.dynamic_index_in_dim(a, me, 1, keepdims=False)
    at = 2 * 2 * HALF
    qv_grad = cut(little[:, :at].reshape(LAYERS, 2, 2, HALF).transpose(0, 2, 1, 3))
    bias_grad = cut(little[:, at : at + 2 * FFH].reshape(LAYERS, 2, FFH))
    at += 2 * FFH
    table_grad = cut(little[:, at : at + HEADS * TABLE].reshape(LAYERS, 2, HEADS // 2, TABLE)).transpose(0, 2, 1)
    at += HEADS * TABLE
    norm_grad = little[:, at:].reshape(LAYERS, 6, D)
    groups = [
        adam_update(w_qkv, m_qkv, v_qkv, qkv_grad, decay_rate),
        adam_update(w_proj, m_proj, v_proj, proj_grad, decay_rate),
        adam_update(w_fc_one, m_fc_one, v_fc_one, one_grad, decay_rate),
        adam_update(w_fc_two, m_fc_two, v_fc_two, two_grad, decay_rate),
        adam_update(qv_bias, m_qv_bias, v_qv_bias, qv_grad, 0.0),
        adam_update(fc_one_bias, m_fc_one_bias, v_fc_one_bias, bias_grad, 0.0),
        adam_update(rel_table, m_rel_table, v_rel_table, table_grad, 0.0),
        adam_update(norm_vec, m_norm_vec, v_norm_vec, norm_grad, 0.0),
    ]
    return (out, x_grad, *[grp[k] for k in range(3) for grp in groups])


def solution(mesh):
    params = (
        P(None, "dp", None, "mp"), P(None, "mp", "dp"), P(None, "dp", "mp"), P(None, "mp", "dp"),
        P(None, None, "mp"), P(None, "mp"), P(None, None, "mp"), P(),
    )
    act = (P("dp", None, None), P("dp", None, None))
    return jax.shard_map(
        functools.partial(local, mesh.shape["dp"] == PEERS),
        mesh=mesh,
        in_specs=(*act, P("dp"), P(), *params, *params, *params),
        out_specs=(*act, *params, *params, *params),
        check_vma=False,
    )
```

```python
import functools

import jax
import jax.numpy as jnp
import numpy as np
from jax import lax
from jax.experimental import pallas as pl
from jax.experimental.pallas import tpu as pltpu
from jax.sharding import PartitionSpec as P

D = 512
HD = 32
SIDE = 14
WIN = 7
SHIFT = 3
SEQ = 196
WSEQ = 49
TABLE = 169
LAYERS = 2
SEQP = 200
PAIR = 2
ROWS = PAIR * SEQP
WROW = 64
WIMG = 4 * WROW
WPAIR = PAIR * WIMG
HALF = 256
GROUP = 4
GROUPS = 4
QUAD = GROUP * HD
LANES = GROUP * WROW
FFH = 1024
QKV = 3 * HALF
COLS = 2 * FFH + QKV + HALF
ATT = 2 * FFH

norm_eps = 1e-05
mask_fill = -100.0
pad_fill = -1e30
beta_one = 0.9
beta_two = 0.999
adam_eps = 1e-08
learn_rate = 0.02
decay_rate = 0.05
adam_step = 3.0
root_half = 0.7071067811865476
inv_root_two_pi = 0.3989422804014327
score_scale = HD**-0.5
log2_e = 1.4426950408889634

f32 = jnp.float32
bf16 = jnp.bfloat16


def dot(a, b, ca=1, cb=0):
    return lax.dot_general(a, b, (((ca,), (cb,)), ((), ())), preferred_element_type=f32)


def window_tokens(shifted):
    off = SHIFT if shifted else 0
    out = np.zeros((4, WSEQ), np.int64)
    for wr in range(2):
        for wc in range(2):
            for p in range(WSEQ):
                r = (7 * wr + p // 7 + off) % SIDE
                c = (7 * wc + p % 7 + off) % SIDE
                out[wr * 2 + wc, p] = r * SIDE + c
    return out


def permutation(shifted):
    tok = window_tokens(shifted)
    perm = np.zeros((WIMG, SEQP), np.float32)
    for w in range(4):
        perm[w * WROW + np.arange(WSEQ), tok[w]] = 1.0
    return perm


def region_mask():
    pos = np.arange(SIDE)
    band = (pos >= SIDE - WIN).astype(int) + (pos >= SIDE - SHIFT).astype(int)
    region = 3 * band[:, None] + band[None, :]
    win = region.reshape(2, WIN, 2, WIN).transpose(0, 2, 1, 3).reshape(4, WSEQ)
    out = np.zeros((4, WROW, WROW), np.float32)
    out[:, :WSEQ, :WSEQ] = np.where(win[:, :, None] != win[:, None, :], mask_fill, 0.0)
    return out


def norm_stats(z):
    mean = jnp.mean(z, -1, keepdims=True)
    cen = z - mean
    var = jnp.mean(cen * cen, -1, keepdims=True)
    inv = lax.rsqrt(var + norm_eps)
    return cen * inv, inv


def norm_back(e, hat, inv, gain):
    s = e * gain
    return inv * (s - jnp.mean(s, -1, keepdims=True) - hat * jnp.mean(s * hat, -1, keepdims=True))


def row_sum(v):
    return jnp.sum(v, 0, keepdims=True)


def put_images(ref, rows, blk, scale=lambda im, v: v):
    part = ref.at[rows, :]
    for im in range(PAIR):
        part[im * SEQP : im * SEQP + SEQ, :] = scale(im, blk[im].astype(f32))
        part[im * SEQP + SEQ : (im + 1) * SEQP, :] = jnp.zeros((SEQP - SEQ, D), f32)


def flat(v):
    return v.reshape(D, v.shape[-1])


def to_window_rows(perm, rows, out_ref):
    for im in range(PAIR):
        part = rows[im * SEQP : (im + 1) * SEQP].astype(bf16)
        out_ref[im * WIMG : (im + 1) * WIMG, :] = dot(perm, part).astype(bf16)


def to_token_rows(perm_t, ref):
    return jnp.concatenate(
        [dot(perm_t, ref[im * WIMG : (im + 1) * WIMG, :]) for im in range(PAIR)], 0
    ).astype(bf16)


def expand_heads(x, hm_ref):
    return jnp.concatenate([x * hm_ref[h : h + 1, :] for h in range(GROUP)], 0)


def fold_heads(o):
    lane = lax.broadcasted_iota(jnp.int32, (WROW, QUAD), 1) // HD
    acc = o[:WROW]
    for h in range(1, GROUP):
        acc = jnp.where(lane == h, o[h * WROW : (h + 1) * WROW], acc)
    return acc


def staged(stages, count, lag, at):
    for t in range(count + lag * (len(stages) - 1)):
        if t > 0 and t % SPAN == 0 and t // SPAN <= 2:
            at("attend", 2 + t // SPAN)
        for n, stage in enumerate(stages):
            if 0 <= t - lag * n < count:
                stage(t - lag * n)


def softmax_cols(s):
    e = jnp.exp2((s - jnp.max(s, 0, keepdims=True)) * (score_scale * log2_e))
    return e * (1.0 / jnp.sum(e, 0, keepdims=True))


def group_cols(g):
    base = (g // 2) * QKV + (g % 2) * QUAD
    return [slice(base + t * HALF, base + t * HALF + QUAD) for t in range(3)]


def attend_forward(x, wa, bias_ref, layer, vec_ref, nv_ref, perm, perm_t, hm_ref, qkv_ref, mixed_ref,
                   nperm, mixw, sc, prc, at):
    hat, _ = norm_stats(x)
    normed = hat * nv_ref[0:1, :] + nv_ref[1:2, :]
    to_window_rows(perm, normed, nperm)
    for m in range(2):
        r = dot(nperm[...], flat(wa[m, ..., :QKV]))
        base = m * QKV
        qkv_ref[:, base : base + HALF] = (r[:, :HALF] + vec_ref[m, layer, 1:2, :HALF]).astype(bf16)
        qkv_ref[:, base + HALF : base + 2 * HALF] = r[:, HALF : 2 * HALF].astype(bf16)
        qkv_ref[:, base + 2 * HALF : base + QKV] = (r[:, 2 * HALF :] + vec_ref[m, layer, 2:3, :HALF]).astype(bf16)
    at("attend", 1)
    units = [(w, g) for w in range(4 * PAIR) for g in range(GROUPS)]

    def scores(t):
        w, g = units[t]
        r = slice(w * WROW, (w + 1) * WROW)
        cq, ck, _ = group_cols(g)
        sc[t % SLOTS] = dot(qkv_ref[r, ck], expand_heads(qkv_ref[r, cq], hm_ref), 1, 1) + bias_ref[g // 2, layer * (1 + w % 4), g % 2]

    def middle(t):
        prc[t % SLOTS] = softmax_cols(sc[t % SLOTS]).astype(bf16)

    def mix(t):
        w, g = units[t]
        r = slice(w * WROW, (w + 1) * WROW)
        o = dot(prc[t % SLOTS], qkv_ref[r, group_cols(g)[2]], 0, 0)
        mixw[r, g * QUAD : (g + 1) * QUAD] = fold_heads(o).astype(bf16)

    staged((scores, middle, mix), len(units), LAG, at)
    mixed = to_token_rows(perm_t, mixw)
    mixed_ref[...] = mixed
    attn = dot(mixed[:, :HALF], flat(wa[0, ..., QKV:]), 1, 1) + dot(mixed[:, HALF:], flat(wa[1, ..., QKV:]), 1, 1)
    return x + attn + nv_ref[4:5, :]


CH = 512
SLOTS = 8
LAG = 2
SPAN = 12


def mlp_forward(mid, wm, vec_ref, layer, nv_ref, act_ref, slope_ref, at):
    hat, _ = norm_stats(mid)
    hid = (hat * nv_ref[2:3, :] + nv_ref[3:4, :]).astype(bf16)
    total = jnp.zeros((ROWS, D), f32)
    for m in range(2):
        for c in range(0, FFH, CH):
            col = m * FFH + c
            u = dot(hid, flat(wm[m, ..., c : c + CH])) + vec_ref[m, layer, 0:1, c : c + CH]
            t = u * root_half
            phi = 0.5 + 0.5 * lax.erf(t)
            act = (u * phi).astype(bf16)
            act_ref[:, col : col + CH] = act
            slope_ref[:, col : col + CH] = (phi + u * (jnp.exp2(t * t * -log2_e) * inv_root_two_pi)).astype(bf16)
            if col > 0:
                at("mlp", col // CH)
            total += dot(act, flat(wm[m, ..., FFH + c : FFH + c + CH]), 1, 1)
    return mid + total + nv_ref[5:6, :]


def mlp_backward(g_s, mid, wm, nv_ref, gp, hid_s, gb_s, rows, b1_acc, nv_acc, at):
    gout = g_s[rows, :]
    hat, inv = norm_stats(mid)
    hid_s[rows, :] = (hat * nv_ref[2:3, :] + nv_ref[3:4, :]).astype(bf16)
    gb = gout.astype(bf16)
    gb_s[rows, :] = gb
    ghid = jnp.zeros((ROWS, D), f32)
    for m in range(2):
        for c in range(0, FFH, CH):
            col = m * FFH + c
            g = dot(gb, flat(wm[m, ..., FFH + c : FFH + c + CH])) * gp[rows, col : col + CH].astype(f32)
            b1_acc[:, col : col + CH] += row_sum(g)
            g = g.astype(bf16)
            gp[rows, col : col + CH] = g
            if col > 0:
                at("mlp", col // CH)
            ghid += dot(g, flat(wm[m, ..., c : c + CH]), 1, 1)
    gmid = gout + norm_back(ghid, hat, inv, nv_ref[2:3, :])
    nv_acc[2:3, :] += row_sum(ghid * hat)
    nv_acc[3:4, :] += row_sum(ghid)
    nv_acc[4:5, :] += row_sum(gmid)
    nv_acc[5:6, :] += row_sum(gout)
    g_s[rows, :] = gmid


def attend_backward(g_s, x, wa, bias_ref, layer, nv_ref, perm, perm_t, hm_ref, qkv_ref,
                    mperm, gmw, gqw, gq_s, mb_s, nb_s, rows, ds_acc, qv_acc, nv_acc, sc, dpc, prc, dsc, at):
    gmid = g_s[rows, :]
    hat, inv = norm_stats(x)
    nb_s[rows, :] = (hat * nv_ref[0:1, :] + nv_ref[1:2, :]).astype(bf16)
    mb_s[rows, :] = gmid.astype(bf16)
    to_window_rows(perm, gmid, mperm)
    for m in range(2):
        gmw[:, m * HALF : (m + 1) * HALF] = dot(mperm[...], flat(wa[m, ..., QKV:])).astype(bf16)
    at("attend", 1)
    units = [(w, g) for w in range(4 * PAIR) for g in range(GROUPS)]

    def scores(t):
        w, g = units[t]
        r = slice(w * WROW, (w + 1) * WROW)
        cq, ck, cv = group_cols(g)
        sc[t % SLOTS] = dot(qkv_ref[r, ck], expand_heads(qkv_ref[r, cq], hm_ref), 1, 1) + bias_ref[g // 2, layer * (1 + w % 4), g % 2]
        dpc[t % SLOTS] = dot(qkv_ref[r, cv], expand_heads(gmw[r, g * QUAD : (g + 1) * QUAD], hm_ref), 1, 1)

    def middle(t):
        g = units[t][1]
        pr = softmax_cols(sc[t % SLOTS])
        prc[t % SLOTS] = pr.astype(bf16)
        dp = dpc[t % SLOTS]
        ds = pr * (dp - jnp.sum(pr * dp, 0, keepdims=True))
        ds_acc[g] += ds
        dsc[t % SLOTS] = ds.astype(bf16)

    def grads(t):
        w, g = units[t]
        r = slice(w * WROW, (w + 1) * WROW)
        cq, ck, cv = group_cols(g)
        own = slice(g * QUAD, (g + 1) * QUAD)
        gv = dot(prc[t % SLOTS], expand_heads(gmw[r, own], hm_ref))
        gk = dot(dsc[t % SLOTS], expand_heads(qkv_ref[r, cq], hm_ref)) * score_scale
        gq = fold_heads(dot(dsc[t % SLOTS], qkv_ref[r, ck], 0, 0)) * score_scale
        qv_acc[0:1, own] += row_sum(gq)
        qv_acc[1:2, own] += row_sum(gv)
        gqw[r, cq] = gq.astype(bf16)
        gqw[r, ck] = gk.astype(bf16)
        gqw[r, cv] = gv.astype(bf16)

    staged((scores, middle, grads), len(units), LAG, at)
    at("attend", 2)
    gq = to_token_rows(perm_t, gqw)
    gq_s[rows, :] = gq
    gnorm = dot(gq[:, :QKV], flat(wa[0, ..., :QKV]), 1, 1) + dot(gq[:, QKV:], flat(wa[1, ..., :QKV]), 1, 1)
    nv_acc[0:1, :] += row_sum(gnorm * hat)
    nv_acc[1:2, :] += row_sum(gnorm)
    g_s[rows, :] = g_s[rows, :] + norm_back(gnorm, hat, inv, nv_ref[0:1, :])


def forward_kernel(fast, steps, tok_ref, *refs):
    shards, refs = refs[: 4 if fast else 2], refs[4 if fast else 2 :]
    (bias_in, vec_in, nv_ref, perm_ref, perm_t_ref, hm_ref,
     out_ref, ys_ref, mid_ref, qkv_ref, mixed_ref, act_ref, slope_ref, wa_out, wm_out, bias_out,
     xs, mids, wa, wm, nperm, mixw, sc, prc, bias_ref, vec_ref, local, *sems) = refs
    s = pl.program_id(0)
    per = 2 * steps
    layer, r = s // per, lax.rem(s, per)
    pair = lax.rem(r, steps)
    rows = pl.ds(pl.multiple_of(pair * ROWS, ROWS), ROWS)
    weights = (wa, wm)
    me = lax.axis_index("mp")
    if fast:
        send, recv, own_a, own_m, ssend, srecv = sems
        own = (own_a, own_m)
        swaps = [
            remote(here, there.at[me], ssend.at[n], srecv.at[n], Place().core())
            for n, (here, there) in enumerate(((bias_in, bias_ref), (vec_in, vec_ref)))
        ]
        gathers = [
            Gather(own[n % 2].at[n // 2], weights[n % 2].at[n // 2], send.at[n], recv.at[n], local.at[n])
            for n in range(2 * LAYERS)
        ]

    def keep(n):
        return pltpu.make_async_copy(weights[n % 2].at[n // 2], (wa_out, wm_out)[n % 2].at[n // 2], local.at[4 + n])

    def at(step, point):
        if not fast:
            return
        for key, todo in FORWARD_PLAN.items():
            if key[1] == point and (key[0] % per < steps) == (step == "attend"):

                @pl.when(s == key[0])
                def _():
                    for n, stage in todo:
                        gathers[n].stage(stage)
                        if stage == Gather.STAGES - 1:
                            keep(n).start()

    keep_bias = pltpu.make_async_copy(bias_ref, bias_out, local.at[8])

    @pl.when(s == 0)
    def _():
        if fast:
            pack_shards(shards, own_a, own_m)
            neighbour_barrier(Place())
            for swap in swaps:
                swap.start()
        else:
            for n in range(2 * LAYERS):
                cp = pltpu.make_async_copy(shards[n % 2].at[n // 2], weights[n % 2].at[n // 2], local.at[n])
                cp.start()
                cp.wait()
            for here, there in ((bias_in, bias_ref), (vec_in, vec_ref)):
                there[...] = here[...]

    at("attend", 0)

    @pl.when(s == 0)
    def _():
        if fast:
            for here, there in ((bias_in, bias_ref), (vec_in, vec_ref)):
                there[me] = here[...]
            for swap in swaps:
                swap.wait()
        keep_bias.start()

    @pl.when(r < steps)
    def _():
        @pl.when(s < steps)
        def _():
            put_images(xs, rows, tok_ref)

        mid = attend_forward(xs[rows, :], wa.at[layer], bias_ref, layer, vec_ref, nv_ref.at[layer],
                             perm_ref[layer], perm_t_ref[layer], hm_ref, qkv_ref, mixed_ref, nperm, mixw, sc, prc, at)
        mid_ref[...] = mid
        mids[rows, :] = mid
        at("attend", 2)

    @pl.when(r >= steps)
    def _():
        at("mlp", 0)
        y = mlp_forward(mids[rows, :], wm.at[layer], vec_ref, layer, nv_ref.at[layer], act_ref, slope_ref, at)

        @pl.when(layer < LAYERS - 1)
        def _():
            xs[rows, :] = y
            ys_ref[...] = y

        @pl.when(layer == LAYERS - 1)
        def _():
            for im in range(PAIR):
                part = y[im * SEQP : im * SEQP + SEQ]
                out_ref[im] = part

    @pl.when(s == LAYERS * per - 1)
    def _():
        keep_bias.wait()
        if fast:
            for n in range(2 * LAYERS):
                keep(n).wait()


def pack_shards(shards, own_a, own_m):
    w_qkv, w_proj, w_one, w_two = shards
    for l in range(LAYERS):
        for k in range(3):
            own_a[l, :, k * HALF : (k + 1) * HALF] = w_qkv[l, k].astype(bf16)
        own_a[l, :, QKV:] = w_proj[l].astype(bf16)
        own_m[l, :, :FFH] = w_one[l].astype(bf16)
        own_m[l, :, FFH:] = w_two[l].astype(bf16)


FORWARD_PLAN = {
    (0, 0): [(0, 0), (1, 0), (0, 1), (0, 2), (0, 3), (1, 1), (0, 4), (1, 2), (1, 3), (0, 5), (0, 6)],
    (1, 1): [(1, 4)],
    (2, 1): [(1, 5)],
    (3, 0): [(2, 0), (1, 6)],
    (3, 2): [(2, 1)],
    (4, 0): [(2, 2)],
    (4, 1): [(2, 3), (3, 0)],
    (4, 3): [(2, 4)],
    (5, 0): [(3, 1)],
    (5, 1): [(2, 5), (3, 2)],
    (6, 0): [(2, 6)],
    (6, 1): [(3, 3)],
    (7, 1): [(3, 4)],
    (8, 1): [(3, 5)],
    (9, 0): [(3, 6)],
}


def backward_kernel(fast, steps, cot_ref, tok_ref, ys_ref, mid_ref, qkv_ref, act_in, slope_in, mixed_in, wa_in, wm_in,
                    bias_ref, nv_ref, perm_ref, perm_t_ref, hm_ref, count_ref, *refs):
    if fast:
        gx_ref, ga_out, sum_m, sum_a, *refs = refs
    else:
        gx_ref, ga_out, gm_out, *refs = refs
    (qv_all, b1_all, ds_all, nv_all, g_s, xs, mperm, gmw, gqw, gp, gq_s, hid_s, gb_s, mb_s, nb_s, act_s, mixed_s,
     wa, wm, gwm, gwa, sc, dpc, prc, dsc, local, *comm) = refs
    s = pl.program_id(0)
    per = 2 * steps + 6
    turn, r = s // per, lax.rem(s, per)
    layer = LAYERS - 1 - turn
    first_g, first_a, last_g = steps, steps + 4, 2 * steps + 4
    pair = jnp.where(r < first_a, jnp.minimum(r, steps - 1), jnp.minimum(r - first_a, steps - 1))
    rows = pl.ds(pl.multiple_of(pair * ROWS, ROWS), ROWS)
    total = steps * ROWS
    qv_acc, b1_acc, ds_acc, nv_acc, nv_ref = (
        ref.at[layer] for ref in (qv_all, b1_all, ds_all, nv_all, nv_ref)
    )
    me = lax.axis_index("mp")
    if fast:
        scatters = [
            Scatter(gw.at[0], gw.at[1], *comm[8 * n : 8 * n + 8]) for n, gw in enumerate((gwm.at[0], gwm.at[1], gwa))
        ]
        pl.when(s == 0)(lambda: neighbour_barrier(Place()))

    def at(step, point):
        if not fast:
            return
        spans = {"mlp": (0, first_g), "g": (first_g, first_a), "attend": (first_a, last_g), "ga": (last_g, per)}
        for key, todo in BACKWARD_PLAN.items():
            lo, hi = spans[step]
            if key[1] == point and lo <= key[0] % per < hi:

                @pl.when(s == key[0])
                def _():
                    for n, stage in todo:
                        if stage == Scatter.STAGES - 1:
                            last = key[0] < per + first_a
                            scatters[n].result(sum_a.at[0] if n == 2 else sum_m.at[n, LAYERS - 1 if last else 0])
                        scatters[n].stage(stage)

    def rows_of(l):
        return pl.ds(l * total, total)

    def load(name, l):
        src, dst, n = {
            "wm": (wm_in.at[l], wm, 0), "wa": (wa_in.at[l], wa, 1), "act": (act_in.at[rows_of(l)], act_s, 2),
            "mixed": (mixed_in.at[rows_of(l)], mixed_s, 3), "slope": (slope_in.at[rows_of(l)], gp, 4),
        }[name]
        return pltpu.make_async_copy(src, dst, local.at[n])

    top = LAYERS - 1

    @pl.when(s == 0)
    def _():
        for name in ("wm", "slope", "wa", "act", "mixed"):
            load(name, top).start()

    for l in range(top, -1, -1):
        base = (top - l) * per
        for name, step in (("wm", 0), ("slope", 0), ("act", first_g), ("wa", first_a), ("mixed", last_g)):
            pl.when(s == base + step)(lambda name=name, l=l: load(name, l).wait())
        if l > 0:
            for name, step in (("wm", first_g), ("slope", first_a), ("act", first_a), ("wa", last_g), ("mixed", per)):
                pl.when(s == base + step)(lambda name=name, l=l: load(name, l - 1).start())

    @pl.when(r == 0)
    def _():
        for ref in (qv_acc, b1_acc, ds_acc, nv_acc):
            ref[...] = jnp.zeros(ref.shape, f32)

    @pl.when(r < first_g)
    def _():
        at("mlp", 0)

        @pl.when(turn == 0)
        def _():
            image = (me * steps + pair) * PAIR
            put_images(g_s, rows, cot_ref, lambda im, v: v * (image + im < count_ref[0]).astype(f32))

        mlp_backward(g_s, mid_ref[...], wm, nv_ref, gp, hid_s, gb_s, rows, b1_acc, nv_acc, at)

    def gradient(left, right, lo, width):
        cols = pl.ds(pl.multiple_of(lo, width), width)
        return dot(left[...], right[:, cols], 0, 0).astype(bf16).reshape(*gwa.shape[1:-1], width)

    @pl.when((r >= first_g) & (r < first_a))
    def _():
        at("g", 0)
        q = r - first_g
        own = lax.rem(q, 2)
        half = jnp.where(own == 1, me, 1 - me)

        @pl.when(q < 2)
        def _():
            gwm[0, own] = gradient(hid_s, gp, half * FFH, FFH)

        @pl.when(q >= 2)
        def _():
            gwm[1, own] = gradient(gb_s, act_s, half * FFH, FFH)

        at("g", 1)

    @pl.when((r >= first_a) & (r < last_g))
    def _():
        at("attend", 0)

        @pl.when(layer == 0)
        def _():
            put_images(xs, slice(None), tok_ref)

        @pl.when(layer > 0)
        def _():
            xs[...] = ys_ref[...]

        attend_backward(g_s, xs[...], wa, bias_ref, layer, nv_ref, perm_ref[layer], perm_t_ref[layer], hm_ref,
                        qkv_ref, mperm, gmw, gqw, gq_s, mb_s, nb_s, rows, ds_acc, qv_acc, nv_acc, sc, dpc, prc, dsc, at)

        @pl.when(layer == 0)
        def _():
            for im in range(PAIR):
                part = g_s.at[rows, :][im * SEQP : im * SEQP + SEQ]
                gx_ref[im] = part

    @pl.when(r >= last_g)
    def _():
        at("ga", 0)
        own = r - last_g
        half = jnp.where(own == 1, me, 1 - me)
        gwa[own, ..., :QKV] = gradient(nb_s, gq_s, half * QKV, QKV)
        gwa[own, ..., QKV:] = gradient(mb_s, mixed_s, half * HALF, HALF)
        at("ga", 1)

    def flush(src, dst):
        cp = pltpu.make_async_copy(src, dst, local.at[5])
        cp.start()
        cp.wait()

    if fast:
        pl.when(s == LAYERS * per - 1)(lambda: flush(gwa, ga_out))
    else:
        pl.when(r == first_a)(lambda: flush(gwm, gm_out.at[layer]))
        pl.when(r == per - 1)(lambda: flush(gwa, ga_out.at[layer]))


BACKWARD_PLAN = {
    (4, 0): [(0, 0)],
    (5, 0): [(0, 1)],
    (6, 0): [(1, 0)],
    (7, 0): [(1, 1)],
    (7, 4): [(0, 2)],
    (8, 1): [(0, 3)],
    (8, 2): [(1, 2)],
    (9, 4): [(1, 3)],
    (10, 0): [(0, 4)],
    (11, 0): [(2, 0)],
    (12, 0): [(2, 1)],
    (13, 0): [(1, 4)],
    (13, 3): [(2, 2)],
    (14, 3): [(2, 3)],
    (16, 0): [(0, 0)],
    (17, 0): [(2, 4), (0, 1)],
    (18, 0): [(1, 0)],
    (19, 0): [(1, 1)],
    (19, 4): [(0, 2)],
    (20, 1): [(0, 3)],
    (20, 2): [(1, 2)],
    (21, 4): [(1, 3)],
    (22, 0): [(0, 4)],
    (23, 1): [(1, 4)],
}


def whole(shape, buffers=1):
    zero = (0,) * len(shape)
    return pl.BlockSpec(shape, lambda i: zero, pipeline_mode=pl.Buffered(buffers))


VLIM = 65000000


def forward(tok, shards, bias, vecs, nv, perm, perm_t, hm, fast, steps):
    per = 2 * steps
    rows = steps * ROWS
    slots = (2, NZ, NY, NX, D // PEERS) if fast else (2, 1, 1, 1, D)
    wide = (COLS - ATT, ATT)
    any_ = pl.BlockSpec(memory_space=pl.ANY)

    def attend(s):
        return s // per * steps + jnp.minimum(lax.rem(s, per), steps - 1)

    def mlp(s):
        return s // per * steps + jnp.maximum(lax.rem(s, per) - steps, 0)

    sems = []
    if fast:
        sems = [pltpu.SemaphoreType.DMA((2 * LAYERS, Gather.SEMS))] * 2
        sems += [pltpu.VMEM((LAYERS, D // PEERS, n), bf16) for n in wide] + [pltpu.SemaphoreType.DMA((2,))] * 2
    halves = [(2, *a.shape) if fast else a.shape for a in (bias, vecs)]
    params = dict(collective_id=1, has_side_effects=True) if fast else {}
    return pl.pallas_call(
        functools.partial(forward_kernel, fast, steps),
        name="forward",
        grid=(LAYERS * per,),
        in_specs=[
            pl.BlockSpec((PAIR, SEQ, D), lambda s: (lax.axis_index("mp") * steps + jnp.minimum(s, steps - 1), 0, 0)),
            *(whole(w.shape) if fast else any_ for w in shards),
            *(whole(a.shape) for a in (bias, vecs, nv, perm, perm_t, hm)),
        ],
        out_specs=[
            pl.BlockSpec((PAIR, SEQ, D), lambda s: (jnp.maximum(s - (LAYERS * per - steps), 0), 0, 0)),
            pl.BlockSpec((ROWS, D), lambda s: (jnp.clip(s - steps, 0, steps - 1), 0)),
            pl.BlockSpec((ROWS, D), lambda s: (attend(s), 0)),
            pl.BlockSpec((WPAIR, 2 * QKV), lambda s: (attend(s), 0)),
            pl.BlockSpec((ROWS, D), lambda s: (attend(s), 0)),
            pl.BlockSpec((ROWS, 2 * FFH), lambda s: (mlp(s), 0)),
            pl.BlockSpec((ROWS, 2 * FFH), lambda s: (mlp(s), 0)),
            any_, any_, any_,
        ],
        out_shape=[
            jax.ShapeDtypeStruct((steps * PAIR, SEQ, D), f32),
            jax.ShapeDtypeStruct((rows, D), f32),
            jax.ShapeDtypeStruct((LAYERS * rows, D), f32),
            jax.ShapeDtypeStruct((LAYERS * steps * WPAIR, 2 * QKV), bf16),
            jax.ShapeDtypeStruct((LAYERS * rows, D), bf16),
            jax.ShapeDtypeStruct((LAYERS * rows, 2 * FFH), bf16),
            jax.ShapeDtypeStruct((LAYERS * rows, 2 * FFH), bf16),
            *(jax.ShapeDtypeStruct((LAYERS, *slots, n), bf16) for n in wide),
            jax.ShapeDtypeStruct(halves[0], f32),
        ],
        scratch_shapes=[
            pltpu.VMEM((rows, D), f32), pltpu.VMEM((rows, D), f32),
            *(pltpu.VMEM((LAYERS, *slots, n), bf16) for n in wide),
            pltpu.VMEM((WPAIR, D), bf16), pltpu.VMEM((WPAIR, D), bf16),
            pltpu.VMEM((SLOTS, WROW, LANES), f32), pltpu.VMEM((SLOTS, WROW, LANES), bf16),
            *(pltpu.VMEM(n, f32) for n in halves),
            pltpu.SemaphoreType.DMA((9,)), *sems,
        ],
        compiler_params=pltpu.CompilerParams(vmem_limit_bytes=VLIM, **params),
    )(tok, *shards, bias, vecs, nv, perm, perm_t, hm)


def backward(cot, tok, saved, weights, bias, nv, perm, perm_t, hm, count, fast, steps):
    ys, mid, qkv, mixed, act, slope = saved
    wa, wm = weights
    per = 2 * steps + 6
    rows = steps * ROWS
    slots = wa.shape[1:-1]
    rest = slots[1:]
    any_ = pl.BlockSpec(memory_space=pl.ANY)

    def clip(v):
        return jnp.clip(v, 0, steps - 1)

    def layer(s):
        return LAYERS - 1 - s // per

    attend0 = (LAYERS - 1) * per + steps + 4
    img = lambda at: pl.BlockSpec((PAIR, SEQ, D), lambda s: (clip(s - at), 0, 0))
    mine = lambda at: pl.BlockSpec((PAIR, SEQ, D), lambda s: (lax.axis_index("mp") * steps + clip(s - at), 0, 0))
    wide = (COLS - ATT, ATT)
    part = rest[-1]
    if fast:
        outs = [
            jax.ShapeDtypeStruct((2, *rest, COLS - ATT), bf16),
            jax.ShapeDtypeStruct((2, LAYERS, part, FFH), f32), jax.ShapeDtypeStruct((1, part, COLS - ATT), f32),
        ]
        specs = [any_, whole(outs[1].shape), whole(outs[2].shape)]
        comm = Scatter.landing(part, FFH) * 2 + Scatter.landing(part, COLS - ATT)
        params = dict(collective_id=2, has_side_effects=True)
    else:
        outs = [
            jax.ShapeDtypeStruct((LAYERS, 2, *rest, COLS - ATT), bf16),
            jax.ShapeDtypeStruct((LAYERS, 2, 2, *rest, FFH), bf16),
        ]
        specs, comm, params = [any_, any_], [], {}
    small = [(LAYERS, 2, 2 * HALF), (LAYERS, 1, 2 * FFH), (LAYERS, GROUPS, WROW, LANES), (LAYERS, 8, D)]
    return pl.pallas_call(
        functools.partial(backward_kernel, fast, steps),
        name="backward",
        grid=(LAYERS * per,),
        in_specs=[
            mine(0), mine(attend0),
            pl.BlockSpec((ROWS, D), lambda s: (clip(s - steps - 4), 0)),
            pl.BlockSpec((ROWS, D), lambda s: (layer(s) * steps + clip(lax.rem(s, per)), 0)),
            pl.BlockSpec((WPAIR, 2 * QKV), lambda s: (layer(s) * steps + clip(lax.rem(s, per) - steps - 4), 0)),
            any_, any_, any_, any_, any_,
            *(whole(a.shape) for a in (bias, nv, perm, perm_t, hm)),
            pl.BlockSpec(memory_space=pltpu.SMEM),
        ],
        out_specs=[img(attend0), *specs, *(whole(n) for n in small)],
        out_shape=[
            jax.ShapeDtypeStruct((steps * PAIR, SEQ, D), f32), *outs, *(jax.ShapeDtypeStruct(n, f32) for n in small),
        ],
        scratch_shapes=[
            pltpu.VMEM((rows, D), f32), pltpu.VMEM((ROWS, D), f32),
            pltpu.VMEM((WPAIR, D), bf16), pltpu.VMEM((WPAIR, D), bf16), pltpu.VMEM((WPAIR, 2 * QKV), bf16),
            pltpu.VMEM((rows, 2 * FFH), bf16), pltpu.VMEM((rows, 2 * QKV), bf16),
            *[pltpu.VMEM((rows, D), bf16)] * 4,
            pltpu.VMEM((rows, 2 * FFH), bf16), pltpu.VMEM((rows, D), bf16),
            *(pltpu.VMEM((*slots, n), bf16) for n in wide),
            pltpu.VMEM((2, 2, *rest, FFH), bf16), pltpu.VMEM((2, *rest, COLS - ATT), bf16),
            *[pltpu.VMEM((SLOTS, WROW, LANES), f32)] * 2, *[pltpu.VMEM((SLOTS, WROW, LANES), bf16)] * 2,
            pltpu.SemaphoreType.DMA((8,)), *comm,
        ],
        compiler_params=pltpu.CompilerParams(vmem_limit_bytes=VLIM, **params),
    )(cot, tok, ys, mid, qkv, act, slope, mixed, wa, wm, bias, nv, perm, perm_t, hm, count)


def head_mask():
    return (np.arange(QUAD)[None, :] // HD == np.arange(GROUP)[:, None]).astype(np.float32)


def exact_parts(a):
    parts = []
    for _ in range(3):
        top = lax.reduce_precision(a, 8, 7)
        parts.append(top.astype(bf16))
        a = a - top
    return jnp.stack(parts)


def bias_cols(onehot, table):
    picked = jnp.einsum("jti,smlth->sjmlhi", onehot.astype(bf16), exact_parts(table), preferred_element_type=f32)
    picked = (picked[0] + picked[1] + picked[2]).transpose(1, 2, 0, 3, 4)
    picked = picked.reshape(-1, LAYERS, WROW, 2, GROUP, WROW).transpose(0, 1, 3, 2, 4, 5)
    apart = np.concatenate([np.zeros((1, WROW, WROW), np.float32), region_mask()])
    apart[:, WSEQ:] = pad_fill
    both = jnp.concatenate([picked[:, :1]] + [picked[:, 1:]] * 4, 1)
    both = (both + jnp.asarray(apart)[:, None, :, None, :]) * (1.0 / score_scale)
    return both.reshape(-1, 5, 2, WROW, LANES)

NZ, NY, NX = 4, 2, 2
PEERS = NZ * NY * NX
MESH_ID = pl.DeviceIdType.MESH


class Place:
    def __init__(self):
        d = lax.axis_index("dp")
        self.d, self.m = d, lax.axis_index("mp")
        self.z, self.y, self.x = d // 4, lax.rem(d // 2, 2), lax.rem(d, 2)

    def chip(self, z, y, x):
        return (z * NY + y) * NX + x

    def at(self, y=None, x=None, m=None):
        y = self.y if y is None else y
        x = self.x if x is None else x
        return (self.chip(self.z, y, x), self.m if m is None else m)

    def xn(self):
        return self.at(x=1 - self.x)

    def yn(self):
        return self.at(y=1 - self.y)

    def core(self):
        return self.at(m=1 - self.m)

    def zn(self, step):
        return (self.chip(self.z + step, self.y, self.x), self.m)

    def has(self, step):
        return self.z < NZ - 1 if step > 0 else self.z > 0

    def column(self, z):
        return (self.chip(z, self.y, self.x), self.m)


def remote(src, dst, send, recv, to):
    return pltpu.make_async_remote_copy(
        src_ref=src, dst_ref=dst, send_sem=send, recv_sem=recv, device_id=to, device_id_type=MESH_ID
    )


def neighbour_barrier(p):
    sem = pltpu.get_barrier_semaphore()
    partners = [p.xn(), p.yn(), p.core()] + [p.column(lax.rem(p.z + n, NZ)) for n in range(1, NZ)]
    for to in partners:
        pl.semaphore_signal(sem, inc=1, device_id=to, device_id_type=MESH_ID)
    pl.semaphore_wait(sem, len(partners))


def each_plane(body):
    lax.fori_loop(0, NZ, lambda k, carry: (body(k), carry)[1], 0)


class Gather:
    SEMS = 52
    BASE = {"z": 0, "xa": 8, "yb": 12, "ya0": 16, "ya1": 20, "xb0": 24, "xb1": 28,
            "own": 32, "ax": 36, "by": 40, "ar": 44, "br": 48}

    def __init__(self, own, full, send, recv, local):
        self.p, self.own, self.full = Place(), own, full
        self.send, self.recv, self.local = send, recv, local
        half = full.shape[-1] // 2
        self.all, self.a, self.b = pl.ds(0, 2 * half), pl.ds(0, half), pl.ds(half, half)

    def region(self, kind, k, arrived):
        p = self.p
        oy, ox = 1 - p.y, 1 - p.x
        if kind == "z":
            return (p.m, k, p.y, p.x), self.all, None
        if kind == "xa":
            return (p.m, k, p.y, ox if arrived else p.x), self.a, p.xn()
        if kind == "yb":
            return (p.m, k, oy if arrived else p.y, p.x), self.b, p.yn()
        if kind in ("ya0", "ya1"):
            return (p.m, k, oy if arrived else p.y, p.x if kind == "ya0" else ox), self.a, p.yn()
        if kind in ("xb0", "xb1"):
            return (p.m, k, p.y if kind == "xb0" else oy, ox if arrived else p.x), self.b, p.xn()
        m = 1 - p.m if arrived else p.m
        if kind == "own":
            return (m, k, p.y, p.x), self.all, p.core()
        if kind == "ax":
            return (m, k, p.y, ox), self.a, p.core()
        if kind == "by":
            return (m, k, oy, p.x), self.b, p.core()
        if kind == "ar":
            return (m, k, oy, slice(None)), self.a, p.core()
        return (m, k, slice(None), ox), self.b, p.core()

    def copy(self, kind, k, own=False, arrived=False, step=0):
        at, cols, to = self.region(kind, k, arrived)
        dst = self.full.at[(*at, slice(None), cols)]
        src = self.own.at[:, cols] if own else dst
        s = self.BASE[kind] + k
        r = s
        if kind == "z":
            to = self.p.zn(step)
            s = s + (4 if step < 0 else 0)
        return remote(src, dst, self.send.at[s], self.recv.at[r], to)

    def keep(self):
        p = self.p
        return pltpu.make_async_copy(
            self.own.at[:, self.all], self.full.at[p.m, p.z, p.y, p.x, :, self.all], self.local
        )

    def fan(self, k, own=False):
        for kind in ("xa", "yb", "ya0", "xb0", "own"):
            self.copy(kind, k, own).start()

    def stage(self, n):
        p = self.p
        if n == 0:
            self.keep().start()
            for step in (1, -1):
                pl.when(p.has(step))(lambda step=step: self.copy("z", p.z, True, step=step).start())
            self.fan(p.z, True)
        elif n <= 3:
            for step in (1, -1):
                k = p.z - step * n
                inside = k >= 0 if step > 0 else k < NZ

                @pl.when(inside)
                def _():
                    self.copy("z", k, arrived=True, step=step).wait_recv()
                    pl.when(p.has(step))(lambda: self.copy("z", k, step=step).start())
                    self.fan(k)
        elif n == 4:

            @each_plane
            def _(k):
                self.copy("xa", k, arrived=True).wait_recv()
                for kind in ("ya1", "ax"):
                    self.copy(kind, k).start()
                self.copy("yb", k, arrived=True).wait_recv()
                for kind in ("xb1", "by"):
                    self.copy(kind, k).start()
        elif n == 5:

            @each_plane
            def _(k):
                for kind, rest in (("ya", "ar"), ("xb", "br")):
                    for rel in ("0", "1"):
                        self.copy(kind + rel, k, arrived=True).wait_recv()
                    self.copy(rest, k).start()
        else:

            @each_plane
            def _(k):
                for kind in ("own", "ax", "by", "ar", "br"):
                    self.copy(kind, k, arrived=True).wait_recv()
                for kind in self.BASE:
                    if kind != "z":
                        self.copy(kind, k).wait_send()
                pl.when((k <= p.z) & p.has(1))(lambda: self.copy("z", k, step=1).wait_send())
                pl.when((k >= p.z) & p.has(-1))(lambda: self.copy("z", k, step=-1).wait_send())

            self.keep().wait()

    STAGES = 7


def add_into(ref, at, other):
    ref[at] = ref[at] + other


class Scatter:
    SEMS = 24
    BASE = {"core": 0, "ya": 4, "xb": 8, "xa": 12, "yb": 16, "z": 20}

    @staticmethod
    def landing(rows, cols):
        half = cols // 2
        return [
            pltpu.VMEM((NZ, NY, NX, rows, cols), bf16),
            pltpu.VMEM((NZ, NX, rows, half), bf16), pltpu.VMEM((NZ, NY, rows, half), bf16),
            pltpu.VMEM((NZ, rows, half), bf16), pltpu.VMEM((NZ, rows, half), bf16),
            pltpu.VMEM((NZ, rows, cols), bf16),
            pltpu.SemaphoreType.DMA((Scatter.SEMS,)), pltpu.SemaphoreType.DMA((Scatter.SEMS,)),
        ]

    def __init__(self, give, part, other, ya, xb, xa, yb, z, send, recv):
        self.p, self.give, self.part, self.other = Place(), give, part, other
        self.land = {"ya": ya, "xb": xb, "xa": xa, "yb": yb, "z": z}
        self.send, self.recv = send, recv
        half = part.shape[-1] // 2
        self.a, self.b = pl.ds(0, half), pl.ds(half, half)

    def copy(self, kind, k):
        p = self.p
        oy, ox = 1 - p.y, 1 - p.x
        full = slice(None)
        if kind == "core":
            src, dst, to = self.give.at[k], self.other.at[k], p.core()
        else:
            at, to = {
                "ya": ((k, oy, full, full, self.a), p.yn()),
                "xb": ((k, full, ox, full, self.b), p.xn()),
                "xa": ((k, p.y, ox, full, self.a), p.xn()),
                "yb": ((k, oy, p.x, full, self.b), p.yn()),
                "z": ((k, p.y, p.x, full, full), p.column(k)),
            }[kind]
            src, dst = self.part.at[at], self.land[kind].at[p.z if kind == "z" else k]
        s = self.BASE[kind] + k
        r = self.BASE[kind] + p.z if kind == "z" else s
        return remote(src, dst, self.send.at[s], self.recv.at[r], to)

    def landed(self, k):
        s = self.BASE["z"] + k
        at = self.land["z"].at[k]
        return remote(at, at, self.send.at[s], self.recv.at[s], self.p.column(k))

    def stage(self, n):
        p = self.p
        oy, ox = 1 - p.y, 1 - p.x
        if n == 0:
            each_plane(lambda k: self.copy("core", k).start())
        elif n == 1:

            @each_plane
            def _(k):
                self.copy("core", k).wait_recv()
                for y in range(NY):
                    for x in range(NX):
                        add_into(self.part, (k, y, x), self.other[k, y, x])
                self.copy("ya", k).start()
                self.copy("xb", k).start()
        elif n == 2:

            @each_plane
            def _(k):
                self.copy("ya", k).wait_recv()
                for x in range(NX):
                    add_into(self.part, (k, p.y, x, slice(None), self.a), self.land["ya"][k, x])
                self.copy("xa", k).start()
                self.copy("xb", k).wait_recv()
                for y in range(NY):
                    add_into(self.part, (k, y, p.x, slice(None), self.b), self.land["xb"][k, y])
                self.copy("yb", k).start()
        elif n == 3:

            @each_plane
            def _(k):
                self.copy("xa", k).wait_recv()
                add_into(self.part, (k, p.y, p.x, slice(None), self.a), self.land["xa"][k])
                self.copy("yb", k).wait_recv()
                add_into(self.part, (k, p.y, p.x, slice(None), self.b), self.land["yb"][k])

            for dist in (3, 2, 1):
                for k in (p.z + dist, p.z - dist):
                    pl.when((k >= 0) & (k < NZ))(lambda k=k: self.copy("z", k).start())
        else:

            @each_plane
            def _(k):
                for kind in ("core", "ya", "xb", "xa", "yb"):
                    self.copy(kind, k).wait_send()
                pl.when(k != p.z)(lambda: self.copy("z", k).wait_send())

    STAGES = 5

    def result(self, out):
        p = self.p
        out[...] = self.part[p.z, p.y, p.x].astype(f32)

        @each_plane
        def _(k):
            @pl.when(k != p.z)
            def _():
                self.landed(k).wait_recv()
                out[...] += self.land["z"][k].astype(f32)


class Total:
    STEPS = 5

    @staticmethod
    def scratch(shape):
        return [
            pltpu.VMEM((Total.STEPS, *shape), f32), pltpu.VMEM((Total.STEPS, *shape), f32),
            pltpu.SemaphoreType.DMA((Total.STEPS,)), pltpu.SemaphoreType.DMA((Total.STEPS,)),
        ]

    def __init__(self, start, held, land, send, recv):
        self.p, self.start, self.held, self.land, self.send, self.recv = Place(), start, held, land, send, recv

    def copy(self, n):
        p = self.p
        pair = p.z + 1 - 2 * lax.rem(p.z, 2)
        far = lax.rem(p.z + 2, NZ)
        to = (p.core(), p.yn(), p.xn(), (p.chip(pair, p.y, p.x), p.m), (p.chip(far, p.y, p.x), p.m))[n]
        src = self.start if n == 0 else self.held.at[n - 1]
        return remote(src, self.land.at[n], self.send.at[n], self.recv.at[n], to)

    def stage(self, n):
        if n > 0:
            self.copy(n - 1).wait_recv()
            before = self.start[...] if n == 1 else self.held[n - 2]
            self.held[n - 1] = before + self.land[n - 1]
        if n < self.STEPS:
            self.copy(n).start()
        else:
            for k in range(self.STEPS):
                self.copy(k).wait_send()


def tail_kernel(grad_ref, small_ref, out_ref, small_out, part, *refs):
    neighbour_barrier(Place())
    total = Total(small_ref, *refs[-4:])
    width = part.shape[-1]
    spans = [pl.ds(n * width, width) for n in range(2)]
    pieces = [
        Scatter(grad_ref.at[0, ..., cols], part.at[n], *refs[8 * n : 8 * n + 8]) for n, cols in enumerate(spans)
    ]
    for s in pieces:
        s.stage(0)
    total.stage(0)
    for n, cols in enumerate(spans):
        part[n] = grad_ref[1, ..., cols]
    for n in range(1, Scatter.STAGES - 1):
        for s in pieces:
            s.stage(n)
        total.stage(n)
    total.stage(Scatter.STAGES - 1)
    for s, cols in zip(pieces, spans):
        s.result(out_ref.at[:, cols])
        s.stage(Scatter.STAGES - 1)
    total.stage(Total.STEPS)
    small_out[...] = total.held[Total.STEPS - 1]


def tail(grad, small):
    rows, cols = grad.shape[-2:]
    half = cols // 2
    vm = pl.BlockSpec(memory_space=pltpu.VMEM)
    return pl.pallas_call(
        tail_kernel,
        name="tail",
        out_shape=[jax.ShapeDtypeStruct((rows, cols), f32), jax.ShapeDtypeStruct(small.shape, f32)],
        in_specs=[vm] * 2,
        out_specs=[vm] * 2,
        scratch_shapes=[pltpu.VMEM((2, *grad.shape[1:-1], half), bf16)] + Scatter.landing(rows, half) * 2
        + Total.scratch(small.shape),
        compiler_params=pltpu.CompilerParams(collective_id=3, has_side_effects=True, vmem_limit_bytes=VLIM),
    )(grad, small)


def adam_update(weight_in, moment_one, moment_two, grad_sum, decay):
    new_one = beta_one * moment_one + (1.0 - beta_one) * grad_sum
    new_two = beta_two * moment_two + (1.0 - beta_two) * grad_sum * grad_sum
    hat_one = new_one / (1.0 - beta_one**adam_step)
    hat_two = new_two / (1.0 - beta_two**adam_step)
    new_weight = weight_in - learn_rate * (hat_one / (jnp.sqrt(hat_two) + adam_eps) + decay * weight_in)
    return (new_weight, new_one, new_two)


def both_halves(mine, me):
    other = lax.ppermute(mine, "mp", [(0, 1), (1, 0)])
    low = jnp.where(me == 0, mine, other)
    high = jnp.where(me == 0, other, mine)
    return jnp.concatenate([low, high], 0)


HEADS = GROUPS * GROUP
LITTLE = 4 * HALF + 2 * FFH + HEADS * TABLE + 6 * D


def lanes_of(a):
    flat = a.reshape(-1)
    return jnp.pad(flat, (0, -flat.size % 1024)).reshape(-1, 128)


def sum_of_all(a):
    a = a.reshape(LAYERS, 2, D, a.shape[-1])
    total = a[:, 1].astype(f32) + lax.ppermute(a[:, 0], "mp", [(0, 1), (1, 0)]).astype(f32)
    return lax.psum_scatter(total.astype(bf16), "dp", scatter_dimension=1, tiled=True).astype(f32)


def pair_onehot(rel_index):
    index = jnp.pad(rel_index.T, ((0, WROW - WSEQ), (0, WROW - WSEQ)), constant_values=-1)
    return (index[:, None, :] == jnp.arange(TABLE, dtype=jnp.int32)[None, :, None]).astype(f32)


def local(
    fast, tokens, cotangent, image_count, rel_index,
    w_qkv, w_proj, w_fc_one, w_fc_two, qv_bias, fc_one_bias, rel_table, norm_vec,
    m_qkv, m_proj, m_fc_one, m_fc_two, m_qv_bias, m_fc_one_bias, m_rel_table, m_norm_vec,
    v_qkv, v_proj, v_fc_one, v_fc_two, v_qv_bias, v_fc_one_bias, v_rel_table, v_norm_vec,
):
    me = lax.axis_index("mp")
    images = tokens.shape[0]
    nimg = images // 2
    steps = nimg // PAIR
    part = w_qkv.shape[1]
    tok, cot = tokens, cotangent
    onehot = pair_onehot(rel_index)
    vecs = jnp.concatenate([fc_one_bias[:, None], jnp.pad(qv_bias, ((0, 0), (0, 5), (0, FFH - HALF)))], 1)
    shards = (w_qkv.transpose(0, 2, 1, 3), w_proj.transpose(0, 2, 1), w_fc_one, w_fc_two.transpose(0, 2, 1))
    if fast:
        bias = bias_cols(onehot, rel_table[None])[0]
    else:
        wm = jnp.concatenate([w_fc_one, w_fc_two.transpose(0, 2, 1)], 2).astype(bf16)
        wa = jnp.concatenate([w_qkv.reshape(LAYERS, part, QKV), w_proj.transpose(0, 2, 1)], 2).astype(bf16)
        shards = [
            lax.all_gather(w, ("mp", "dp")).reshape(2, -1, LAYERS, part, w.shape[-1]).transpose(2, 0, 1, 3, 4)
            .reshape(LAYERS, 2, 1, 1, 1, D, w.shape[-1])
            for w in (wa, wm)
        ]
        vecs = lax.all_gather(vecs, "mp")
        bias = bias_cols(onehot, lax.all_gather(rel_table, "mp"))
    hm = jnp.asarray(head_mask(), bf16)
    perms = np.stack([permutation(layer % 2 == 1) for layer in range(LAYERS)])
    perm, perm_t = jnp.asarray(perms, bf16), jnp.asarray(perms.transpose(0, 2, 1), bf16)
    out, *saved, all_wa, all_wm, bias = forward(
        tok, shards, bias, vecs, norm_vec, perm, perm_t, hm, fast, steps
    )
    weights = (all_wa, all_wm) if fast else shards
    out = both_halves(out, me)
    x_grad, *grads, gqv, gb1, ds, gnv = backward(
        cot, tok, saved, weights, bias, norm_vec, perm, perm_t, hm, image_count, fast, steps
    )
    x_grad = both_halves(x_grad, me)
    ds = ds.reshape(LAYERS, GROUPS, WROW, GROUP, WROW)
    gt = jnp.einsum("lgjhi,jti->lght", ds, onehot, precision=lax.Precision.HIGHEST)
    little = jnp.concatenate([a.reshape(LAYERS, -1) for a in (gqv, gb1, gt, gnv[:, :6])], 1)
    if fast:
        ga, sum_m, sum_a = grads
        last, total = tail(ga, lanes_of(little))
        big_a, big_m = jnp.stack([last, sum_a[0]]), sum_m
        little = total.reshape(-1)[: LAYERS * LITTLE].reshape(LAYERS, LITTLE)
    else:
        ga, gm = grads
        big_a, big_m = sum_of_all(ga), jnp.stack([sum_of_all(gm[:, n]) for n in range(2)])
        little = lax.psum(little, ("dp", "mp"))
    one_grad = big_m[0]
    two_grad = big_m[1].transpose(0, 2, 1)
    qkv_grad = big_a[:, :, :QKV].reshape(LAYERS, part, 3, HALF)
    proj_grad = big_a[:, :, QKV:].transpose(0, 2, 1)
    cut = lambda a: lax.dynamic_index_in_dim(a, me, 1, keepdims=False)
    at = 2 * 2 * HALF
    qv_grad = cut(little[:, :at].reshape(LAYERS, 2, 2, HALF).transpose(0, 2, 1, 3))
    bias_grad = cut(little[:, at : at + 2 * FFH].reshape(LAYERS, 2, FFH))
    at += 2 * FFH
    table_grad = cut(little[:, at : at + HEADS * TABLE].reshape(LAYERS, 2, HEADS // 2, TABLE)).transpose(0, 2, 1)
    at += HEADS * TABLE
    norm_grad = little[:, at:].reshape(LAYERS, 6, D)
    groups = [
        adam_update(w_qkv, m_qkv, v_qkv, qkv_grad, decay_rate),
        adam_update(w_proj, m_proj, v_proj, proj_grad, decay_rate),
        adam_update(w_fc_one, m_fc_one, v_fc_one, one_grad, decay_rate),
        adam_update(w_fc_two, m_fc_two, v_fc_two, two_grad, decay_rate),
        adam_update(qv_bias, m_qv_bias, v_qv_bias, qv_grad, 0.0),
        adam_update(fc_one_bias, m_fc_one_bias, v_fc_one_bias, bias_grad, 0.0),
        adam_update(rel_table, m_rel_table, v_rel_table, table_grad, 0.0),
        adam_update(norm_vec, m_norm_vec, v_norm_vec, norm_grad, 0.0),
    ]
    return (out, x_grad, *[grp[k] for k in range(3) for grp in groups])


def solution(mesh):
    params = (
        P(None, "dp", None, "mp"), P(None, "mp", "dp"), P(None, "dp", "mp"), P(None, "mp", "dp"),
        P(None, None, "mp"), P(None, "mp"), P(None, None, "mp"), P(),
    )
    act = (P("dp", None, None), P("dp", None, None))
    return jax.shard_map(
        functools.partial(local, mesh.shape["dp"] == PEERS),
        mesh=mesh,
        in_specs=(*act, P("dp"), P(), *params, *params, *params),
        out_specs=(*act, *params, *params, *params),
        check_vma=False,
    )
```

```python
import functools

import jax
import jax.numpy as jnp
import numpy as np
from jax import lax
from jax.experimental import pallas as pl
from jax.experimental.pallas import tpu as pltpu
from jax.sharding import PartitionSpec as P

D = 512
HD = 32
SIDE = 14
WIN = 7
SHIFT = 3
SEQ = 196
WSEQ = 49
TABLE = 169
LAYERS = 2
SEQP = 200
PAIR = 2
ROWS = PAIR * SEQP
WROW = 64
WIMG = 4 * WROW
WPAIR = PAIR * WIMG
HALF = 256
GROUP = 4
GROUPS = 4
QUAD = GROUP * HD
LANES = GROUP * WROW
FFH = 1024
QKV = 3 * HALF
COLS = 2 * FFH + QKV + HALF
ATT = 2 * FFH

norm_eps = 1e-05
mask_fill = -100.0
pad_fill = -1e30
beta_one = 0.9
beta_two = 0.999
adam_eps = 1e-08
learn_rate = 0.02
decay_rate = 0.05
adam_step = 3.0
root_half = 0.7071067811865476
inv_root_two_pi = 0.3989422804014327
score_scale = HD**-0.5
log2_e = 1.4426950408889634

f32 = jnp.float32
bf16 = jnp.bfloat16


def dot(a, b, ca=1, cb=0):
    return lax.dot_general(a, b, (((ca,), (cb,)), ((), ())), preferred_element_type=f32)


def window_tokens(shifted):
    off = SHIFT if shifted else 0
    out = np.zeros((4, WSEQ), np.int64)
    for wr in range(2):
        for wc in range(2):
            for p in range(WSEQ):
                r = (7 * wr + p // 7 + off) % SIDE
                c = (7 * wc + p % 7 + off) % SIDE
                out[wr * 2 + wc, p] = r * SIDE + c
    return out


def permutation(shifted):
    tok = window_tokens(shifted)
    perm = np.zeros((WIMG, SEQP), np.float32)
    for w in range(4):
        perm[w * WROW + np.arange(WSEQ), tok[w]] = 1.0
    return perm


def region_mask():
    pos = np.arange(SIDE)
    band = (pos >= SIDE - WIN).astype(int) + (pos >= SIDE - SHIFT).astype(int)
    region = 3 * band[:, None] + band[None, :]
    win = region.reshape(2, WIN, 2, WIN).transpose(0, 2, 1, 3).reshape(4, WSEQ)
    out = np.zeros((4, WROW, WROW), np.float32)
    out[:, :WSEQ, :WSEQ] = np.where(win[:, :, None] != win[:, None, :], mask_fill, 0.0)
    return out


def norm_stats(z):
    mean = jnp.mean(z, -1, keepdims=True)
    cen = z - mean
    var = jnp.mean(cen * cen, -1, keepdims=True)
    inv = lax.rsqrt(var + norm_eps)
    return cen * inv, inv


def norm_back(e, hat, inv, gain):
    s = e * gain
    return inv * (s - jnp.mean(s, -1, keepdims=True) - hat * jnp.mean(s * hat, -1, keepdims=True))


def row_sum(v):
    return jnp.sum(v, 0, keepdims=True)


def put_images(ref, rows, blk, scale=lambda im, v: v):
    part = ref.at[rows, :]
    for im in range(PAIR):
        part[im * SEQP : im * SEQP + SEQ, :] = scale(im, blk[im].astype(f32))
        part[im * SEQP + SEQ : (im + 1) * SEQP, :] = jnp.zeros((SEQP - SEQ, D), f32)


def flat(v):
    return v.reshape(D, v.shape[-1])


def to_window_rows(perm, rows, out_ref):
    for im in range(PAIR):
        part = rows[im * SEQP : (im + 1) * SEQP].astype(bf16)
        out_ref[im * WIMG : (im + 1) * WIMG, :] = dot(perm, part).astype(bf16)


def to_token_rows(perm_t, ref):
    return jnp.concatenate(
        [dot(perm_t, ref[im * WIMG : (im + 1) * WIMG, :]) for im in range(PAIR)], 0
    ).astype(bf16)


def expand_heads(x, hm_ref):
    return jnp.concatenate([x * hm_ref[h : h + 1, :] for h in range(GROUP)], 0)


def fold_heads(o):
    lane = lax.broadcasted_iota(jnp.int32, (WROW, QUAD), 1) // HD
    acc = o[:WROW]
    for h in range(1, GROUP):
        acc = jnp.where(lane == h, o[h * WROW : (h + 1) * WROW], acc)
    return acc


def staged(stages, count, lag, at):
    for t in range(count + lag * (len(stages) - 1)):
        if t > 0 and t % SPAN == 0 and t // SPAN <= 2:
            at("attend", 2 + t // SPAN)
        for n, stage in enumerate(stages):
            if 0 <= t - lag * n < count:
                stage(t - lag * n)


def softmax_cols(s):
    e = jnp.exp2((s - jnp.max(s, 0, keepdims=True)) * (score_scale * log2_e))
    return e * (1.0 / jnp.sum(e, 0, keepdims=True))


def group_cols(g):
    base = (g // 2) * QKV + (g % 2) * QUAD
    return [slice(base + t * HALF, base + t * HALF + QUAD) for t in range(3)]


def attend_forward(x, wa, bias_ref, layer, vec_ref, nv_ref, perm, perm_t, hm_ref, qkv_ref, mixed_ref,
                   nperm, mixw, sc, prc, at):
    hat, _ = norm_stats(x)
    normed = hat * nv_ref[0:1, :] + nv_ref[1:2, :]
    to_window_rows(perm, normed, nperm)
    for m in range(2):
        r = dot(nperm[...], flat(wa[m, ..., :QKV]))
        base = m * QKV
        qkv_ref[:, base : base + HALF] = (r[:, :HALF] + vec_ref[m, layer, 1:2, :HALF]).astype(bf16)
        qkv_ref[:, base + HALF : base + 2 * HALF] = r[:, HALF : 2 * HALF].astype(bf16)
        qkv_ref[:, base + 2 * HALF : base + QKV] = (r[:, 2 * HALF :] + vec_ref[m, layer, 2:3, :HALF]).astype(bf16)
    at("attend", 1)
    units = [(w, g) for w in range(4 * PAIR) for g in range(GROUPS)]

    def scores(t):
        w, g = units[t]
        r = slice(w * WROW, (w + 1) * WROW)
        cq, ck, _ = group_cols(g)
        sc[t % SLOTS] = dot(qkv_ref[r, ck], expand_heads(qkv_ref[r, cq], hm_ref), 1, 1) + bias_ref[g // 2, layer * (1 + w % 4), g % 2]

    def middle(t):
        prc[t % SLOTS] = softmax_cols(sc[t % SLOTS]).astype(bf16)

    def mix(t):
        w, g = units[t]
        r = slice(w * WROW, (w + 1) * WROW)
        o = dot(prc[t % SLOTS], qkv_ref[r, group_cols(g)[2]], 0, 0)
        mixw[r, g * QUAD : (g + 1) * QUAD] = fold_heads(o).astype(bf16)

    staged((scores, middle, mix), len(units), LAG, at)
    mixed = to_token_rows(perm_t, mixw)
    mixed_ref[...] = mixed
    attn = dot(mixed[:, :HALF], flat(wa[0, ..., QKV:]), 1, 1) + dot(mixed[:, HALF:], flat(wa[1, ..., QKV:]), 1, 1)
    return x + attn + nv_ref[4:5, :]


CH = 512
SLOTS = 8
LAG = 2
SPAN = 12


def mlp_forward(mid, wm, vec_ref, layer, nv_ref, act_ref, slope_ref, at):
    hat, _ = norm_stats(mid)
    hid = (hat * nv_ref[2:3, :] + nv_ref[3:4, :]).astype(bf16)
    total = jnp.zeros((ROWS, D), f32)
    for m in range(2):
        for c in range(0, FFH, CH):
            col = m * FFH + c
            u = dot(hid, flat(wm[m, ..., c : c + CH])) + vec_ref[m, layer, 0:1, c : c + CH]
            t = u * root_half
            phi = 0.5 + 0.5 * lax.erf(t)
            act = (u * phi).astype(bf16)
            act_ref[:, col : col + CH] = act
            slope_ref[:, col : col + CH] = (phi + u * (jnp.exp2(t * t * -log2_e) * inv_root_two_pi)).astype(bf16)
            if col > 0:
                at("mlp", col // CH)
            total += dot(act, flat(wm[m, ..., FFH + c : FFH + c + CH]), 1, 1)
    return mid + total + nv_ref[5:6, :]


def mlp_backward(g_s, mid, wm, nv_ref, gp, hid_s, gb_s, rows, b1_acc, nv_acc, at):
    gout = g_s[rows, :]
    hat, inv = norm_stats(mid)
    hid_s[rows, :] = (hat * nv_ref[2:3, :] + nv_ref[3:4, :]).astype(bf16)
    gb = gout.astype(bf16)
    gb_s[rows, :] = gb
    ghid = jnp.zeros((ROWS, D), f32)
    for m in range(2):
        for c in range(0, FFH, CH):
            col = m * FFH + c
            g = dot(gb, flat(wm[m, ..., FFH + c : FFH + c + CH])) * gp[rows, col : col + CH].astype(f32)
            b1_acc[:, col : col + CH] += row_sum(g)
            g = g.astype(bf16)
            gp[rows, col : col + CH] = g
            if col > 0:
                at("mlp", col // CH)
            ghid += dot(g, flat(wm[m, ..., c : c + CH]), 1, 1)
    gmid = gout + norm_back(ghid, hat, inv, nv_ref[2:3, :])
    nv_acc[2:3, :] += row_sum(ghid * hat)
    nv_acc[3:4, :] += row_sum(ghid)
    nv_acc[4:5, :] += row_sum(gmid)
    nv_acc[5:6, :] += row_sum(gout)
    g_s[rows, :] = gmid


def attend_backward(g_s, x, wa, bias_ref, layer, nv_ref, perm, perm_t, hm_ref, qkv_ref,
                    mperm, gmw, gqw, gq_s, mb_s, nb_s, rows, ds_acc, qv_acc, nv_acc, sc, dpc, prc, dsc, at):
    gmid = g_s[rows, :]
    hat, inv = norm_stats(x)
    nb_s[rows, :] = (hat * nv_ref[0:1, :] + nv_ref[1:2, :]).astype(bf16)
    mb_s[rows, :] = gmid.astype(bf16)
    to_window_rows(perm, gmid, mperm)
    for m in range(2):
        gmw[:, m * HALF : (m + 1) * HALF] = dot(mperm[...], flat(wa[m, ..., QKV:])).astype(bf16)
    at("attend", 1)
    units = [(w, g) for w in range(4 * PAIR) for g in range(GROUPS)]

    def scores(t):
        w, g = units[t]
        r = slice(w * WROW, (w + 1) * WROW)
        cq, ck, cv = group_cols(g)
        sc[t % SLOTS] = dot(qkv_ref[r, ck], expand_heads(qkv_ref[r, cq], hm_ref), 1, 1) + bias_ref[g // 2, layer * (1 + w % 4), g % 2]
        dpc[t % SLOTS] = dot(qkv_ref[r, cv], expand_heads(gmw[r, g * QUAD : (g + 1) * QUAD], hm_ref), 1, 1)

    def middle(t):
        g = units[t][1]
        pr = softmax_cols(sc[t % SLOTS])
        prc[t % SLOTS] = pr.astype(bf16)
        dp = dpc[t % SLOTS]
        ds = pr * (dp - jnp.sum(pr * dp, 0, keepdims=True))
        ds_acc[g] += ds
        dsc[t % SLOTS] = ds.astype(bf16)

    def grads(t):
        w, g = units[t]
        r = slice(w * WROW, (w + 1) * WROW)
        cq, ck, cv = group_cols(g)
        own = slice(g * QUAD, (g + 1) * QUAD)
        gv = dot(prc[t % SLOTS], expand_heads(gmw[r, own], hm_ref))
        gk = dot(dsc[t % SLOTS], expand_heads(qkv_ref[r, cq], hm_ref)) * score_scale
        gq = fold_heads(dot(dsc[t % SLOTS], qkv_ref[r, ck], 0, 0)) * score_scale
        qv_acc[0:1, own] += row_sum(gq)
        qv_acc[1:2, own] += row_sum(gv)
        gqw[r, cq] = gq.astype(bf16)
        gqw[r, ck] = gk.astype(bf16)
        gqw[r, cv] = gv.astype(bf16)

    staged((scores, middle, grads), len(units), LAG, at)
    at("attend", 2)
    gq = to_token_rows(perm_t, gqw)
    gq_s[rows, :] = gq
    gnorm = dot(gq[:, :QKV], flat(wa[0, ..., :QKV]), 1, 1) + dot(gq[:, QKV:], flat(wa[1, ..., :QKV]), 1, 1)
    nv_acc[0:1, :] += row_sum(gnorm * hat)
    nv_acc[1:2, :] += row_sum(gnorm)
    g_s[rows, :] = g_s[rows, :] + norm_back(gnorm, hat, inv, nv_ref[0:1, :])


def forward_kernel(fast, steps, tok_ref, *refs):
    shards, refs = refs[: 4 if fast else 2], refs[4 if fast else 2 :]
    (bias_in, vec_in, nv_ref, perm_ref, perm_t_ref, hm_ref,
     out_ref, ys_ref, mid_ref, qkv_ref, mixed_ref, act_ref, slope_ref, wa_out, wm_out, bias_out,
     xs, mids, wa, wm, nperm, mixw, sc, prc, bias_ref, vec_ref, local, *sems) = refs
    s = pl.program_id(0)
    per = 2 * steps
    layer, r = s // per, lax.rem(s, per)
    pair = lax.rem(r, steps)
    rows = pl.ds(pl.multiple_of(pair * ROWS, ROWS), ROWS)
    weights = (wa, wm)
    me = lax.axis_index("mp")
    if fast:
        send, recv, own_a, own_m, ssend, srecv = sems
        own = (own_a, own_m)
        swaps = [
            remote(here, there.at[me], ssend.at[n], srecv.at[n], Place().core())
            for n, (here, there) in enumerate(((bias_in, bias_ref), (vec_in, vec_ref)))
        ]
        gathers = [
            Gather(own[n % 2].at[n // 2], weights[n % 2].at[n // 2], send.at[n], recv.at[n], local.at[n])
            for n in range(2 * LAYERS)
        ]

    def keep(n):
        return pltpu.make_async_copy(weights[n % 2].at[n // 2], (wa_out, wm_out)[n % 2].at[n // 2], local.at[4 + n])

    def at(step, point):
        if not fast:
            return
        for key, todo in FORWARD_PLAN.items():
            if key[1] == point and (key[0] % per < steps) == (step == "attend"):

                @pl.when(s == key[0])
                def _():
                    for n, stage in todo:
                        gathers[n].stage(stage)
                        if stage == Gather.STAGES - 1:
                            keep(n).start()

    keep_bias = pltpu.make_async_copy(bias_ref, bias_out, local.at[8])

    @pl.when(s == 0)
    def _():
        if fast:
            pack_shards(shards, own_a, own_m)
            neighbour_barrier(Place())
            for swap in swaps:
                swap.start()
        else:
            for n in range(2 * LAYERS):
                cp = pltpu.make_async_copy(shards[n % 2].at[n // 2], weights[n % 2].at[n // 2], local.at[n])
                cp.start()
                cp.wait()
            for here, there in ((bias_in, bias_ref), (vec_in, vec_ref)):
                there[...] = here[...]

    at("attend", 0)

    @pl.when(s == 0)
    def _():
        if fast:
            for here, there in ((bias_in, bias_ref), (vec_in, vec_ref)):
                there[me] = here[...]
            for swap in swaps:
                swap.wait()
        keep_bias.start()

    @pl.when(r < steps)
    def _():
        @pl.when(s < steps)
        def _():
            put_images(xs, rows, tok_ref)

        mid = attend_forward(xs[rows, :], wa.at[layer], bias_ref, layer, vec_ref, nv_ref.at[layer],
                             perm_ref[layer], perm_t_ref[layer], hm_ref, qkv_ref, mixed_ref, nperm, mixw, sc, prc, at)
        mid_ref[...] = mid
        mids[rows, :] = mid
        at("attend", 2)

    @pl.when(r >= steps)
    def _():
        at("mlp", 0)
        y = mlp_forward(mids[rows, :], wm.at[layer], vec_ref, layer, nv_ref.at[layer], act_ref, slope_ref, at)

        @pl.when(layer < LAYERS - 1)
        def _():
            xs[rows, :] = y
            ys_ref[...] = y

        @pl.when(layer == LAYERS - 1)
        def _():
            for im in range(PAIR):
                part = y[im * SEQP : im * SEQP + SEQ]
                out_ref[im] = part

    @pl.when(s == LAYERS * per - 1)
    def _():
        keep_bias.wait()
        if fast:
            for n in range(2 * LAYERS):
                keep(n).wait()


def pack_shards(shards, own_a, own_m):
    w_qkv, w_proj, w_one, w_two = shards
    for l in range(LAYERS):
        for k in range(3):
            own_a[l, :, k * HALF : (k + 1) * HALF] = w_qkv[l, k].astype(bf16)
        own_a[l, :, QKV:] = w_proj[l].astype(bf16)
        own_m[l, :, :FFH] = w_one[l].astype(bf16)
        own_m[l, :, FFH:] = w_two[l].astype(bf16)


FORWARD_PLAN = {(0, 0): [(0, 0), (1, 0), (0, 1), (0, 2), (0, 3), (1, 1), (0, 4), (1, 2), (1, 3), (0, 5), (0, 6), (2, 0)], (1, 1): [(1, 4), (3, 0)], (2, 1): [(1, 5), (2, 1)], (2, 2): [(2, 2), (2, 3)], (3, 0): [(1, 6)], (3, 2): [(2, 4), (3, 1)], (4, 0): [(3, 2)], (4, 2): [(2, 5), (3, 3)], (5, 2): [(2, 6)], (6, 1): [(3, 4)], (7, 4): [(3, 5)], (9, 0): [(3, 6)]}


def backward_kernel(fast, steps, cot_ref, tok_ref, ys_ref, mid_ref, qkv_ref, act_in, slope_in, mixed_in, wa_in, wm_in,
                    bias_ref, nv_ref, perm_ref, perm_t_ref, hm_ref, count_ref, *refs):
    if fast:
        gx_ref, ga_out, sum_m, sum_a, *refs = refs
    else:
        gx_ref, ga_out, gm_out, *refs = refs
    (qv_all, b1_all, ds_all, nv_all, g_s, xs, mperm, gmw, gqw, gp, gq_s, hid_s, gb_s, mb_s, nb_s, act_s, mixed_s,
     wa, wm, gwm, gwa, sc, dpc, prc, dsc, local, *comm) = refs
    s = pl.program_id(0)
    per = 2 * steps + 6
    turn, r = s // per, lax.rem(s, per)
    layer = LAYERS - 1 - turn
    first_g, first_a, last_g = steps, steps + 4, 2 * steps + 4
    pair = jnp.where(r < first_a, jnp.minimum(r, steps - 1), jnp.minimum(r - first_a, steps - 1))
    rows = pl.ds(pl.multiple_of(pair * ROWS, ROWS), ROWS)
    total = steps * ROWS
    qv_acc, b1_acc, ds_acc, nv_acc, nv_ref = (
        ref.at[layer] for ref in (qv_all, b1_all, ds_all, nv_all, nv_ref)
    )
    me = lax.axis_index("mp")
    if fast:
        scatters = [
            Scatter(gw.at[0], gw.at[1], *comm[8 * n : 8 * n + 8]) for n, gw in enumerate((gwm.at[0], gwm.at[1], gwa))
        ]
        pl.when(s == 0)(lambda: neighbour_barrier(Place()))

    def at(step, point):
        if not fast:
            return
        spans = {"mlp": (0, first_g), "g": (first_g, first_a), "attend": (first_a, last_g), "ga": (last_g, per)}
        for key, todo in BACKWARD_PLAN.items():
            lo, hi = spans[step]
            if key[1] == point and lo <= key[0] % per < hi:

                @pl.when(s == key[0])
                def _():
                    for n, stage in todo:
                        if stage == Scatter.STAGES - 1:
                            last = key[0] < per + first_a
                            scatters[n].result(sum_a.at[0] if n == 2 else sum_m.at[n, LAYERS - 1 if last else 0])
                        scatters[n].stage(stage)

    def rows_of(l):
        return pl.ds(l * total, total)

    def load(name, l):
        src, dst, n = {
            "wm": (wm_in.at[l], wm, 0), "wa": (wa_in.at[l], wa, 1), "act": (act_in.at[rows_of(l)], act_s, 2),
            "mixed": (mixed_in.at[rows_of(l)], mixed_s, 3), "slope": (slope_in.at[rows_of(l)], gp, 4),
        }[name]
        return pltpu.make_async_copy(src, dst, local.at[n])

    top = LAYERS - 1

    @pl.when(s == 0)
    def _():
        for name in ("wm", "slope", "wa", "act", "mixed"):
            load(name, top).start()

    for l in range(top, -1, -1):
        base = (top - l) * per
        for name, step in (("wm", 0), ("slope", 0), ("act", first_g), ("wa", first_a), ("mixed", last_g)):
            pl.when(s == base + step)(lambda name=name, l=l: load(name, l).wait())
        if l > 0:
            for name, step in (("wm", first_g), ("slope", first_a), ("act", first_a), ("wa", last_g), ("mixed", per)):
                pl.when(s == base + step)(lambda name=name, l=l: load(name, l - 1).start())

    @pl.when(r == 0)
    def _():
        for ref in (qv_acc, b1_acc, ds_acc, nv_acc):
            ref[...] = jnp.zeros(ref.shape, f32)

    @pl.when(r < first_g)
    def _():
        at("mlp", 0)

        @pl.when(turn == 0)
        def _():
            image = (me * steps + pair) * PAIR
            put_images(g_s, rows, cot_ref, lambda im, v: v * (image + im < count_ref[0]).astype(f32))

        mlp_backward(g_s, mid_ref[...], wm, nv_ref, gp, hid_s, gb_s, rows, b1_acc, nv_acc, at)

    def gradient(left, right, lo, width):
        cols = pl.ds(pl.multiple_of(lo, width), width)
        return dot(left[...], right[:, cols], 0, 0).astype(bf16).reshape(*gwa.shape[1:-1], width)

    @pl.when((r >= first_g) & (r < first_a))
    def _():
        at("g", 0)
        q = r - first_g
        own = lax.rem(q, 2)
        half = jnp.where(own == 1, me, 1 - me)

        @pl.when(q < 2)
        def _():
            gwm[0, own] = gradient(hid_s, gp, half * FFH, FFH)

        @pl.when(q >= 2)
        def _():
            gwm[1, own] = gradient(gb_s, act_s, half * FFH, FFH)

        at("g", 1)

    @pl.when((r >= first_a) & (r < last_g))
    def _():
        at("attend", 0)

        @pl.when(layer == 0)
        def _():
            put_images(xs, slice(None), tok_ref)

        @pl.when(layer > 0)
        def _():
            xs[...] = ys_ref[...]

        attend_backward(g_s, xs[...], wa, bias_ref, layer, nv_ref, perm_ref[layer], perm_t_ref[layer], hm_ref,
                        qkv_ref, mperm, gmw, gqw, gq_s, mb_s, nb_s, rows, ds_acc, qv_acc, nv_acc, sc, dpc, prc, dsc, at)

        @pl.when(layer == 0)
        def _():
            for im in range(PAIR):
                part = g_s.at[rows, :][im * SEQP : im * SEQP + SEQ]
                gx_ref[im] = part

    @pl.when(r >= last_g)
    def _():
        at("ga", 0)
        own = r - last_g
        half = jnp.where(own == 1, me, 1 - me)
        gwa[own, ..., :QKV] = gradient(nb_s, gq_s, half * QKV, QKV)
        gwa[own, ..., QKV:] = gradient(mb_s, mixed_s, half * HALF, HALF)
        at("ga", 1)

    def flush(src, dst):
        cp = pltpu.make_async_copy(src, dst, local.at[5])
        cp.start()
        cp.wait()

    if fast:
        pl.when(s == LAYERS * per - 1)(lambda: flush(gwa, ga_out))
    else:
        pl.when(r == first_a)(lambda: flush(gwm, gm_out.at[layer]))
        pl.when(r == per - 1)(lambda: flush(gwa, ga_out.at[layer]))


BACKWARD_PLAN = {(4, 0): [(0, 0)], (5, 1): [(0, 1)], (6, 0): [(1, 0)], (7, 1): [(1, 1)], (7, 2): [(0, 2)], (8, 4): [(0, 3)], (8, 2): [(1, 2)], (9, 2): [(1, 3)], (10, 1): [(0, 4)], (11, 0): [(2, 0)], (12, 1): [(2, 1)], (13, 1): [(1, 4)], (14, 0): [(2, 2)], (15, 0): [(2, 3)], (16, 0): [(0, 0)], (17, 0): [(2, 4)], (17, 1): [(0, 1)], (18, 0): [(1, 0)], (19, 1): [(1, 1)], (19, 2): [(0, 2)], (20, 4): [(0, 3)], (20, 2): [(1, 2)], (21, 2): [(1, 3)], (22, 1): [(0, 4)], (23, 1): [(1, 4)]}


def whole(shape, buffers=1):
    zero = (0,) * len(shape)
    return pl.BlockSpec(shape, lambda i: zero, pipeline_mode=pl.Buffered(buffers))


VLIM = 65000000


def forward(tok, shards, bias, vecs, nv, perm, perm_t, hm, fast, steps):
    per = 2 * steps
    rows = steps * ROWS
    slots = (2, NZ, NY, NX, D // PEERS) if fast else (2, 1, 1, 1, D)
    wide = (COLS - ATT, ATT)
    any_ = pl.BlockSpec(memory_space=pl.ANY)

    def attend(s):
        return s // per * steps + jnp.minimum(lax.rem(s, per), steps - 1)

    def mlp(s):
        return s // per * steps + jnp.maximum(lax.rem(s, per) - steps, 0)

    sems = []
    if fast:
        sems = [pltpu.SemaphoreType.DMA((2 * LAYERS, Gather.SEMS))] * 2
        sems += [pltpu.VMEM((LAYERS, D // PEERS, n), bf16) for n in wide] + [pltpu.SemaphoreType.DMA((2,))] * 2
    halves = [(2, *a.shape) if fast else a.shape for a in (bias, vecs)]
    params = dict(collective_id=1, has_side_effects=True) if fast else {}
    return pl.pallas_call(
        functools.partial(forward_kernel, fast, steps),
        name="forward",
        grid=(LAYERS * per,),
        in_specs=[
            pl.BlockSpec((PAIR, SEQ, D), lambda s: (lax.axis_index("mp") * steps + jnp.minimum(s, steps - 1), 0, 0)),
            *(whole(w.shape) if fast else any_ for w in shards),
            *(whole(a.shape) for a in (bias, vecs, nv, perm, perm_t, hm)),
        ],
        out_specs=[
            pl.BlockSpec((PAIR, SEQ, D), lambda s: (jnp.maximum(s - (LAYERS * per - steps), 0), 0, 0)),
            pl.BlockSpec((ROWS, D), lambda s: (jnp.clip(s - steps, 0, steps - 1), 0)),
            pl.BlockSpec((ROWS, D), lambda s: (attend(s), 0)),
            pl.BlockSpec((WPAIR, 2 * QKV), lambda s: (attend(s), 0)),
            pl.BlockSpec((ROWS, D), lambda s: (attend(s), 0)),
            pl.BlockSpec((ROWS, 2 * FFH), lambda s: (mlp(s), 0)),
            pl.BlockSpec((ROWS, 2 * FFH), lambda s: (mlp(s), 0)),
            any_, any_, any_,
        ],
        out_shape=[
            jax.ShapeDtypeStruct((steps * PAIR, SEQ, D), f32),
            jax.ShapeDtypeStruct((rows, D), f32),
            jax.ShapeDtypeStruct((LAYERS * rows, D), f32),
            jax.ShapeDtypeStruct((LAYERS * steps * WPAIR, 2 * QKV), bf16),
            jax.ShapeDtypeStruct((LAYERS * rows, D), bf16),
            jax.ShapeDtypeStruct((LAYERS * rows, 2 * FFH), bf16),
            jax.ShapeDtypeStruct((LAYERS * rows, 2 * FFH), bf16),
            *(jax.ShapeDtypeStruct((LAYERS, *slots, n), bf16) for n in wide),
            jax.ShapeDtypeStruct(halves[0], f32),
        ],
        scratch_shapes=[
            pltpu.VMEM((rows, D), f32), pltpu.VMEM((rows, D), f32),
            *(pltpu.VMEM((LAYERS, *slots, n), bf16) for n in wide),
            pltpu.VMEM((WPAIR, D), bf16), pltpu.VMEM((WPAIR, D), bf16),
            pltpu.VMEM((SLOTS, WROW, LANES), f32), pltpu.VMEM((SLOTS, WROW, LANES), bf16),
            *(pltpu.VMEM(n, f32) for n in halves),
            pltpu.SemaphoreType.DMA((9,)), *sems,
        ],
        compiler_params=pltpu.CompilerParams(vmem_limit_bytes=VLIM, **params),
    )(tok, *shards, bias, vecs, nv, perm, perm_t, hm)


def backward(cot, tok, saved, weights, bias, nv, perm, perm_t, hm, count, fast, steps):
    ys, mid, qkv, mixed, act, slope = saved
    wa, wm = weights
    per = 2 * steps + 6
    rows = steps * ROWS
    slots = wa.shape[1:-1]
    rest = slots[1:]
    any_ = pl.BlockSpec(memory_space=pl.ANY)

    def clip(v):
        return jnp.clip(v, 0, steps - 1)

    def layer(s):
        return LAYERS - 1 - s // per

    attend0 = (LAYERS - 1) * per + steps + 4
    img = lambda at: pl.BlockSpec((PAIR, SEQ, D), lambda s: (clip(s - at), 0, 0))
    mine = lambda at: pl.BlockSpec((PAIR, SEQ, D), lambda s: (lax.axis_index("mp") * steps + clip(s - at), 0, 0))
    wide = (COLS - ATT, ATT)
    part = rest[-1]
    if fast:
        outs = [
            jax.ShapeDtypeStruct((2, *rest, COLS - ATT), bf16),
            jax.ShapeDtypeStruct((2, LAYERS, part, FFH), f32), jax.ShapeDtypeStruct((1, part, COLS - ATT), f32),
        ]
        specs = [any_, whole(outs[1].shape), whole(outs[2].shape)]
        comm = Scatter.landing(part, FFH) * 2 + Scatter.landing(part, COLS - ATT)
        params = dict(collective_id=2, has_side_effects=True)
    else:
        outs = [
            jax.ShapeDtypeStruct((LAYERS, 2, *rest, COLS - ATT), bf16),
            jax.ShapeDtypeStruct((LAYERS, 2, 2, *rest, FFH), bf16),
        ]
        specs, comm, params = [any_, any_], [], {}
    small = [(LAYERS, 2, 2 * HALF), (LAYERS, 1, 2 * FFH), (LAYERS, GROUPS, WROW, LANES), (LAYERS, 8, D)]
    return pl.pallas_call(
        functools.partial(backward_kernel, fast, steps),
        name="backward",
        grid=(LAYERS * per,),
        in_specs=[
            mine(0), mine(attend0),
            pl.BlockSpec((ROWS, D), lambda s: (clip(s - steps - 4), 0)),
            pl.BlockSpec((ROWS, D), lambda s: (layer(s) * steps + clip(lax.rem(s, per)), 0)),
            pl.BlockSpec((WPAIR, 2 * QKV), lambda s: (layer(s) * steps + clip(lax.rem(s, per) - steps - 4), 0)),
            any_, any_, any_, any_, any_,
            *(whole(a.shape) for a in (bias, nv, perm, perm_t, hm)),
            pl.BlockSpec(memory_space=pltpu.SMEM),
        ],
        out_specs=[img(attend0), *specs, *(whole(n) for n in small)],
        out_shape=[
            jax.ShapeDtypeStruct((steps * PAIR, SEQ, D), f32), *outs, *(jax.ShapeDtypeStruct(n, f32) for n in small),
        ],
        scratch_shapes=[
            pltpu.VMEM((rows, D), f32), pltpu.VMEM((ROWS, D), f32),
            pltpu.VMEM((WPAIR, D), bf16), pltpu.VMEM((WPAIR, D), bf16), pltpu.VMEM((WPAIR, 2 * QKV), bf16),
            pltpu.VMEM((rows, 2 * FFH), bf16), pltpu.VMEM((rows, 2 * QKV), bf16),
            *[pltpu.VMEM((rows, D), bf16)] * 4,
            pltpu.VMEM((rows, 2 * FFH), bf16), pltpu.VMEM((rows, D), bf16),
            *(pltpu.VMEM((*slots, n), bf16) for n in wide),
            pltpu.VMEM((2, 2, *rest, FFH), bf16), pltpu.VMEM((2, *rest, COLS - ATT), bf16),
            *[pltpu.VMEM((SLOTS, WROW, LANES), f32)] * 2, *[pltpu.VMEM((SLOTS, WROW, LANES), bf16)] * 2,
            pltpu.SemaphoreType.DMA((8,)), *comm,
        ],
        compiler_params=pltpu.CompilerParams(vmem_limit_bytes=VLIM, **params),
    )(cot, tok, ys, mid, qkv, act, slope, mixed, wa, wm, bias, nv, perm, perm_t, hm, count)


def head_mask():
    return (np.arange(QUAD)[None, :] // HD == np.arange(GROUP)[:, None]).astype(np.float32)


def exact_parts(a):
    parts = []
    for _ in range(3):
        top = lax.reduce_precision(a, 8, 7)
        parts.append(top.astype(bf16))
        a = a - top
    return jnp.stack(parts)


def bias_cols(onehot, table):
    picked = jnp.einsum("jti,smlth->sjmlhi", onehot.astype(bf16), exact_parts(table), preferred_element_type=f32)
    picked = (picked[0] + picked[1] + picked[2]).transpose(1, 2, 0, 3, 4)
    picked = picked.reshape(-1, LAYERS, WROW, 2, GROUP, WROW).transpose(0, 1, 3, 2, 4, 5)
    apart = np.concatenate([np.zeros((1, WROW, WROW), np.float32), region_mask()])
    apart[:, WSEQ:] = pad_fill
    both = jnp.concatenate([picked[:, :1]] + [picked[:, 1:]] * 4, 1)
    both = (both + jnp.asarray(apart)[:, None, :, None, :]) * (1.0 / score_scale)
    return both.reshape(-1, 5, 2, WROW, LANES)

NZ, NY, NX = 4, 2, 2
PEERS = NZ * NY * NX
MESH_ID = pl.DeviceIdType.MESH


class Place:
    def __init__(self):
        d = lax.axis_index("dp")
        self.d, self.m = d, lax.axis_index("mp")
        self.z, self.y, self.x = d // 4, lax.rem(d // 2, 2), lax.rem(d, 2)

    def chip(self, z, y, x):
        return (z * NY + y) * NX + x

    def at(self, y=None, x=None, m=None):
        y = self.y if y is None else y
        x = self.x if x is None else x
        return (self.chip(self.z, y, x), self.m if m is None else m)

    def xn(self):
        return self.at(x=1 - self.x)

    def yn(self):
        return self.at(y=1 - self.y)

    def core(self):
        return self.at(m=1 - self.m)

    def column(self, z):
        return (self.chip(z, self.y, self.x), self.m)


def remote(src, dst, send, recv, to):
    return pltpu.make_async_remote_copy(
        src_ref=src, dst_ref=dst, send_sem=send, recv_sem=recv, device_id=to, device_id_type=MESH_ID
    )


def neighbour_barrier(p):
    sem = pltpu.get_barrier_semaphore()
    partners = [p.xn(), p.yn(), p.core()] + [p.column(lax.rem(p.z + n, NZ)) for n in range(1, NZ)]
    for to in partners:
        pl.semaphore_signal(sem, inc=1, device_id=to, device_id_type=MESH_ID)
    pl.semaphore_wait(sem, len(partners))


def each_plane(body):
    lax.fori_loop(0, NZ, lambda k, carry: (body(k), carry)[1], 0)


class Gather:
    SEMS = 48
    BASE = {"z": 0, "xa": 4, "yb": 8, "ya0": 12, "ya1": 16, "xb0": 20, "xb1": 24,
            "own": 28, "ax": 32, "by": 36, "ar": 40, "br": 44}

    def __init__(self, own, full, send, recv, local):
        self.p, self.own, self.full = Place(), own, full
        self.send, self.recv, self.local = send, recv, local
        half = full.shape[-1] // 2
        self.all, self.a, self.b = pl.ds(0, 2 * half), pl.ds(0, half), pl.ds(half, half)

    def region(self, kind, k, arrived):
        p = self.p
        oy, ox = 1 - p.y, 1 - p.x
        if kind == "z":
            return (p.m, k if arrived else p.z, p.y, p.x), self.all, p.column(k)
        if kind == "xa":
            return (p.m, k, p.y, ox if arrived else p.x), self.a, p.xn()
        if kind == "yb":
            return (p.m, k, oy if arrived else p.y, p.x), self.b, p.yn()
        if kind in ("ya0", "ya1"):
            return (p.m, k, oy if arrived else p.y, p.x if kind == "ya0" else ox), self.a, p.yn()
        if kind in ("xb0", "xb1"):
            return (p.m, k, p.y if kind == "xb0" else oy, ox if arrived else p.x), self.b, p.xn()
        m = 1 - p.m if arrived else p.m
        if kind == "own":
            return (m, k, p.y, p.x), self.all, p.core()
        if kind == "ax":
            return (m, k, p.y, ox), self.a, p.core()
        if kind == "by":
            return (m, k, oy, p.x), self.b, p.core()
        if kind == "ar":
            return (m, k, oy, slice(None)), self.a, p.core()
        return (m, k, slice(None), ox), self.b, p.core()

    def copy(self, kind, k, own=False, arrived=False):
        at, cols, to = self.region(kind, k, arrived)
        dst = self.full.at[(*at, slice(None), cols)]
        src = self.own.at[:, cols] if own else dst
        s = self.BASE[kind] + k
        r = self.p.z if kind == "z" and not arrived else s
        return remote(src, dst, self.send.at[s], self.recv.at[r], to)

    def keep(self):
        p = self.p
        return pltpu.make_async_copy(
            self.own.at[:, self.all], self.full.at[p.m, p.z, p.y, p.x, :, self.all], self.local
        )

    def fan(self, k, own=False):
        for kind in ("xa", "yb", "ya0", "xb0", "own"):
            self.copy(kind, k, own).start()

    def stage(self, n):
        p = self.p
        if n == 0:
            self.keep().start()
            for dist in (1, 2, 3):
                for k in (p.z + dist, p.z - dist):
                    pl.when((k >= 0) & (k < NZ))(lambda k=k: self.copy("z", k, True).start())
            self.fan(p.z, True)
        elif n <= 3:
            for k in (p.z + n, p.z - n):

                @pl.when((k >= 0) & (k < NZ))
                def _():
                    self.copy("z", k, arrived=True).wait_recv()
                    self.fan(k)
        elif n == 4:

            @each_plane
            def _(k):
                self.copy("xa", k, arrived=True).wait_recv()
                for kind in ("ya1", "ax"):
                    self.copy(kind, k).start()
                self.copy("yb", k, arrived=True).wait_recv()
                for kind in ("xb1", "by"):
                    self.copy(kind, k).start()
        elif n == 5:

            @each_plane
            def _(k):
                for kind, rest in (("ya", "ar"), ("xb", "br")):
                    for rel in ("0", "1"):
                        self.copy(kind + rel, k, arrived=True).wait_recv()
                    self.copy(rest, k).start()
        else:

            @each_plane
            def _(k):
                for kind in ("own", "ax", "by", "ar", "br"):
                    self.copy(kind, k, arrived=True).wait_recv()
                for kind in self.BASE:
                    if kind != "z":
                        self.copy(kind, k).wait_send()
                pl.when(k != p.z)(lambda: self.copy("z", k, True).wait_send())

            self.keep().wait()

    STAGES = 7


def add_into(ref, at, other):
    ref[at] = ref[at] + other


class Scatter:
    SEMS = 24
    BASE = {"core": 0, "ya": 4, "xb": 8, "xa": 12, "yb": 16, "z": 20}

    @staticmethod
    def landing(rows, cols):
        half = cols // 2
        return [
            pltpu.VMEM((NZ, NY, NX, rows, cols), bf16),
            pltpu.VMEM((NZ, NX, rows, half), bf16), pltpu.VMEM((NZ, NY, rows, half), bf16),
            pltpu.VMEM((NZ, rows, half), bf16), pltpu.VMEM((NZ, rows, half), bf16),
            pltpu.VMEM((NZ, rows, cols), bf16),
            pltpu.SemaphoreType.DMA((Scatter.SEMS,)), pltpu.SemaphoreType.DMA((Scatter.SEMS,)),
        ]

    def __init__(self, give, part, other, ya, xb, xa, yb, z, send, recv):
        self.p, self.give, self.part, self.other = Place(), give, part, other
        self.land = {"ya": ya, "xb": xb, "xa": xa, "yb": yb, "z": z}
        self.send, self.recv = send, recv
        half = part.shape[-1] // 2
        self.a, self.b = pl.ds(0, half), pl.ds(half, half)

    def copy(self, kind, k):
        p = self.p
        oy, ox = 1 - p.y, 1 - p.x
        full = slice(None)
        if kind == "core":
            src, dst, to = self.give.at[k], self.other.at[k], p.core()
        else:
            at, to = {
                "ya": ((k, oy, full, full, self.a), p.yn()),
                "xb": ((k, full, ox, full, self.b), p.xn()),
                "xa": ((k, p.y, ox, full, self.a), p.xn()),
                "yb": ((k, oy, p.x, full, self.b), p.yn()),
                "z": ((k, p.y, p.x, full, full), p.column(k)),
            }[kind]
            src, dst = self.part.at[at], self.land[kind].at[p.z if kind == "z" else k]
        s = self.BASE[kind] + k
        r = self.BASE[kind] + p.z if kind == "z" else s
        return remote(src, dst, self.send.at[s], self.recv.at[r], to)

    def landed(self, k):
        s = self.BASE["z"] + k
        at = self.land["z"].at[k]
        return remote(at, at, self.send.at[s], self.recv.at[s], self.p.column(k))

    def stage(self, n):
        p = self.p
        oy, ox = 1 - p.y, 1 - p.x
        if n == 0:
            each_plane(lambda k: self.copy("core", k).start())
        elif n == 1:

            @each_plane
            def _(k):
                self.copy("core", k).wait_recv()
                for y in range(NY):
                    for x in range(NX):
                        add_into(self.part, (k, y, x), self.other[k, y, x])
                self.copy("ya", k).start()
                self.copy("xb", k).start()
        elif n == 2:

            @each_plane
            def _(k):
                self.copy("ya", k).wait_recv()
                for x in range(NX):
                    add_into(self.part, (k, p.y, x, slice(None), self.a), self.land["ya"][k, x])
                self.copy("xa", k).start()
                self.copy("xb", k).wait_recv()
                for y in range(NY):
                    add_into(self.part, (k, y, p.x, slice(None), self.b), self.land["xb"][k, y])
                self.copy("yb", k).start()
        elif n == 3:

            @each_plane
            def _(k):
                self.copy("xa", k).wait_recv()
                add_into(self.part, (k, p.y, p.x, slice(None), self.a), self.land["xa"][k])
                self.copy("yb", k).wait_recv()
                add_into(self.part, (k, p.y, p.x, slice(None), self.b), self.land["yb"][k])

            for dist in (3, 2, 1):
                for k in (p.z + dist, p.z - dist):
                    pl.when((k >= 0) & (k < NZ))(lambda k=k: self.copy("z", k).start())
        else:

            @each_plane
            def _(k):
                for kind in ("core", "ya", "xb", "xa", "yb"):
                    self.copy(kind, k).wait_send()
                pl.when(k != p.z)(lambda: self.copy("z", k).wait_send())

    STAGES = 5

    def result(self, out):
        p = self.p
        out[...] = self.part[p.z, p.y, p.x].astype(f32)

        @each_plane
        def _(k):
            @pl.when(k != p.z)
            def _():
                self.landed(k).wait_recv()
                out[...] += self.land["z"][k].astype(f32)


class Total:
    STEPS = 5

    @staticmethod
    def scratch(shape):
        return [
            pltpu.VMEM((Total.STEPS, *shape), f32), pltpu.VMEM((Total.STEPS, *shape), f32),
            pltpu.SemaphoreType.DMA((Total.STEPS,)), pltpu.SemaphoreType.DMA((Total.STEPS,)),
        ]

    def __init__(self, start, held, land, send, recv):
        self.p, self.start, self.held, self.land, self.send, self.recv = Place(), start, held, land, send, recv

    def copy(self, n):
        p = self.p
        pair = p.z + 1 - 2 * lax.rem(p.z, 2)
        far = lax.rem(p.z + 2, NZ)
        to = (p.core(), p.yn(), p.xn(), (p.chip(pair, p.y, p.x), p.m), (p.chip(far, p.y, p.x), p.m))[n]
        src = self.start if n == 0 else self.held.at[n - 1]
        return remote(src, self.land.at[n], self.send.at[n], self.recv.at[n], to)

    def stage(self, n):
        if n > 0:
            self.copy(n - 1).wait_recv()
            before = self.start[...] if n == 1 else self.held[n - 2]
            self.held[n - 1] = before + self.land[n - 1]
        if n < self.STEPS:
            self.copy(n).start()
        else:
            for k in range(self.STEPS):
                self.copy(k).wait_send()


def tail_kernel(grad_ref, small_ref, out_ref, small_out, part, *refs):
    neighbour_barrier(Place())
    total = Total(small_ref, *refs[-4:])
    width = part.shape[-1]
    spans = [pl.ds(n * width, width) for n in range(2)]
    pieces = [
        Scatter(grad_ref.at[0, ..., cols], part.at[n], *refs[8 * n : 8 * n + 8]) for n, cols in enumerate(spans)
    ]
    for s in pieces:
        s.stage(0)
    total.stage(0)
    for n, cols in enumerate(spans):
        part[n] = grad_ref[1, ..., cols]
    for n in range(1, Scatter.STAGES - 1):
        for s in pieces:
            s.stage(n)
        total.stage(n)
    total.stage(Scatter.STAGES - 1)
    for s, cols in zip(pieces, spans):
        s.result(out_ref.at[:, cols])
        s.stage(Scatter.STAGES - 1)
    total.stage(Total.STEPS)
    small_out[...] = total.held[Total.STEPS - 1]


def tail(grad, small):
    rows, cols = grad.shape[-2:]
    half = cols // 2
    vm = pl.BlockSpec(memory_space=pltpu.VMEM)
    return pl.pallas_call(
        tail_kernel,
        name="tail",
        out_shape=[jax.ShapeDtypeStruct((rows, cols), f32), jax.ShapeDtypeStruct(small.shape, f32)],
        in_specs=[vm] * 2,
        out_specs=[vm] * 2,
        scratch_shapes=[pltpu.VMEM((2, *grad.shape[1:-1], half), bf16)] + Scatter.landing(rows, half) * 2
        + Total.scratch(small.shape),
        compiler_params=pltpu.CompilerParams(collective_id=3, has_side_effects=True, vmem_limit_bytes=VLIM),
    )(grad, small)


def adam_update(weight_in, moment_one, moment_two, grad_sum, decay):
    new_one = beta_one * moment_one + (1.0 - beta_one) * grad_sum
    new_two = beta_two * moment_two + (1.0 - beta_two) * grad_sum * grad_sum
    hat_one = new_one / (1.0 - beta_one**adam_step)
    hat_two = new_two / (1.0 - beta_two**adam_step)
    new_weight = weight_in - learn_rate * (hat_one / (jnp.sqrt(hat_two) + adam_eps) + decay * weight_in)
    return (new_weight, new_one, new_two)


def both_halves(mine, me):
    other = lax.ppermute(mine, "mp", [(0, 1), (1, 0)])
    low = jnp.where(me == 0, mine, other)
    high = jnp.where(me == 0, other, mine)
    return jnp.concatenate([low, high], 0)


HEADS = GROUPS * GROUP
LITTLE = 4 * HALF + 2 * FFH + HEADS * TABLE + 6 * D


def lanes_of(a):
    flat = a.reshape(-1)
    return jnp.pad(flat, (0, -flat.size % 1024)).reshape(-1, 128)


def sum_of_all(a):
    a = a.reshape(LAYERS, 2, D, a.shape[-1])
    total = a[:, 1].astype(f32) + lax.ppermute(a[:, 0], "mp", [(0, 1), (1, 0)]).astype(f32)
    return lax.psum_scatter(total.astype(bf16), "dp", scatter_dimension=1, tiled=True).astype(f32)


def pair_onehot(rel_index):
    index = jnp.pad(rel_index.T, ((0, WROW - WSEQ), (0, WROW - WSEQ)), constant_values=-1)
    return (index[:, None, :] == jnp.arange(TABLE, dtype=jnp.int32)[None, :, None]).astype(f32)


def local(
    fast, tokens, cotangent, image_count, rel_index,
    w_qkv, w_proj, w_fc_one, w_fc_two, qv_bias, fc_one_bias, rel_table, norm_vec,
    m_qkv, m_proj, m_fc_one, m_fc_two, m_qv_bias, m_fc_one_bias, m_rel_table, m_norm_vec,
    v_qkv, v_proj, v_fc_one, v_fc_two, v_qv_bias, v_fc_one_bias, v_rel_table, v_norm_vec,
):
    me = lax.axis_index("mp")
    images = tokens.shape[0]
    nimg = images // 2
    steps = nimg // PAIR
    part = w_qkv.shape[1]
    tok, cot = tokens, cotangent
    onehot = pair_onehot(rel_index)
    vecs = jnp.concatenate([fc_one_bias[:, None], jnp.pad(qv_bias, ((0, 0), (0, 5), (0, FFH - HALF)))], 1)
    shards = (w_qkv.transpose(0, 2, 1, 3), w_proj.transpose(0, 2, 1), w_fc_one, w_fc_two.transpose(0, 2, 1))
    if fast:
        bias = bias_cols(onehot, rel_table[None])[0]
    else:
        wm = jnp.concatenate([w_fc_one, w_fc_two.transpose(0, 2, 1)], 2).astype(bf16)
        wa = jnp.concatenate([w_qkv.reshape(LAYERS, part, QKV), w_proj.transpose(0, 2, 1)], 2).astype(bf16)
        shards = [
            lax.all_gather(w, ("mp", "dp")).reshape(2, -1, LAYERS, part, w.shape[-1]).transpose(2, 0, 1, 3, 4)
            .reshape(LAYERS, 2, 1, 1, 1, D, w.shape[-1])
            for w in (wa, wm)
        ]
        vecs = lax.all_gather(vecs, "mp")
        bias = bias_cols(onehot, lax.all_gather(rel_table, "mp"))
    hm = jnp.asarray(head_mask(), bf16)
    perms = np.stack([permutation(layer % 2 == 1) for layer in range(LAYERS)])
    perm, perm_t = jnp.asarray(perms, bf16), jnp.asarray(perms.transpose(0, 2, 1), bf16)
    out, *saved, all_wa, all_wm, bias = forward(
        tok, shards, bias, vecs, norm_vec, perm, perm_t, hm, fast, steps
    )
    weights = (all_wa, all_wm) if fast else shards
    out = both_halves(out, me)
    x_grad, *grads, gqv, gb1, ds, gnv = backward(
        cot, tok, saved, weights, bias, norm_vec, perm, perm_t, hm, image_count, fast, steps
    )
    x_grad = both_halves(x_grad, me)
    ds = ds.reshape(LAYERS, GROUPS, WROW, GROUP, WROW)
    gt = jnp.einsum("lgjhi,jti->lght", ds, onehot, precision=lax.Precision.HIGHEST)
    little = jnp.concatenate([a.reshape(LAYERS, -1) for a in (gqv, gb1, gt, gnv[:, :6])], 1)
    if fast:
        ga, sum_m, sum_a = grads
        last, total = tail(ga, lanes_of(little))
        big_a, big_m = jnp.stack([last, sum_a[0]]), sum_m
        little = total.reshape(-1)[: LAYERS * LITTLE].reshape(LAYERS, LITTLE)
    else:
        ga, gm = grads
        big_a, big_m = sum_of_all(ga), jnp.stack([sum_of_all(gm[:, n]) for n in range(2)])
        little = lax.psum(little, ("dp", "mp"))
    one_grad = big_m[0]
    two_grad = big_m[1].transpose(0, 2, 1)
    qkv_grad = big_a[:, :, :QKV].reshape(LAYERS, part, 3, HALF)
    proj_grad = big_a[:, :, QKV:].transpose(0, 2, 1)
    cut = lambda a: lax.dynamic_index_in_dim(a, me, 1, keepdims=False)
    at = 2 * 2 * HALF
    qv_grad = cut(little[:, :at].reshape(LAYERS, 2, 2, HALF).transpose(0, 2, 1, 3))
    bias_grad = cut(little[:, at : at + 2 * FFH].reshape(LAYERS, 2, FFH))
    at += 2 * FFH
    table_grad = cut(little[:, at : at + HEADS * TABLE].reshape(LAYERS, 2, HEADS // 2, TABLE)).transpose(0, 2, 1)
    at += HEADS * TABLE
    norm_grad = little[:, at:].reshape(LAYERS, 6, D)
    groups = [
        adam_update(w_qkv, m_qkv, v_qkv, qkv_grad, decay_rate),
        adam_update(w_proj, m_proj, v_proj, proj_grad, decay_rate),
        adam_update(w_fc_one, m_fc_one, v_fc_one, one_grad, decay_rate),
        adam_update(w_fc_two, m_fc_two, v_fc_two, two_grad, decay_rate),
        adam_update(qv_bias, m_qv_bias, v_qv_bias, qv_grad, 0.0),
        adam_update(fc_one_bias, m_fc_one_bias, v_fc_one_bias, bias_grad, 0.0),
        adam_update(rel_table, m_rel_table, v_rel_table, table_grad, 0.0),
        adam_update(norm_vec, m_norm_vec, v_norm_vec, norm_grad, 0.0),
    ]
    return (out, x_grad, *[grp[k] for k in range(3) for grp in groups])


def solution(mesh):
    params = (
        P(None, "dp", None, "mp"), P(None, "mp", "dp"), P(None, "dp", "mp"), P(None, "mp", "dp"),
        P(None, None, "mp"), P(None, "mp"), P(None, None, "mp"), P(),
    )
    act = (P("dp", None, None), P("dp", None, None))
    return jax.shard_map(
        functools.partial(local, mesh.shape["dp"] == PEERS),
        mesh=mesh,
        in_specs=(*act, P("dp"), P(), *params, *params, *params),
        out_specs=(*act, *params, *params, *params),
        check_vma=False,
    )
```

```python
import functools

import jax
import jax.numpy as jnp
import numpy as np
from jax import lax
from jax.experimental import pallas as pl
from jax.experimental.pallas import tpu as pltpu
from jax.sharding import PartitionSpec as P

D = 512
HD = 32
SIDE = 14
WIN = 7
SHIFT = 3
SEQ = 196
WSEQ = 49
TABLE = 169
LAYERS = 2
SEQP = 200
PAIR = 2
ROWS = PAIR * SEQP
WROW = 64
WIMG = 4 * WROW
WPAIR = PAIR * WIMG
HALF = 256
GROUP = 4
GROUPS = 4
QUAD = GROUP * HD
LANES = GROUP * WROW
FFH = 1024
QKV = 3 * HALF
COLS = 2 * FFH + QKV + HALF
ATT = 2 * FFH

norm_eps = 1e-05
mask_fill = -100.0
pad_fill = -1e30
beta_one = 0.9
beta_two = 0.999
adam_eps = 1e-08
learn_rate = 0.02
decay_rate = 0.05
adam_step = 3.0
root_half = 0.7071067811865476
inv_root_two_pi = 0.3989422804014327
score_scale = HD**-0.5
log2_e = 1.4426950408889634

f32 = jnp.float32
bf16 = jnp.bfloat16


def dot(a, b, ca=1, cb=0):
    return lax.dot_general(a, b, (((ca,), (cb,)), ((), ())), preferred_element_type=f32)


def window_tokens(shifted):
    off = SHIFT if shifted else 0
    out = np.zeros((4, WSEQ), np.int64)
    for wr in range(2):
        for wc in range(2):
            for p in range(WSEQ):
                r = (7 * wr + p // 7 + off) % SIDE
                c = (7 * wc + p % 7 + off) % SIDE
                out[wr * 2 + wc, p] = r * SIDE + c
    return out


def permutation(shifted):
    tok = window_tokens(shifted)
    perm = np.zeros((WIMG, SEQP), np.float32)
    for w in range(4):
        perm[w * WROW + np.arange(WSEQ), tok[w]] = 1.0
    return perm


def region_mask():
    pos = np.arange(SIDE)
    band = (pos >= SIDE - WIN).astype(int) + (pos >= SIDE - SHIFT).astype(int)
    region = 3 * band[:, None] + band[None, :]
    win = region.reshape(2, WIN, 2, WIN).transpose(0, 2, 1, 3).reshape(4, WSEQ)
    out = np.zeros((4, WROW, WROW), np.float32)
    out[:, :WSEQ, :WSEQ] = np.where(win[:, :, None] != win[:, None, :], mask_fill, 0.0)
    return out


def norm_stats(z):
    mean = jnp.mean(z, -1, keepdims=True)
    cen = z - mean
    var = jnp.mean(cen * cen, -1, keepdims=True)
    inv = lax.rsqrt(var + norm_eps)
    return cen * inv, inv


def norm_back(e, hat, inv, gain):
    s = e * gain
    return inv * (s - jnp.mean(s, -1, keepdims=True) - hat * jnp.mean(s * hat, -1, keepdims=True))


def row_sum(v):
    return jnp.sum(v, 0, keepdims=True)


def put_images(ref, rows, blk, scale=lambda im, v: v):
    part = ref.at[rows, :]
    for im in range(PAIR):
        part[im * SEQP : im * SEQP + SEQ, :] = scale(im, blk[im].astype(f32))
        part[im * SEQP + SEQ : (im + 1) * SEQP, :] = jnp.zeros((SEQP - SEQ, D), f32)


def flat(v):
    return v.reshape(D, v.shape[-1])


def to_window_rows(perm, rows, out_ref):
    for im in range(PAIR):
        part = rows[im * SEQP : (im + 1) * SEQP].astype(bf16)
        out_ref[im * WIMG : (im + 1) * WIMG, :] = dot(perm, part).astype(bf16)


def to_token_rows(perm_t, ref):
    return jnp.concatenate(
        [dot(perm_t, ref[im * WIMG : (im + 1) * WIMG, :]) for im in range(PAIR)], 0
    ).astype(bf16)


def expand_heads(x, hm_ref):
    return jnp.concatenate([x * hm_ref[h : h + 1, :] for h in range(GROUP)], 0)


def fold_heads(o):
    lane = lax.broadcasted_iota(jnp.int32, (WROW, QUAD), 1) // HD
    acc = o[:WROW]
    for h in range(1, GROUP):
        acc = jnp.where(lane == h, o[h * WROW : (h + 1) * WROW], acc)
    return acc


def staged(stages, count, lag, at):
    for t in range(count + lag * (len(stages) - 1)):
        if t > 0 and t % SPAN == 0 and t // SPAN <= 2:
            at("attend", 2 + t // SPAN)
        for n, stage in enumerate(stages):
            if 0 <= t - lag * n < count:
                stage(t - lag * n)


def softmax_cols(s):
    e = jnp.exp2((s - jnp.max(s, 0, keepdims=True)) * (score_scale * log2_e))
    return e * (1.0 / jnp.sum(e, 0, keepdims=True))


def group_cols(g):
    base = (g // 2) * QKV + (g % 2) * QUAD
    return [slice(base + t * HALF, base + t * HALF + QUAD) for t in range(3)]


def attend_forward(x, wa, bias_ref, layer, vec_ref, nv_ref, perm, perm_t, hm_ref, qkv_ref, mixed_ref,
                   nperm, mixw, sc, prc, at):
    hat, _ = norm_stats(x)
    normed = hat * nv_ref[0:1, :] + nv_ref[1:2, :]
    to_window_rows(perm, normed, nperm)
    for m in range(2):
        r = dot(nperm[...], flat(wa[m, ..., :QKV]))
        base = m * QKV
        qkv_ref[:, base : base + HALF] = (r[:, :HALF] + vec_ref[m, layer, 1:2, :HALF]).astype(bf16)
        qkv_ref[:, base + HALF : base + 2 * HALF] = r[:, HALF : 2 * HALF].astype(bf16)
        qkv_ref[:, base + 2 * HALF : base + QKV] = (r[:, 2 * HALF :] + vec_ref[m, layer, 2:3, :HALF]).astype(bf16)
    at("attend", 1)
    units = [(w, g) for w in range(4 * PAIR) for g in range(GROUPS)]

    def scores(t):
        w, g = units[t]
        r = slice(w * WROW, (w + 1) * WROW)
        cq, ck, _ = group_cols(g)
        sc[t % SLOTS] = dot(qkv_ref[r, ck], expand_heads(qkv_ref[r, cq], hm_ref), 1, 1) + bias_ref[g // 2, layer * (1 + w % 4), g % 2]

    def middle(t):
        prc[t % SLOTS] = softmax_cols(sc[t % SLOTS]).astype(bf16)

    def mix(t):
        w, g = units[t]
        r = slice(w * WROW, (w + 1) * WROW)
        o = dot(prc[t % SLOTS], qkv_ref[r, group_cols(g)[2]], 0, 0)
        mixw[r, g * QUAD : (g + 1) * QUAD] = fold_heads(o).astype(bf16)

    staged((scores, middle, mix), len(units), LAG, at)
    mixed = to_token_rows(perm_t, mixw)
    mixed_ref[...] = mixed
    attn = dot(mixed[:, :HALF], flat(wa[0, ..., QKV:]), 1, 1) + dot(mixed[:, HALF:], flat(wa[1, ..., QKV:]), 1, 1)
    return x + attn + nv_ref[4:5, :]


CH = 1024
SLOTS = 6
LAG = 2
SPAN = 12


def mlp_forward(mid, wm, vec_ref, layer, nv_ref, act_ref, slope_ref, at):
    hat, _ = norm_stats(mid)
    hid = (hat * nv_ref[2:3, :] + nv_ref[3:4, :]).astype(bf16)
    total = jnp.zeros((ROWS, D), f32)
    for m in range(2):
        for c in range(0, FFH, CH):
            col = m * FFH + c
            u = dot(hid, flat(wm[m, ..., c : c + CH])) + vec_ref[m, layer, 0:1, c : c + CH]
            t = u * root_half
            phi = 0.5 + 0.5 * lax.erf(t)
            act = (u * phi).astype(bf16)
            act_ref[:, col : col + CH] = act
            slope_ref[:, col : col + CH] = (phi + u * (jnp.exp2(t * t * -log2_e) * inv_root_two_pi)).astype(bf16)
            if col > 0:
                for point in range(col // CH, 4 if col + CH == 2 * FFH else col // CH + 1):
                    at("mlp", point)
            total += dot(act, flat(wm[m, ..., FFH + c : FFH + c + CH]), 1, 1)
    return mid + total + nv_ref[5:6, :]


def mlp_backward(g_s, mid, wm, nv_ref, gp, hid_s, gb_s, rows, b1_acc, nv_acc, at):
    gout = g_s[rows, :]
    hat, inv = norm_stats(mid)
    hid_s[rows, :] = (hat * nv_ref[2:3, :] + nv_ref[3:4, :]).astype(bf16)
    gb = gout.astype(bf16)
    gb_s[rows, :] = gb
    ghid = jnp.zeros((ROWS, D), f32)
    for m in range(2):
        for c in range(0, FFH, CH):
            col = m * FFH + c
            g = dot(gb, flat(wm[m, ..., FFH + c : FFH + c + CH])) * gp[rows, col : col + CH].astype(f32)
            b1_acc[:, col : col + CH] += row_sum(g)
            g = g.astype(bf16)
            gp[rows, col : col + CH] = g
            if col > 0:
                for point in range(col // CH, 4 if col + CH == 2 * FFH else col // CH + 1):
                    at("mlp", point)
            ghid += dot(g, flat(wm[m, ..., c : c + CH]), 1, 1)
    gmid = gout + norm_back(ghid, hat, inv, nv_ref[2:3, :])
    nv_acc[2:3, :] += row_sum(ghid * hat)
    nv_acc[3:4, :] += row_sum(ghid)
    nv_acc[4:5, :] += row_sum(gmid)
    nv_acc[5:6, :] += row_sum(gout)
    g_s[rows, :] = gmid


def attend_backward(g_s, x, wa, bias_ref, layer, nv_ref, perm, perm_t, hm_ref, qkv_ref,
                    mperm, gmw, gqw, gq_s, mb_s, nb_s, rows, ds_acc, qv_acc, nv_acc, sc, dpc, prc, dsc, at):
    gmid = g_s[rows, :]
    hat, inv = norm_stats(x)
    nb_s[rows, :] = (hat * nv_ref[0:1, :] + nv_ref[1:2, :]).astype(bf16)
    mb_s[rows, :] = gmid.astype(bf16)
    to_window_rows(perm, gmid, mperm)
    for m in range(2):
        gmw[:, m * HALF : (m + 1) * HALF] = dot(mperm[...], flat(wa[m, ..., QKV:])).astype(bf16)
    at("attend", 1)
    units = [(w, g) for w in range(4 * PAIR) for g in range(GROUPS)]

    def scores(t):
        w, g = units[t]
        r = slice(w * WROW, (w + 1) * WROW)
        cq, ck, cv = group_cols(g)
        sc[t % SLOTS] = dot(qkv_ref[r, ck], expand_heads(qkv_ref[r, cq], hm_ref), 1, 1) + bias_ref[g // 2, layer * (1 + w % 4), g % 2]
        dpc[t % SLOTS] = dot(qkv_ref[r, cv], expand_heads(gmw[r, g * QUAD : (g + 1) * QUAD], hm_ref), 1, 1)

    def middle(t):
        g = units[t][1]
        pr = softmax_cols(sc[t % SLOTS])
        prc[t % SLOTS] = pr.astype(bf16)
        dp = dpc[t % SLOTS]
        ds = pr * (dp - jnp.sum(pr * dp, 0, keepdims=True))
        ds_acc[g] += ds
        dsc[t % SLOTS] = ds.astype(bf16)

    def grads(t):
        w, g = units[t]
        r = slice(w * WROW, (w + 1) * WROW)
        cq, ck, cv = group_cols(g)
        own = slice(g * QUAD, (g + 1) * QUAD)
        gv = dot(prc[t % SLOTS], expand_heads(gmw[r, own], hm_ref))
        gk = dot(dsc[t % SLOTS], expand_heads(qkv_ref[r, cq], hm_ref)) * score_scale
        gq = fold_heads(dot(dsc[t % SLOTS], qkv_ref[r, ck], 0, 0)) * score_scale
        qv_acc[0:1, own] += row_sum(gq)
        qv_acc[1:2, own] += row_sum(gv)
        gqw[r, cq] = gq.astype(bf16)
        gqw[r, ck] = gk.astype(bf16)
        gqw[r, cv] = gv.astype(bf16)

    staged((scores, middle, grads), len(units), LAG, at)
    at("attend", 2)
    gq = to_token_rows(perm_t, gqw)
    gq_s[rows, :] = gq
    gnorm = dot(gq[:, :QKV], flat(wa[0, ..., :QKV]), 1, 1) + dot(gq[:, QKV:], flat(wa[1, ..., :QKV]), 1, 1)
    nv_acc[0:1, :] += row_sum(gnorm * hat)
    nv_acc[1:2, :] += row_sum(gnorm)
    g_s[rows, :] = g_s[rows, :] + norm_back(gnorm, hat, inv, nv_ref[0:1, :])


def forward_kernel(fast, steps, tok_ref, *refs):
    shards, refs = refs[: 4 if fast else 2], refs[4 if fast else 2 :]
    (bias_in, vec_in, nv_ref, perm_ref, perm_t_ref, hm_ref,
     out_ref, ys_ref, mid_ref, qkv_ref, mixed_ref, act_ref, slope_ref, wa_out, wm_out, bias_out,
     xs, mids, wa, wm, nperm, mixw, sc, prc, bias_ref, vec_ref, local, *sems) = refs
    s = pl.program_id(0)
    per = 2 * steps
    layer, r = s // per, lax.rem(s, per)
    pair = lax.rem(r, steps)
    rows = pl.ds(pl.multiple_of(pair * ROWS, ROWS), ROWS)
    weights = (wa, wm)
    me = lax.axis_index("mp")
    if fast:
        send, recv, own_a, own_m, ssend, srecv = sems
        own = (own_a, own_m)
        swaps = [
            remote(here, there.at[me], ssend.at[n], srecv.at[n], Place().core())
            for n, (here, there) in enumerate(((bias_in, bias_ref), (vec_in, vec_ref)))
        ]
        gathers = [
            Gather(own[n % 2].at[n // 2], weights[n % 2].at[n // 2], send.at[n], recv.at[n], local.at[n])
            for n in range(2 * LAYERS)
        ]

    def keep(n):
        return pltpu.make_async_copy(weights[n % 2].at[n // 2], (wa_out, wm_out)[n % 2].at[n // 2], local.at[4 + n])

    def at(step, point):
        if not fast:
            return
        for key, todo in FORWARD_PLAN.items():
            if key[1] == point and (key[0] % per < steps) == (step == "attend"):

                @pl.when(s == key[0])
                def _():
                    for n, stage in todo:
                        gathers[n].stage(stage)
                        if stage == Gather.STAGES - 1:
                            keep(n).start()

    keep_bias = pltpu.make_async_copy(bias_ref, bias_out, local.at[8])

    @pl.when(s == 0)
    def _():
        if fast:
            pack_shards(shards, own_a, own_m)
            neighbour_barrier(Place())
            for swap in swaps:
                swap.start()
        else:
            for n in range(2 * LAYERS):
                cp = pltpu.make_async_copy(shards[n % 2].at[n // 2], weights[n % 2].at[n // 2], local.at[n])
                cp.start()
                cp.wait()
            for here, there in ((bias_in, bias_ref), (vec_in, vec_ref)):
                there[...] = here[...]

    at("attend", 0)

    @pl.when(s == 0)
    def _():
        if fast:
            for here, there in ((bias_in, bias_ref), (vec_in, vec_ref)):
                there[me] = here[...]
            for swap in swaps:
                swap.wait()
        keep_bias.start()

    @pl.when(r < steps)
    def _():
        @pl.when(s < steps)
        def _():
            put_images(xs, rows, tok_ref)

        mid = attend_forward(xs[rows, :], wa.at[layer], bias_ref, layer, vec_ref, nv_ref.at[layer],
                             perm_ref[layer], perm_t_ref[layer], hm_ref, qkv_ref, mixed_ref, nperm, mixw, sc, prc, at)
        mid_ref[...] = mid
        mids[rows, :] = mid
        at("attend", 2)

    @pl.when(r >= steps)
    def _():
        at("mlp", 0)
        y = mlp_forward(mids[rows, :], wm.at[layer], vec_ref, layer, nv_ref.at[layer], act_ref, slope_ref, at)

        @pl.when(layer < LAYERS - 1)
        def _():
            xs[rows, :] = y
            ys_ref[...] = y

        @pl.when(layer == LAYERS - 1)
        def _():
            for im in range(PAIR):
                part = y[im * SEQP : im * SEQP + SEQ]
                out_ref[im] = part

    @pl.when(s == LAYERS * per - 1)
    def _():
        keep_bias.wait()
        if fast:
            for n in range(2 * LAYERS):
                keep(n).wait()


def pack_shards(shards, own_a, own_m):
    w_qkv, w_proj, w_one, w_two = shards
    for l in range(LAYERS):
        for k in range(3):
            own_a[l, :, k * HALF : (k + 1) * HALF] = w_qkv[l, k].astype(bf16)
        own_a[l, :, QKV:] = w_proj[l].astype(bf16)
        own_m[l, :, :FFH] = w_one[l].astype(bf16)
        own_m[l, :, FFH:] = w_two[l].astype(bf16)


FORWARD_PLAN = {(0, 0): [(0, 0), (1, 0), (0, 1), (0, 2), (0, 3), (1, 1), (0, 4), (1, 2), (1, 3), (0, 5), (0, 6), (2, 0)], (1, 1): [(1, 4), (3, 0)], (2, 1): [(1, 5), (2, 1)], (2, 2): [(2, 2), (2, 3)], (3, 0): [(1, 6)], (3, 2): [(2, 4), (3, 1)], (4, 0): [(3, 2)], (4, 2): [(2, 5), (3, 3)], (5, 2): [(2, 6)], (6, 1): [(3, 4)], (7, 4): [(3, 5)], (9, 0): [(3, 6)]}


def backward_kernel(fast, steps, cot_ref, tok_ref, ys_ref, mid_ref, qkv_ref, act_in, slope_in, mixed_in, wa_in, wm_in,
                    bias_ref, nv_ref, perm_ref, perm_t_ref, hm_ref, count_ref, *refs):
    if fast:
        gx_ref, ga_out, sum_m, sum_a, *refs = refs
    else:
        gx_ref, ga_out, gm_out, *refs = refs
    (qv_all, b1_all, ds_all, nv_all, g_s, xs, mperm, gmw, gqw, gp, gq_s, hid_s, gb_s, mb_s, nb_s, act_s, mixed_s,
     wa, wm, gwm, gwa, sc, dpc, prc, dsc, local, *comm) = refs
    s = pl.program_id(0)
    per = 2 * steps + 6
    turn, r = s // per, lax.rem(s, per)
    layer = LAYERS - 1 - turn
    first_g, first_a, last_g = steps, steps + 4, 2 * steps + 4
    pair = jnp.where(r < first_a, jnp.minimum(r, steps - 1), jnp.minimum(r - first_a, steps - 1))
    rows = pl.ds(pl.multiple_of(pair * ROWS, ROWS), ROWS)
    total = steps * ROWS
    qv_acc, b1_acc, ds_acc, nv_acc, nv_ref = (
        ref.at[layer] for ref in (qv_all, b1_all, ds_all, nv_all, nv_ref)
    )
    me = lax.axis_index("mp")
    if fast:
        scatters = [
            Scatter(gw.at[0], gw.at[1], *comm[8 * n : 8 * n + 8]) for n, gw in enumerate((gwm.at[0], gwm.at[1], gwa))
        ]
        pl.when(s == 0)(lambda: neighbour_barrier(Place()))

    def at(step, point):
        if not fast:
            return
        spans = {"mlp": (0, first_g), "g": (first_g, first_a), "attend": (first_a, last_g), "ga": (last_g, per)}
        for key, todo in BACKWARD_PLAN.items():
            lo, hi = spans[step]
            if key[1] == point and lo <= key[0] % per < hi:

                @pl.when(s == key[0])
                def _():
                    for n, stage in todo:
                        if stage == Scatter.STAGES - 1:
                            last = key[0] < per + first_a
                            scatters[n].result(sum_a.at[0] if n == 2 else sum_m.at[n, LAYERS - 1 if last else 0])
                        scatters[n].stage(stage)

    def rows_of(l):
        return pl.ds(l * total, total)

    def load(name, l):
        src, dst, n = {
            "wm": (wm_in.at[l], wm, 0), "wa": (wa_in.at[l], wa, 1), "act": (act_in.at[rows_of(l)], act_s, 2),
            "mixed": (mixed_in.at[rows_of(l)], mixed_s, 3), "slope": (slope_in.at[rows_of(l)], gp, 4),
        }[name]
        return pltpu.make_async_copy(src, dst, local.at[n])

    top = LAYERS - 1

    @pl.when(s == 0)
    def _():
        for name in ("wm", "slope", "wa", "act", "mixed"):
            load(name, top).start()

    for l in range(top, -1, -1):
        base = (top - l) * per
        for name, step in (("wm", 0), ("slope", 0), ("act", first_g), ("wa", first_a), ("mixed", last_g)):
            pl.when(s == base + step)(lambda name=name, l=l: load(name, l).wait())
        if l > 0:
            for name, step in (("wm", first_g), ("slope", first_a), ("act", first_a), ("wa", last_g), ("mixed", per)):
                pl.when(s == base + step)(lambda name=name, l=l: load(name, l - 1).start())

    @pl.when(r == 0)
    def _():
        for ref in (qv_acc, b1_acc, ds_acc, nv_acc):
            ref[...] = jnp.zeros(ref.shape, f32)

    @pl.when(r < first_g)
    def _():
        at("mlp", 0)

        @pl.when(turn == 0)
        def _():
            image = (me * steps + pair) * PAIR
            put_images(g_s, rows, cot_ref, lambda im, v: v * (image + im < count_ref[0]).astype(f32))

        mlp_backward(g_s, mid_ref[...], wm, nv_ref, gp, hid_s, gb_s, rows, b1_acc, nv_acc, at)

    def gradient(left, right, lo, width):
        cols = pl.ds(pl.multiple_of(lo, width), width)
        return dot(left[...], right[:, cols], 0, 0).astype(bf16).reshape(*gwa.shape[1:-1], width)

    @pl.when((r >= first_g) & (r < first_a))
    def _():
        at("g", 0)
        q = r - first_g
        own = lax.rem(q, 2)
        half = jnp.where(own == 1, me, 1 - me)

        @pl.when(q < 2)
        def _():
            gwm[0, own] = gradient(hid_s, gp, half * FFH, FFH)

        @pl.when(q >= 2)
        def _():
            gwm[1, own] = gradient(gb_s, act_s, half * FFH, FFH)

        at("g", 1)

    @pl.when((r >= first_a) & (r < last_g))
    def _():
        at("attend", 0)

        @pl.when(layer == 0)
        def _():
            put_images(xs, slice(None), tok_ref)

        @pl.when(layer > 0)
        def _():
            xs[...] = ys_ref[...]

        attend_backward(g_s, xs[...], wa, bias_ref, layer, nv_ref, perm_ref[layer], perm_t_ref[layer], hm_ref,
                        qkv_ref, mperm, gmw, gqw, gq_s, mb_s, nb_s, rows, ds_acc, qv_acc, nv_acc, sc, dpc, prc, dsc, at)

        @pl.when(layer == 0)
        def _():
            for im in range(PAIR):
                part = g_s.at[rows, :][im * SEQP : im * SEQP + SEQ]
                gx_ref[im] = part

    @pl.when(r >= last_g)
    def _():
        at("ga", 0)
        own = r - last_g
        half = jnp.where(own == 1, me, 1 - me)
        gwa[own, ..., :QKV] = gradient(nb_s, gq_s, half * QKV, QKV)
        gwa[own, ..., QKV:] = gradient(mb_s, mixed_s, half * HALF, HALF)
        at("ga", 1)

    def flush(src, dst):
        cp = pltpu.make_async_copy(src, dst, local.at[5])
        cp.start()
        cp.wait()

    if fast:
        pl.when(s == LAYERS * per - 1)(lambda: flush(gwa, ga_out))
    else:
        pl.when(r == first_a)(lambda: flush(gwm, gm_out.at[layer]))
        pl.when(r == per - 1)(lambda: flush(gwa, ga_out.at[layer]))


BACKWARD_PLAN = {(4, 0): [(0, 0)], (5, 1): [(0, 1)], (6, 0): [(1, 0)], (7, 1): [(1, 1)], (7, 2): [(0, 2)], (8, 4): [(0, 3)], (8, 2): [(1, 2)], (9, 2): [(1, 3)], (10, 1): [(0, 4)], (11, 0): [(2, 0)], (12, 1): [(2, 1)], (13, 1): [(1, 4)], (14, 0): [(2, 2)], (15, 0): [(2, 3)], (16, 0): [(0, 0)], (17, 0): [(2, 4)], (17, 1): [(0, 1)], (18, 0): [(1, 0)], (19, 1): [(1, 1)], (19, 2): [(0, 2)], (20, 4): [(0, 3)], (20, 2): [(1, 2)], (21, 2): [(1, 3)], (22, 1): [(0, 4)], (23, 1): [(1, 4)]}


def whole(shape, buffers=1):
    zero = (0,) * len(shape)
    return pl.BlockSpec(shape, lambda i: zero, pipeline_mode=pl.Buffered(buffers))


VLIM = 67000000


def forward(tok, shards, bias, vecs, nv, perm, perm_t, hm, fast, steps):
    per = 2 * steps
    rows = steps * ROWS
    slots = (2, NZ, NY, NX, D // PEERS) if fast else (2, 1, 1, 1, D)
    wide = (COLS - ATT, ATT)
    any_ = pl.BlockSpec(memory_space=pl.ANY)

    def attend(s):
        return s // per * steps + jnp.minimum(lax.rem(s, per), steps - 1)

    def mlp(s):
        return s // per * steps + jnp.maximum(lax.rem(s, per) - steps, 0)

    sems = []
    if fast:
        sems = [pltpu.SemaphoreType.DMA((2 * LAYERS, Gather.SEMS))] * 2
        sems += [pltpu.VMEM((LAYERS, D // PEERS, n), bf16) for n in wide] + [pltpu.SemaphoreType.DMA((2,))] * 2
    halves = [(2, *a.shape) if fast else a.shape for a in (bias, vecs)]
    params = dict(collective_id=1, has_side_effects=True) if fast else {}
    return pl.pallas_call(
        functools.partial(forward_kernel, fast, steps),
        name="forward",
        grid=(LAYERS * per,),
        in_specs=[
            pl.BlockSpec((PAIR, SEQ, D), lambda s: (lax.axis_index("mp") * steps + jnp.minimum(s, steps - 1), 0, 0)),
            *(whole(w.shape) if fast else any_ for w in shards),
            *(whole(a.shape) for a in (bias, vecs, nv, perm, perm_t, hm)),
        ],
        out_specs=[
            pl.BlockSpec((PAIR, SEQ, D), lambda s: (jnp.maximum(s - (LAYERS * per - steps), 0), 0, 0)),
            pl.BlockSpec((ROWS, D), lambda s: (jnp.clip(s - steps, 0, steps - 1), 0)),
            pl.BlockSpec((ROWS, D), lambda s: (attend(s), 0)),
            pl.BlockSpec((WPAIR, 2 * QKV), lambda s: (attend(s), 0)),
            pl.BlockSpec((ROWS, D), lambda s: (attend(s), 0)),
            pl.BlockSpec((ROWS, 2 * FFH), lambda s: (mlp(s), 0)),
            pl.BlockSpec((ROWS, 2 * FFH), lambda s: (mlp(s), 0)),
            any_, any_, any_,
        ],
        out_shape=[
            jax.ShapeDtypeStruct((steps * PAIR, SEQ, D), f32),
            jax.ShapeDtypeStruct((rows, D), f32),
            jax.ShapeDtypeStruct((LAYERS * rows, D), f32),
            jax.ShapeDtypeStruct((LAYERS * steps * WPAIR, 2 * QKV), bf16),
            jax.ShapeDtypeStruct((LAYERS * rows, D), bf16),
            jax.ShapeDtypeStruct((LAYERS * rows, 2 * FFH), bf16),
            jax.ShapeDtypeStruct((LAYERS * rows, 2 * FFH), bf16),
            *(jax.ShapeDtypeStruct((LAYERS, *slots, n), bf16) for n in wide),
            jax.ShapeDtypeStruct(halves[0], f32),
        ],
        scratch_shapes=[
            pltpu.VMEM((rows, D), f32), pltpu.VMEM((rows, D), f32),
            *(pltpu.VMEM((LAYERS, *slots, n), bf16) for n in wide),
            pltpu.VMEM((WPAIR, D), bf16), pltpu.VMEM((WPAIR, D), bf16),
            pltpu.VMEM((SLOTS, WROW, LANES), f32), pltpu.VMEM((SLOTS, WROW, LANES), bf16),
            *(pltpu.VMEM(n, f32) for n in halves),
            pltpu.SemaphoreType.DMA((9,)), *sems,
        ],
        compiler_params=pltpu.CompilerParams(vmem_limit_bytes=VLIM, **params),
    )(tok, *shards, bias, vecs, nv, perm, perm_t, hm)


def backward(cot, tok, saved, weights, bias, nv, perm, perm_t, hm, count, fast, steps):
    ys, mid, qkv, mixed, act, slope = saved
    wa, wm = weights
    per = 2 * steps + 6
    rows = steps * ROWS
    slots = wa.shape[1:-1]
    rest = slots[1:]
    any_ = pl.BlockSpec(memory_space=pl.ANY)

    def clip(v):
        return jnp.clip(v, 0, steps - 1)

    def layer(s):
        return LAYERS - 1 - s // per

    attend0 = (LAYERS - 1) * per + steps + 4
    img = lambda at: pl.BlockSpec((PAIR, SEQ, D), lambda s: (clip(s - at), 0, 0))
    mine = lambda at: pl.BlockSpec((PAIR, SEQ, D), lambda s: (lax.axis_index("mp") * steps + clip(s - at), 0, 0))
    wide = (COLS - ATT, ATT)
    part = rest[-1]
    if fast:
        outs = [
            jax.ShapeDtypeStruct((2, *rest, COLS - ATT), bf16),
            jax.ShapeDtypeStruct((2, LAYERS, part, FFH), f32), jax.ShapeDtypeStruct((1, part, COLS - ATT), f32),
        ]
        specs = [any_, whole(outs[1].shape), whole(outs[2].shape)]
        comm = Scatter.landing(part, FFH) * 2 + Scatter.landing(part, COLS - ATT)
        params = dict(collective_id=2, has_side_effects=True)
    else:
        outs = [
            jax.ShapeDtypeStruct((LAYERS, 2, *rest, COLS - ATT), bf16),
            jax.ShapeDtypeStruct((LAYERS, 2, 2, *rest, FFH), bf16),
        ]
        specs, comm, params = [any_, any_], [], {}
    small = [(LAYERS, 2, 2 * HALF), (LAYERS, 1, 2 * FFH), (LAYERS, GROUPS, WROW, LANES), (LAYERS, 8, D)]
    return pl.pallas_call(
        functools.partial(backward_kernel, fast, steps),
        name="backward",
        grid=(LAYERS * per,),
        in_specs=[
            mine(0), mine(attend0),
            pl.BlockSpec((ROWS, D), lambda s: (clip(s - steps - 4), 0)),
            pl.BlockSpec((ROWS, D), lambda s: (layer(s) * steps + clip(lax.rem(s, per)), 0)),
            pl.BlockSpec((WPAIR, 2 * QKV), lambda s: (layer(s) * steps + clip(lax.rem(s, per) - steps - 4), 0)),
            any_, any_, any_, any_, any_,
            *(whole(a.shape) for a in (bias, nv, perm, perm_t, hm)),
            pl.BlockSpec(memory_space=pltpu.SMEM),
        ],
        out_specs=[img(attend0), *specs, *(whole(n) for n in small)],
        out_shape=[
            jax.ShapeDtypeStruct((steps * PAIR, SEQ, D), f32), *outs, *(jax.ShapeDtypeStruct(n, f32) for n in small),
        ],
        scratch_shapes=[
            pltpu.VMEM((rows, D), f32), pltpu.VMEM((ROWS, D), f32),
            pltpu.VMEM((WPAIR, D), bf16), pltpu.VMEM((WPAIR, D), bf16), pltpu.VMEM((WPAIR, 2 * QKV), bf16),
            pltpu.VMEM((rows, 2 * FFH), bf16), pltpu.VMEM((rows, 2 * QKV), bf16),
            *[pltpu.VMEM((rows, D), bf16)] * 4,
            pltpu.VMEM((rows, 2 * FFH), bf16), pltpu.VMEM((rows, D), bf16),
            *(pltpu.VMEM((*slots, n), bf16) for n in wide),
            pltpu.VMEM((2, 2, *rest, FFH), bf16), pltpu.VMEM((2, *rest, COLS - ATT), bf16),
            *[pltpu.VMEM((SLOTS, WROW, LANES), f32)] * 2, *[pltpu.VMEM((SLOTS, WROW, LANES), bf16)] * 2,
            pltpu.SemaphoreType.DMA((8,)), *comm,
        ],
        compiler_params=pltpu.CompilerParams(vmem_limit_bytes=VLIM, **params),
    )(cot, tok, ys, mid, qkv, act, slope, mixed, wa, wm, bias, nv, perm, perm_t, hm, count)


def head_mask():
    return (np.arange(QUAD)[None, :] // HD == np.arange(GROUP)[:, None]).astype(np.float32)


def exact_parts(a):
    parts = []
    for _ in range(3):
        top = lax.reduce_precision(a, 8, 7)
        parts.append(top.astype(bf16))
        a = a - top
    return jnp.stack(parts)


def bias_cols(onehot, table):
    picked = jnp.einsum("jti,smlth->sjmlhi", onehot.astype(bf16), exact_parts(table), preferred_element_type=f32)
    picked = (picked[0] + picked[1] + picked[2]).transpose(1, 2, 0, 3, 4)
    picked = picked.reshape(-1, LAYERS, WROW, 2, GROUP, WROW).transpose(0, 1, 3, 2, 4, 5)
    apart = np.concatenate([np.zeros((1, WROW, WROW), np.float32), region_mask()])
    apart[:, WSEQ:] = pad_fill
    both = jnp.concatenate([picked[:, :1]] + [picked[:, 1:]] * 4, 1)
    both = (both + jnp.asarray(apart)[:, None, :, None, :]) * (1.0 / score_scale)
    return both.reshape(-1, 5, 2, WROW, LANES)

NZ, NY, NX = 4, 2, 2
PEERS = NZ * NY * NX
MESH_ID = pl.DeviceIdType.MESH


class Place:
    def __init__(self):
        d = lax.axis_index("dp")
        self.d, self.m = d, lax.axis_index("mp")
        self.z, self.y, self.x = d // 4, lax.rem(d // 2, 2), lax.rem(d, 2)

    def chip(self, z, y, x):
        return (z * NY + y) * NX + x

    def at(self, y=None, x=None, m=None):
        y = self.y if y is None else y
        x = self.x if x is None else x
        return (self.chip(self.z, y, x), self.m if m is None else m)

    def xn(self):
        return self.at(x=1 - self.x)

    def yn(self):
        return self.at(y=1 - self.y)

    def core(self):
        return self.at(m=1 - self.m)

    def column(self, z):
        return (self.chip(z, self.y, self.x), self.m)


def remote(src, dst, send, recv, to):
    return pltpu.make_async_remote_copy(
        src_ref=src, dst_ref=dst, send_sem=send, recv_sem=recv, device_id=to, device_id_type=MESH_ID
    )


def neighbour_barrier(p):
    sem = pltpu.get_barrier_semaphore()
    partners = [p.xn(), p.yn(), p.core()] + [p.column(lax.rem(p.z + n, NZ)) for n in range(1, NZ)]
    for to in partners:
        pl.semaphore_signal(sem, inc=1, device_id=to, device_id_type=MESH_ID)
    pl.semaphore_wait(sem, len(partners))


def each_plane(body):
    lax.fori_loop(0, NZ, lambda k, carry: (body(k), carry)[1], 0)


class Gather:
    SEMS = 48
    BASE = {"z": 0, "xa": 4, "yb": 8, "ya0": 12, "ya1": 16, "xb0": 20, "xb1": 24,
            "own": 28, "ax": 32, "by": 36, "ar": 40, "br": 44}

    def __init__(self, own, full, send, recv, local):
        self.p, self.own, self.full = Place(), own, full
        self.send, self.recv, self.local = send, recv, local
        half = full.shape[-1] // 2
        self.all, self.a, self.b = pl.ds(0, 2 * half), pl.ds(0, half), pl.ds(half, half)

    def region(self, kind, k, arrived):
        p = self.p
        oy, ox = 1 - p.y, 1 - p.x
        if kind == "z":
            return (p.m, k if arrived else p.z, p.y, p.x), self.all, p.column(k)
        if kind == "xa":
            return (p.m, k, p.y, ox if arrived else p.x), self.a, p.xn()
        if kind == "yb":
            return (p.m, k, oy if arrived else p.y, p.x), self.b, p.yn()
        if kind in ("ya0", "ya1"):
            return (p.m, k, oy if arrived else p.y, p.x if kind == "ya0" else ox), self.a, p.yn()
        if kind in ("xb0", "xb1"):
            return (p.m, k, p.y if kind == "xb0" else oy, ox if arrived else p.x), self.b, p.xn()
        m = 1 - p.m if arrived else p.m
        if kind == "own":
            return (m, k, p.y, p.x), self.all, p.core()
        if kind == "ax":
            return (m, k, p.y, ox), self.a, p.core()
        if kind == "by":
            return (m, k, oy, p.x), self.b, p.core()
        if kind == "ar":
            return (m, k, oy, slice(None)), self.a, p.core()
        return (m, k, slice(None), ox), self.b, p.core()

    def copy(self, kind, k, own=False, arrived=False):
        at, cols, to = self.region(kind, k, arrived)
        dst = self.full.at[(*at, slice(None), cols)]
        src = self.own.at[:, cols] if own else dst
        s = self.BASE[kind] + k
        r = self.p.z if kind == "z" and not arrived else s
        return remote(src, dst, self.send.at[s], self.recv.at[r], to)

    def keep(self):
        p = self.p
        return pltpu.make_async_copy(
            self.own.at[:, self.all], self.full.at[p.m, p.z, p.y, p.x, :, self.all], self.local
        )

    def fan(self, k, own=False):
        for kind in ("xa", "yb", "ya0", "xb0", "own"):
            self.copy(kind, k, own).start()

    def stage(self, n):
        p = self.p
        if n == 0:
            self.keep().start()
            for dist in (1, 2, 3):
                for k in (p.z + dist, p.z - dist):
                    pl.when((k >= 0) & (k < NZ))(lambda k=k: self.copy("z", k, True).start())
            self.fan(p.z, True)
        elif n <= 3:
            for k in (p.z + n, p.z - n):

                @pl.when((k >= 0) & (k < NZ))
                def _():
                    self.copy("z", k, arrived=True).wait_recv()
                    self.fan(k)
        elif n == 4:

            @each_plane
            def _(k):
                self.copy("xa", k, arrived=True).wait_recv()
                for kind in ("ya1", "ax"):
                    self.copy(kind, k).start()
                self.copy("yb", k, arrived=True).wait_recv()
                for kind in ("xb1", "by"):
                    self.copy(kind, k).start()
        elif n == 5:

            @each_plane
            def _(k):
                for kind, rest in (("ya", "ar"), ("xb", "br")):
                    for rel in ("0", "1"):
                        self.copy(kind + rel, k, arrived=True).wait_recv()
                    self.copy(rest, k).start()
        else:

            @each_plane
            def _(k):
                for kind in ("own", "ax", "by", "ar", "br"):
                    self.copy(kind, k, arrived=True).wait_recv()
                for kind in self.BASE:
                    if kind != "z":
                        self.copy(kind, k).wait_send()
                pl.when(k != p.z)(lambda: self.copy("z", k, True).wait_send())

            self.keep().wait()

    STAGES = 7


def add_into(ref, at, other):
    ref[at] = ref[at] + other


class Scatter:
    SEMS = 24
    BASE = {"core": 0, "ya": 4, "xb": 8, "xa": 12, "yb": 16, "z": 20}

    @staticmethod
    def landing(rows, cols):
        half = cols // 2
        return [
            pltpu.VMEM((NZ, NY, NX, rows, cols), bf16),
            pltpu.VMEM((NZ, NX, rows, half), bf16), pltpu.VMEM((NZ, NY, rows, half), bf16),
            pltpu.VMEM((NZ, rows, half), bf16), pltpu.VMEM((NZ, rows, half), bf16),
            pltpu.VMEM((NZ, rows, cols), bf16),
            pltpu.SemaphoreType.DMA((Scatter.SEMS,)), pltpu.SemaphoreType.DMA((Scatter.SEMS,)),
        ]

    def __init__(self, give, part, other, ya, xb, xa, yb, z, send, recv):
        self.p, self.give, self.part, self.other = Place(), give, part, other
        self.land = {"ya": ya, "xb": xb, "xa": xa, "yb": yb, "z": z}
        self.send, self.recv = send, recv
        half = part.shape[-1] // 2
        self.a, self.b = pl.ds(0, half), pl.ds(half, half)

    def copy(self, kind, k):
        p = self.p
        oy, ox = 1 - p.y, 1 - p.x
        full = slice(None)
        if kind == "core":
            src, dst, to = self.give.at[k], self.other.at[k], p.core()
        else:
            at, to = {
                "ya": ((k, oy, full, full, self.a), p.yn()),
                "xb": ((k, full, ox, full, self.b), p.xn()),
                "xa": ((k, p.y, ox, full, self.a), p.xn()),
                "yb": ((k, oy, p.x, full, self.b), p.yn()),
                "z": ((k, p.y, p.x, full, full), p.column(k)),
            }[kind]
            src, dst = self.part.at[at], self.land[kind].at[p.z if kind == "z" else k]
        s = self.BASE[kind] + k
        r = self.BASE[kind] + p.z if kind == "z" else s
        return remote(src, dst, self.send.at[s], self.recv.at[r], to)

    def landed(self, k):
        s = self.BASE["z"] + k
        at = self.land["z"].at[k]
        return remote(at, at, self.send.at[s], self.recv.at[s], self.p.column(k))

    def stage(self, n):
        p = self.p
        oy, ox = 1 - p.y, 1 - p.x
        if n == 0:
            each_plane(lambda k: self.copy("core", k).start())
        elif n == 1:

            @each_plane
            def _(k):
                self.copy("core", k).wait_recv()
                for y in range(NY):
                    for x in range(NX):
                        add_into(self.part, (k, y, x), self.other[k, y, x])
                self.copy("ya", k).start()
                self.copy("xb", k).start()
        elif n == 2:

            @each_plane
            def _(k):
                self.copy("ya", k).wait_recv()
                for x in range(NX):
                    add_into(self.part, (k, p.y, x, slice(None), self.a), self.land["ya"][k, x])
                self.copy("xa", k).start()
                self.copy("xb", k).wait_recv()
                for y in range(NY):
                    add_into(self.part, (k, y, p.x, slice(None), self.b), self.land["xb"][k, y])
                self.copy("yb", k).start()
        elif n == 3:

            @each_plane
            def _(k):
                self.copy("xa", k).wait_recv()
                add_into(self.part, (k, p.y, p.x, slice(None), self.a), self.land["xa"][k])
                self.copy("yb", k).wait_recv()
                add_into(self.part, (k, p.y, p.x, slice(None), self.b), self.land["yb"][k])

            for dist in (3, 2, 1):
                for k in (p.z + dist, p.z - dist):
                    pl.when((k >= 0) & (k < NZ))(lambda k=k: self.copy("z", k).start())
        else:

            @each_plane
            def _(k):
                for kind in ("core", "ya", "xb", "xa", "yb"):
                    self.copy(kind, k).wait_send()
                pl.when(k != p.z)(lambda: self.copy("z", k).wait_send())

    STAGES = 5

    def result(self, out):
        p = self.p
        out[...] = self.part[p.z, p.y, p.x].astype(f32)

        @each_plane
        def _(k):
            @pl.when(k != p.z)
            def _():
                self.landed(k).wait_recv()
                out[...] += self.land["z"][k].astype(f32)


class Total:
    STEPS = 5

    @staticmethod
    def scratch(shape):
        return [
            pltpu.VMEM((Total.STEPS, *shape), f32), pltpu.VMEM((Total.STEPS, *shape), f32),
            pltpu.SemaphoreType.DMA((Total.STEPS,)), pltpu.SemaphoreType.DMA((Total.STEPS,)),
        ]

    def __init__(self, start, held, land, send, recv):
        self.p, self.start, self.held, self.land, self.send, self.recv = Place(), start, held, land, send, recv

    def copy(self, n):
        p = self.p
        pair = p.z + 1 - 2 * lax.rem(p.z, 2)
        far = lax.rem(p.z + 2, NZ)
        to = (p.core(), p.yn(), p.xn(), (p.chip(pair, p.y, p.x), p.m), (p.chip(far, p.y, p.x), p.m))[n]
        src = self.start if n == 0 else self.held.at[n - 1]
        return remote(src, self.land.at[n], self.send.at[n], self.recv.at[n], to)

    def stage(self, n):
        if n > 0:
            self.copy(n - 1).wait_recv()
            before = self.start[...] if n == 1 else self.held[n - 2]
            self.held[n - 1] = before + self.land[n - 1]
        if n < self.STEPS:
            self.copy(n).start()
        else:
            for k in range(self.STEPS):
                self.copy(k).wait_send()


def tail_kernel(grad_ref, small_ref, out_ref, small_out, part, *refs):
    neighbour_barrier(Place())
    total = Total(small_ref, *refs[-4:])
    width = part.shape[-1]
    spans = [pl.ds(n * width, width) for n in range(2)]
    pieces = [
        Scatter(grad_ref.at[0, ..., cols], part.at[n], *refs[8 * n : 8 * n + 8]) for n, cols in enumerate(spans)
    ]
    for s in pieces:
        s.stage(0)
    total.stage(0)
    for n, cols in enumerate(spans):
        part[n] = grad_ref[1, ..., cols]
    for n in range(1, Scatter.STAGES - 1):
        for s in pieces:
            s.stage(n)
        total.stage(n)
    total.stage(Scatter.STAGES - 1)
    for s, cols in zip(pieces, spans):
        s.result(out_ref.at[:, cols])
        s.stage(Scatter.STAGES - 1)
    total.stage(Total.STEPS)
    small_out[...] = total.held[Total.STEPS - 1]


def tail(grad, small):
    rows, cols = grad.shape[-2:]
    half = cols // 2
    vm = pl.BlockSpec(memory_space=pltpu.VMEM)
    return pl.pallas_call(
        tail_kernel,
        name="tail",
        out_shape=[jax.ShapeDtypeStruct((rows, cols), f32), jax.ShapeDtypeStruct(small.shape, f32)],
        in_specs=[vm] * 2,
        out_specs=[vm] * 2,
        scratch_shapes=[pltpu.VMEM((2, *grad.shape[1:-1], half), bf16)] + Scatter.landing(rows, half) * 2
        + Total.scratch(small.shape),
        compiler_params=pltpu.CompilerParams(collective_id=3, has_side_effects=True, vmem_limit_bytes=VLIM),
    )(grad, small)


def adam_update(weight_in, moment_one, moment_two, grad_sum, decay):
    new_one = beta_one * moment_one + (1.0 - beta_one) * grad_sum
    new_two = beta_two * moment_two + (1.0 - beta_two) * grad_sum * grad_sum
    hat_one = new_one / (1.0 - beta_one**adam_step)
    hat_two = new_two / (1.0 - beta_two**adam_step)
    new_weight = weight_in - learn_rate * (hat_one / (jnp.sqrt(hat_two) + adam_eps) + decay * weight_in)
    return (new_weight, new_one, new_two)


def both_halves(mine, me):
    other = lax.ppermute(mine, "mp", [(0, 1), (1, 0)])
    low = jnp.where(me == 0, mine, other)
    high = jnp.where(me == 0, other, mine)
    return jnp.concatenate([low, high], 0)


HEADS = GROUPS * GROUP
LITTLE = 4 * HALF + 2 * FFH + HEADS * TABLE + 6 * D


def lanes_of(a):
    flat = a.reshape(-1)
    return jnp.pad(flat, (0, -flat.size % 1024)).reshape(-1, 128)


def sum_of_all(a):
    a = a.reshape(LAYERS, 2, D, a.shape[-1])
    total = a[:, 1].astype(f32) + lax.ppermute(a[:, 0], "mp", [(0, 1), (1, 0)]).astype(f32)
    return lax.psum_scatter(total.astype(bf16), "dp", scatter_dimension=1, tiled=True).astype(f32)


def pair_onehot(rel_index):
    index = jnp.pad(rel_index.T, ((0, WROW - WSEQ), (0, WROW - WSEQ)), constant_values=-1)
    return (index[:, None, :] == jnp.arange(TABLE, dtype=jnp.int32)[None, :, None]).astype(f32)


def local(
    fast, tokens, cotangent, image_count, rel_index,
    w_qkv, w_proj, w_fc_one, w_fc_two, qv_bias, fc_one_bias, rel_table, norm_vec,
    m_qkv, m_proj, m_fc_one, m_fc_two, m_qv_bias, m_fc_one_bias, m_rel_table, m_norm_vec,
    v_qkv, v_proj, v_fc_one, v_fc_two, v_qv_bias, v_fc_one_bias, v_rel_table, v_norm_vec,
):
    me = lax.axis_index("mp")
    images = tokens.shape[0]
    nimg = images // 2
    steps = nimg // PAIR
    part = w_qkv.shape[1]
    tok, cot = tokens, cotangent
    onehot = pair_onehot(rel_index)
    vecs = jnp.concatenate([fc_one_bias[:, None], jnp.pad(qv_bias, ((0, 0), (0, 5), (0, FFH - HALF)))], 1)
    shards = (w_qkv.transpose(0, 2, 1, 3), w_proj.transpose(0, 2, 1), w_fc_one, w_fc_two.transpose(0, 2, 1))
    if fast:
        bias = bias_cols(onehot, rel_table[None])[0]
    else:
        wm = jnp.concatenate([w_fc_one, w_fc_two.transpose(0, 2, 1)], 2).astype(bf16)
        wa = jnp.concatenate([w_qkv.reshape(LAYERS, part, QKV), w_proj.transpose(0, 2, 1)], 2).astype(bf16)
        shards = [
            lax.all_gather(w, ("mp", "dp")).reshape(2, -1, LAYERS, part, w.shape[-1]).transpose(2, 0, 1, 3, 4)
            .reshape(LAYERS, 2, 1, 1, 1, D, w.shape[-1])
            for w in (wa, wm)
        ]
        vecs = lax.all_gather(vecs, "mp")
        bias = bias_cols(onehot, lax.all_gather(rel_table, "mp"))
    hm = jnp.asarray(head_mask(), bf16)
    perms = np.stack([permutation(layer % 2 == 1) for layer in range(LAYERS)])
    perm, perm_t = jnp.asarray(perms, bf16), jnp.asarray(perms.transpose(0, 2, 1), bf16)
    out, *saved, all_wa, all_wm, bias = forward(
        tok, shards, bias, vecs, norm_vec, perm, perm_t, hm, fast, steps
    )
    weights = (all_wa, all_wm) if fast else shards
    out = both_halves(out, me)
    x_grad, *grads, gqv, gb1, ds, gnv = backward(
        cot, tok, saved, weights, bias, norm_vec, perm, perm_t, hm, image_count, fast, steps
    )
    x_grad = both_halves(x_grad, me)
    ds = ds.reshape(LAYERS, GROUPS, WROW, GROUP, WROW)
    gt = jnp.einsum("lgjhi,jti->lght", ds, onehot, precision=lax.Precision.HIGHEST)
    little = jnp.concatenate([a.reshape(LAYERS, -1) for a in (gqv, gb1, gt, gnv[:, :6])], 1)
    if fast:
        ga, sum_m, sum_a = grads
        last, total = tail(ga, lanes_of(little))
        big_a, big_m = jnp.stack([last, sum_a[0]]), sum_m
        little = total.reshape(-1)[: LAYERS * LITTLE].reshape(LAYERS, LITTLE)
    else:
        ga, gm = grads
        big_a, big_m = sum_of_all(ga), jnp.stack([sum_of_all(gm[:, n]) for n in range(2)])
        little = lax.psum(little, ("dp", "mp"))
    one_grad = big_m[0]
    two_grad = big_m[1].transpose(0, 2, 1)
    qkv_grad = big_a[:, :, :QKV].reshape(LAYERS, part, 3, HALF)
    proj_grad = big_a[:, :, QKV:].transpose(0, 2, 1)
    cut = lambda a: lax.dynamic_index_in_dim(a, me, 1, keepdims=False)
    at = 2 * 2 * HALF
    qv_grad = cut(little[:, :at].reshape(LAYERS, 2, 2, HALF).transpose(0, 2, 1, 3))
    bias_grad = cut(little[:, at : at + 2 * FFH].reshape(LAYERS, 2, FFH))
    at += 2 * FFH
    table_grad = cut(little[:, at : at + HEADS * TABLE].reshape(LAYERS, 2, HEADS // 2, TABLE)).transpose(0, 2, 1)
    at += HEADS * TABLE
    norm_grad = little[:, at:].reshape(LAYERS, 6, D)
    groups = [
        adam_update(w_qkv, m_qkv, v_qkv, qkv_grad, decay_rate),
        adam_update(w_proj, m_proj, v_proj, proj_grad, decay_rate),
        adam_update(w_fc_one, m_fc_one, v_fc_one, one_grad, decay_rate),
        adam_update(w_fc_two, m_fc_two, v_fc_two, two_grad, decay_rate),
        adam_update(qv_bias, m_qv_bias, v_qv_bias, qv_grad, 0.0),
        adam_update(fc_one_bias, m_fc_one_bias, v_fc_one_bias, bias_grad, 0.0),
        adam_update(rel_table, m_rel_table, v_rel_table, table_grad, 0.0),
        adam_update(norm_vec, m_norm_vec, v_norm_vec, norm_grad, 0.0),
    ]
    return (out, x_grad, *[grp[k] for k in range(3) for grp in groups])


def solution(mesh):
    params = (
        P(None, "dp", None, "mp"), P(None, "mp", "dp"), P(None, "dp", "mp"), P(None, "mp", "dp"),
        P(None, None, "mp"), P(None, "mp"), P(None, None, "mp"), P(),
    )
    act = (P("dp", None, None), P("dp", None, None))
    return jax.shard_map(
        functools.partial(local, mesh.shape["dp"] == PEERS),
        mesh=mesh,
        in_specs=(*act, P("dp"), P(), *params, *params, *params),
        out_specs=(*act, *params, *params, *params),
        check_vma=False,
    )
```
